32 devices in a mesh: dp: 1, sp: 32 (over x, y, z, core).
Axes of the slice: x: 2, y: 2, z: 4, core: 2. Of those that a mesh axis runs over, the one named last changes fastest.
Arguments:
- x: bfloat16 [4096, 4096], P(('dp', 'sp'))
- gain: bfloat16 [4096], replicated
- wq: bfloat16 [4096, 4096], replicated
- wk: bfloat16 [4096, 512], replicated
- wv: bfloat16 [4096, 512], replicated
- wo: bfloat16 [4096, 4096], replicated
Outputs:
- output: bfloat16 [4096, 4096], P(('dp', 'sp'))
All inputs are finite; a program needn't handle non-finite values.
Results may differ from the reference program's by a relative error of at most 0.012.
Values are sent between devices in bfloat16 or wider.
A program may use at most 2 GiB of HBM per device.

```python
import jax
import jax.numpy as jnp
from jax import lax

ROWS = 4096
D = 4096
HEADS = 32
KV_HEADS = 4
HEAD = 128
THETA = 10000


def setup_inputs(seed: int = 0, part: int = 0) -> dict:
    kx, kn, kq, kk, kv, ko = jax.random.split(jax.random.key(seed), 6)

    def weights(key, rows, columns):
        return jax.random.normal(key, (rows, columns), jnp.float32) * rows**-0.5

    drawn = {
        "x": jax.random.normal(jax.random.fold_in(kx, part), (ROWS, D), jnp.float32),
        "gain": 1 + 0.1 * jax.random.normal(kn, (D,), jnp.float32),
        "wq": 2 * weights(kq, D, HEADS * HEAD),
        "wk": 2 * weights(kk, D, KV_HEADS * HEAD),
        "wv": 4 * weights(kv, D, KV_HEADS * HEAD),
        "wo": weights(ko, HEADS * HEAD, D),
    }
    return {k: v.astype(jnp.bfloat16) for k, v in drawn.items()}


def normed(x, gain):
    wide = x.astype(jnp.float32)
    scale = lax.rsqrt(jnp.mean(wide * wide, -1, keepdims=True) + 1e-6)
    return (wide * scale * gain.astype(jnp.float32)).astype(jnp.bfloat16)


def turned(t, place, theta):
    half = t.shape[-1] // 2
    angle = place.astype(jnp.float32)[:, None] * theta ** (-jnp.arange(half, dtype=jnp.float32) / half)
    cos, sin = jnp.cos(angle)[:, None], jnp.sin(angle)[:, None]
    a, b = t[..., :half].astype(jnp.float32), t[..., half:].astype(jnp.float32)
    return jnp.concatenate([a * cos - b * sin, b * cos + a * sin], -1).astype(jnp.bfloat16)


def matmul(a, w):
    return jnp.dot(a, w, preferred_element_type=jnp.float32).astype(jnp.bfloat16)


def einsum(form, a, b):
    return jnp.einsum(form, a.astype(jnp.float32), b.astype(jnp.float32))


def attention(q, k, v):
    scores = einsum("tgsd,ugd->gstu", q, k) * q.shape[-1] ** -0.5
    token = jnp.arange(q.shape[0])
    scores = jnp.where(token[:, None] >= token, scores, -jnp.inf)
    weights = jax.nn.softmax(scores, -1).astype(jnp.bfloat16)
    return einsum("gstu,ugd->tgsd", weights, v).astype(jnp.bfloat16)


def reference(x, gain, wq, wk, wv, wo):
    a, place = normed(x, gain), jnp.arange(ROWS)
    q = turned(matmul(a, wq).reshape(ROWS, HEADS, HEAD), place, THETA).reshape(ROWS, KV_HEADS, -1, HEAD)
    k = turned(matmul(a, wk).reshape(ROWS, KV_HEADS, HEAD), place, THETA)
    v = matmul(a, wv).reshape(ROWS, KV_HEADS, HEAD)
    seen = attention(q, k, v).reshape(ROWS, HEADS * HEAD)
    return (x.astype(jnp.float32) + jnp.dot(seen, wo, preferred_element_type=jnp.float32)).astype(jnp.bfloat16)
```

```python
import functools

import jax
import jax.numpy as jnp
from jax import lax
from jax.experimental import pallas as pl
from jax.experimental.pallas import tpu as pltpu
from jax.sharding import PartitionSpec as P

HEAD = 128
THETA = 10000
LOG2E = 1.4426950408889634
HIDDEN = -2e30
D = 4096
OWN = 128
UNIT = 256
CHUNK = 512
E = HEAD**-0.5 * LOG2E
BF, F32 = jnp.bfloat16, jnp.float32


def _dot(a, b):
    return lax.dot_general(a, b, (((1,), (0,)), ((), ())), preferred_element_type=F32)


def kernel(x_hbm, gain_ref, wq_hbm, wk_hbm, wv_hbm, wo_hbm, cos_ref, sin_ref, y_ref,
           xs, a_s, wks, wvs, wqs, wos, kb, vb, qt, top_s, mix_s, seen_s, part_s, other_s,
           x_sem, k_sem, q_sem, o_sem, swap_sem, part_send, part_recv, send_sem, recv_sem):
    me = lax.axis_index("sp")
    core, chip = lax.rem(me, 2), lax.div(me, 2)
    z, line = lax.rem(chip, 4), lax.div(chip, 4)
    y, x = lax.rem(line, 2), lax.div(line, 2)
    partner = me + 1 - 2 * core
    over_x, over_y = me + 16 - 32 * x, me + 8 - 16 * y

    half = pl.multiple_of(core * 256, 256)
    get_x = pltpu.make_async_copy(x_hbm, xs.at[core], x_sem)
    get_k = pltpu.make_async_copy(wk_hbm.at[:, pl.ds(half, 256)], wks, k_sem.at[0])
    get_v = pltpu.make_async_copy(wv_hbm.at[:, pl.ds(half, 256)], wvs, k_sem.at[1])

    def get_q(c):
        at = pl.multiple_of(core * 2048 + c * CHUNK, CHUNK)
        return pltpu.make_async_copy(wq_hbm.at[:, pl.ds(at, CHUNK)], wqs.at[lax.rem(c, 3)], q_sem.at[c])

    def get_o(c):
        rows = pl.multiple_of(core * 2048, 2048)
        return pltpu.make_async_copy(wo_hbm.at[pl.ds(rows, 2048), pl.ds(pl.multiple_of(c * CHUNK, CHUNK), CHUNK)], wos.at[c], o_sem.at[c])

    get_x.start()
    get_k.start()
    get_v.start()
    for c in range(3):
        get_q(c).start()

    barrier = pltpu.get_barrier_semaphore()

    def greet(device):
        pl.semaphore_signal(barrier, inc=1, device_id={"sp": device}, device_id_type=pl.DeviceIdType.MESH)

    greet(partner)
    greet(over_x)
    greet(over_y)
    pl.when(z > 0)(lambda: greet(me - 2))
    pl.when(z < 3)(lambda: greet(me + 2))
    pl.semaphore_wait(barrier, jnp.where((z > 0) & (z < 3), 5, 4))

    def remote(src, dst, send, recv, device):
        return pltpu.make_async_remote_copy(src_ref=src, dst_ref=dst, send_sem=send, recv_sem=recv, device_id={"sp": device},
                                            device_id_type=pl.DeviceIdType.MESH)

    get_x.wait()
    swap = remote(xs.at[core], xs.at[core], swap_sem.at[0], swap_sem.at[1], partner)
    swap.start()

    def norm(which):
        def rows(r, _):
            at = pl.ds(pl.multiple_of(r * 32, 32), 32)
            wide = xs[which, at, :].astype(F32)
            scale = lax.rsqrt(jnp.mean(wide * wide, -1, keepdims=True) + 1e-6)
            a_s[which, at, :] = (wide * scale * gain_ref[...].astype(F32)).astype(BF)

        lax.fori_loop(0, OWN // 32, rows, None)

    norm(core)
    remote(xs.at[1 - core], xs.at[1 - core], swap_sem.at[0], swap_sem.at[1], partner).wait_recv()
    norm(1 - core)

    def turned(t):
        t = t.astype(F32)
        return (t * cos_ref[...] + pltpu.roll(t, HEAD // 2, 1) * sin_ref[...]).astype(BF)

    a = a_s[...].reshape(UNIT, D)
    get_k.wait()
    k = _dot(a, wks[...]).astype(BF)
    for i in range(2):
        kb[chip, i] = turned(k[:, i * HEAD : (i + 1) * HEAD])
    get_v.wait()
    v = _dot(a, wvs[...]).astype(BF)
    for i in range(2):
        vb[chip, i] = v[:, i * HEAD : (i + 1) * HEAD].T

    def block_copy(kind, j, port):
        device = (me + 2, me - 2, over_x, over_y)[port]
        buf = (kb, vb)[kind]
        return remote(buf.at[j], buf.at[j], send_sem.at[kind, port, j], recv_sem.at[kind, j], device)

    def arrived(kind, j):
        block_copy(kind, j, 2).wait_recv()

    def own_line(kind, zj):
        yes = [(zj <= z) & (z < 3), (zj >= z) & (z > 0) & (line < 3), x == 0, y == 0]
        return yes

    def forward_own(kind, zj, act):
        for port, yes in enumerate(own_line(kind, zj)):
            pl.when(yes)(lambda port=port: act(block_copy(kind, line * 4 + zj, port)))

    start = lambda copy: copy.start()
    for kind in range(2):
        forward_own(kind, z, start)

    def foreign(kind, lj):
        if lj == 0:
            return (2, 1) if kind == 0 else (3, 2)
        return (3, 3)

    def forward_foreign(kind, lj, zj, act):
        port, through = foreign(kind, lj)
        pl.when(line == through)(lambda: act(block_copy(kind, lj * 4 + zj, port)))

    def take_own(zj):
        for kind in range(2):
            arrived(kind, line * 4 + zj)
            forward_own(kind, zj, start)

    def take_foreign(lj, zj):
        for kind in range(2):
            arrived(kind, lj * 4 + zj)
            if lj < 2:
                forward_foreign(kind, lj, zj, start)

    def project_q(c, _):
        get_q(c).wait()
        q = _dot(a_s[...].reshape(UNIT, D), wqs[lax.rem(c, 3)]).astype(BF)
        for n in range(4):
            at = (n % 2) * UNIT
            qt[2 * c + n // 2, :, at : at + UNIT] = turned(q[:, n * HEAD : (n + 1) * HEAD]).T
        pl.when(c == 0)(lambda: get_q(3).start())

    lax.fori_loop(0, 4, project_q, None)
    for c in range(8):
        get_o(c).start()

    def attend(blocks, first=False):
        keys_n = len(blocks) * UNIT

        def head(i, _):
            keys = jnp.concatenate([kb[j, i] for j in blocks], 0)
            values = jnp.concatenate([jnp.concatenate([vb[j, i] for j in blocks], 1), jnp.ones((8, keys_n), BF)], 0)
            scores = [_dot(keys, qt[4 * i + n]) for n in range(4)]
            weights, keeps = [], []
            for n, s in enumerate(scores):
                if first:
                    key = lax.broadcasted_iota(jnp.int32, s.shape, 0)
                    query = lax.rem(lax.broadcasted_iota(jnp.int32, s.shape, 1), UNIT)
                    s = jnp.where(query >= key, s, HIDDEN)
                top = s.max(axis=0, keepdims=True)
                if not first:
                    old = top_s[4 * i + n]
                    top = jnp.maximum(old, top)
                    keeps.append(jnp.exp2((old - top) * E))
                top_s[4 * i + n] = top
                weights.append(jnp.exp2((s - top) * E).astype(BF))
            for n, p in enumerate(weights):
                new = _dot(values, p)
                mix_s[4 * i + n] = new if first else mix_s[4 * i + n] * keeps[n] + new

        lax.fori_loop(0, 2, head, None)

    attend([chip], first=True)

    def nth(k):
        low = z < 2
        return jnp.where(k == 0, z, jnp.where(k == 1, z + 1 - 2 * lax.rem(z, 2),
                         jnp.where(k == 2, jnp.where(low, 2, 1), jnp.where(low, 3, 0))))

    def round_(k, _):
        zk, before = nth(k), nth(k - 1)
        live = k < 4
        mine = live & (k > 0) & ((line < 3) | (zk < z))
        pl.when(mine)(lambda: take_own(zk))
        pl.when(live & ((line == 1) | (line == 2)))(lambda: take_foreign(0, zk))
        pl.when((line == 2) & (k > 0))(lambda: take_foreign(1, before))

        @pl.when(live & (line == 3))
        def _():
            take_foreign(1, zk)
            take_foreign(2, zk)
            take_foreign(0, zk)
            attend([zk, 4 + zk, 8 + zk])

        pl.when((line == 2) & live & (k > 0))(lambda: attend([zk, 4 + before]))
        lone = (line == 1) & live | (line == 2) & ((k == 0) | (k == 4))
        pl.when(lone)(lambda: attend([jnp.where(k == 4, 4 + before, zk)]))
        pl.when(mine & (zk < z))(lambda: attend([line * 4 + zk]))

    lax.fori_loop(0, 5, round_, None)

    for n in range(8):
        out = (mix_s[n, :HEAD, :] * (1 / mix_s[n, HEAD : HEAD + 1, :])).astype(BF)
        for m in range(2):
            h = 2 * n + m
            seen_s[:, h * HEAD : (h + 1) * HEAD] = out[:, m * UNIT : (m + 1) * UNIT].T

    def give(c):
        return remote(part_s.at[c, 1 - core], other_s.at[c], part_send.at[c], part_recv.at[c], partner)

    def finish(c):
        give(c).wait_recv()
        at = pl.ds(pl.multiple_of(c * CHUNK, CHUNK), CHUNK)
        y_ref[:, at] = (xs[core, :, at].astype(F32) + (part_s[c, core] + other_s[c])).astype(BF)

    def project_o(c, _):
        get_o(c).wait()
        part_s[c] = _dot(seen_s[...], wos[c]).reshape(2, OWN, CHUNK)
        give(c).start()
        pl.when(c >= 2)(lambda: finish(c - 2))

    lax.fori_loop(0, 8, project_o, None)
    finish(6)
    finish(7)

    swap.wait_send()
    lax.fori_loop(0, 8, lambda c, _: give(c).wait_send(), None)
    sent = lambda copy: copy.wait_send()

    def drain(zj, _):
        for kind in range(2):
            pl.when((line < 3) | (zj <= z))(lambda kind=kind: forward_own(kind, zj, sent))
            for lj in range(2):
                forward_foreign(kind, lj, zj, sent)

    lax.fori_loop(0, 4, drain, None)


def solution(mesh):
    def step(x, gain, wq, wk, wv, wo):
        chip = lax.axis_index("sp") // 2
        place = chip * UNIT + jnp.arange(UNIT)
        half = HEAD // 2
        angle = place.astype(F32)[:, None] * THETA ** (-jnp.arange(half, dtype=F32) / half)
        cos, sin = jnp.cos(angle), jnp.sin(angle)
        cos, sin = jnp.concatenate([cos, cos], -1), jnp.concatenate([-sin, sin], -1)
        hbm, vmem = pl.BlockSpec(memory_space=pl.ANY), pl.BlockSpec(memory_space=pltpu.VMEM)
        dma = pltpu.SemaphoreType.DMA
        return pl.pallas_call(
            kernel,
            out_shape=jax.ShapeDtypeStruct((OWN, D), BF),
            in_specs=[hbm, vmem, hbm, hbm, hbm, hbm, vmem, vmem],
            out_specs=vmem,
            scratch_shapes=[
                pltpu.VMEM((2, OWN, D), BF),
                pltpu.VMEM((2, OWN, D), BF),
                pltpu.VMEM((D, 256), BF),
                pltpu.VMEM((D, 256), BF),
                pltpu.VMEM((3, D, CHUNK), BF),
                pltpu.VMEM((8, 2048, CHUNK), BF),
                pltpu.VMEM((16, 2, UNIT, HEAD), BF),
                pltpu.VMEM((16, 2, HEAD, UNIT), BF),
                pltpu.VMEM((8, HEAD, 2 * UNIT), BF),
                pltpu.VMEM((8, 1, 2 * UNIT), F32),
                pltpu.VMEM((8, HEAD + 8, 2 * UNIT), F32),
                pltpu.VMEM((UNIT, 2048), BF),
                pltpu.VMEM((8, 2, OWN, CHUNK), F32),
                pltpu.VMEM((8, OWN, CHUNK), F32),
                dma, dma((2,)), dma((4,)), dma((8,)), dma((2,)), dma((8,)), dma((8,)), dma((2, 4, 16)), dma((2, 16)),
            ],
            compiler_params=pltpu.CompilerParams(collective_id=0, has_side_effects=True, vmem_limit_bytes=67043328),
        )(x, gain[None], wq, wk, wv, wo, cos, sin)

    tokens, whole = P(("dp", "sp"), None), P(None, None)
    return jax.shard_map(
        step,
        mesh=mesh,
        in_specs=(tokens, P(None), whole, whole, whole, whole),
        out_specs=tokens,
        check_vma=False,
    )
```

```python
import functools

import jax
import jax.numpy as jnp
from jax import lax
from jax.experimental import pallas as pl
from jax.experimental.pallas import tpu as pltpu
from jax.sharding import PartitionSpec as P

HEAD = 128
THETA = 10000
LOG2E = 1.4426950408889634
HIDDEN = -2e30
D = 4096
OWN = 128
PIECE = 32
UNIT = 256
CHUNK = 512
E = HEAD**-0.5 * LOG2E
BF, F32 = jnp.bfloat16, jnp.float32


def _dot(a, b):
    return lax.dot_general(a, b, (((1,), (0,)), ((), ())), preferred_element_type=F32)


def kernel(x_hbm, gain_ref, wq_hbm, wk_hbm, wv_hbm, wo_hbm, freq_ref, y_ref,
           xs, a_s, cos_s, sin_s, wkv, wqs, wos, kb, vb, qt, top_s, mix_s, seen_s, part_s, other_s,
           x_sem, k_sem, q_sem, o_sem, swap_send, swap_recv, part_send, part_recv, send_sem, recv_sem):
    me = lax.axis_index("sp")
    core, chip = lax.rem(me, 2), lax.div(me, 2)
    z, line = lax.rem(chip, 4), lax.div(chip, 4)
    y, x = lax.rem(line, 2), lax.div(line, 2)
    partner = me + 1 - 2 * core
    over_x, over_y = me + 16 - 32 * x, me + 8 - 16 * y

    half = pl.multiple_of(core * 256, 256)

    def get_x(r):
        return pltpu.make_async_copy(x_hbm.at[pl.ds(r * PIECE, PIECE)], xs.at[core, pl.ds(r * PIECE, PIECE)], x_sem.at[r])

    get_k = pltpu.make_async_copy(wk_hbm.at[:, pl.ds(half, 256)], wkv.at[:, :256], k_sem.at[0])
    get_v = pltpu.make_async_copy(wv_hbm.at[:, pl.ds(half, 256)], wkv.at[:, 256:], k_sem.at[1])

    def get_q(c):
        at = pl.multiple_of(core * 2048 + c * CHUNK, CHUNK)
        return pltpu.make_async_copy(wq_hbm.at[:, pl.ds(at, CHUNK)], wqs.at[lax.rem(c, 3)], q_sem.at[c])

    def get_o(c):
        rows = pl.multiple_of(core * 2048, 2048)
        return pltpu.make_async_copy(wo_hbm.at[pl.ds(rows, 2048), pl.ds(pl.multiple_of(c * CHUNK, CHUNK), CHUNK)], wos.at[c], o_sem.at[c])

    for r in range(OWN // PIECE):
        get_x(r).start()
    get_k.start()
    get_v.start()

    barrier = pltpu.get_barrier_semaphore()

    def greet(device):
        pl.semaphore_signal(barrier, inc=1, device_id={"sp": device}, device_id_type=pl.DeviceIdType.MESH)

    greet(partner)
    greet(over_x)
    greet(over_y)
    pl.when(z > 0)(lambda: greet(me - 2))
    pl.when(z < 3)(lambda: greet(me + 2))
    pl.semaphore_wait(barrier, jnp.where((z > 0) & (z < 3), 5, 4))

    def remote(src, dst, send, recv, device):
        return pltpu.make_async_remote_copy(src_ref=src, dst_ref=dst, send_sem=send, recv_sem=recv, device_id={"sp": device},
                                            device_id_type=pl.DeviceIdType.MESH)

    def swap(which, r):
        at = pl.ds(r * PIECE, PIECE)
        return remote(xs.at[which, at], xs.at[which, at], swap_send.at[r], swap_recv.at[r], partner)

    for r in range(OWN // PIECE):
        get_x(r).wait()
        swap(core, r).start()
    for c in range(3):
        get_q(c).start()

    place = chip * UNIT + lax.broadcasted_iota(jnp.int32, (UNIT, HEAD), 0)
    angle = place.astype(F32) * freq_ref[...]
    first_half = lax.broadcasted_iota(jnp.int32, (UNIT, HEAD), 1) < HEAD // 2
    cos_s[...] = jnp.cos(angle)
    sin = jnp.sin(angle)
    sin_s[...] = jnp.where(first_half, -sin, sin)

    def norm(which, r):
        at = pl.ds(r * PIECE, PIECE)
        wide = xs[which, at, :].astype(F32)
        scale = lax.rsqrt(jnp.mean(wide * wide, -1, keepdims=True) + 1e-6)
        a_s[which, at, :] = (wide * scale * gain_ref[...].astype(F32).reshape(1, D)).astype(BF)

    for r in range(OWN // PIECE):
        norm(core, r)
    for r in range(OWN // PIECE):
        swap(1 - core, r).wait_recv()
        norm(1 - core, r)

    def turned(t):
        t = t.astype(F32)
        return (t * cos_s[...] + pltpu.roll(t, HEAD // 2, 1) * sin_s[...]).astype(BF)

    a = a_s[...].reshape(UNIT, D)
    get_k.wait()
    get_v.wait()
    t = _dot(a, wkv[...]).astype(BF)
    for i in range(2):
        kb[chip, i] = turned(t[:, i * HEAD : (i + 1) * HEAD])
        vb[chip, i] = t[:, (2 + i) * HEAD : (3 + i) * HEAD].T

    def block_copy(kind, j, port):
        device = (me + 2, me - 2, over_x, over_y)[port]
        buf = (kb, vb)[kind]
        return remote(buf.at[j], buf.at[j], send_sem.at[kind, port, j], recv_sem.at[kind, j], device)

    def arrived(kind, j):
        block_copy(kind, j, 2).wait_recv()

    def own_line(kind, zj):
        yes = [(zj <= z) & (z < 3), (zj >= z) & (z > 0) & (line < 3), x == 0, y == 0]
        return yes

    def forward_own(kind, zj, act):
        for port, yes in enumerate(own_line(kind, zj)):
            pl.when(yes)(lambda port=port: act(block_copy(kind, line * 4 + zj, port)))

    start = lambda copy: copy.start()
    for kind in range(2):
        forward_own(kind, z, start)

    def foreign(kind, lj):
        if lj == 0:
            return (2, 1) if kind == 0 else (3, 2)
        return (3, 3)

    def forward_foreign(kind, lj, zj, act):
        port, through = foreign(kind, lj)
        pl.when(line == through)(lambda: act(block_copy(kind, lj * 4 + zj, port)))

    def take_own(zj):
        for kind in range(2):
            arrived(kind, line * 4 + zj)
            forward_own(kind, zj, start)

    def take_foreign(lj, zj):
        for kind in range(2):
            arrived(kind, lj * 4 + zj)
            if lj < 2:
                forward_foreign(kind, lj, zj, start)

    def project_q(c, _):
        get_q(c).wait()
        q = _dot(a_s[...].reshape(UNIT, D), wqs[lax.rem(c, 3)]).astype(BF)
        for n in range(4):
            at = (n % 2) * UNIT
            qt[2 * c + n // 2, :, at : at + UNIT] = turned(q[:, n * HEAD : (n + 1) * HEAD]).T
        pl.when(c == 0)(lambda: get_q(3).start())

    lax.fori_loop(0, 4, project_q, None)
    for c in range(8):
        get_o(c).start()

    def attend(blocks, first=False):
        keys_n = len(blocks) * UNIT

        def head(i, _):
            keys = jnp.concatenate([kb[j, i] for j in blocks], 0)
            values = jnp.concatenate([jnp.concatenate([vb[j, i] for j in blocks], 1), jnp.ones((8, keys_n), BF)], 0)
            scores = [_dot(keys, qt[4 * i + n]) for n in range(4)]
            weights, keeps = [], []
            for n, s in enumerate(scores):
                if first:
                    key = lax.broadcasted_iota(jnp.int32, s.shape, 0)
                    query = lax.rem(lax.broadcasted_iota(jnp.int32, s.shape, 1), UNIT)
                    s = jnp.where(query >= key, s, HIDDEN)
                top = s.max(axis=0, keepdims=True)
                if not first:
                    old = top_s[4 * i + n]
                    top = jnp.maximum(old, top)
                    keeps.append(jnp.exp2((old - top) * E))
                top_s[4 * i + n] = top
                weights.append(jnp.exp2((s - top) * E).astype(BF))
            for n, p in enumerate(weights):
                new = _dot(values, p)
                mix_s[4 * i + n] = new if first else mix_s[4 * i + n] * keeps[n] + new

        lax.fori_loop(0, 2, head, None)

    attend([chip], first=True)

    def nth(k):
        low = z < 2
        return jnp.where(k == 0, z, jnp.where(k == 1, z + 1 - 2 * lax.rem(z, 2),
                         jnp.where(k == 2, jnp.where(low, 2, 1), jnp.where(low, 3, 0))))

    def mine(k):
        return (k > 0) & (k < 4) & (nth(k) < z)

    def round_(k, _):
        zk, before = nth(k), nth(k - 1)
        live, own = k < 4, line * 4 + nth(k)
        pl.when(live & (k > 0) & (line < 3))(lambda: take_own(zk))
        pl.when(live & ((line == 1) | (line == 2)))(lambda: take_foreign(0, zk))
        pl.when((line == 2) & (k > 0))(lambda: take_foreign(1, before))

        @pl.when(live & (line == 3))
        def _():
            take_foreign(1, zk)
            pl.when(mine(k + 1))(lambda: take_own(nth(k + 1)))
            take_foreign(2, zk)
            pl.when((k == 3) & mine(k))(lambda: attend([4 + zk, 8 + zk, own]))
            pl.when((k == 3) & ~mine(k))(lambda: attend([4 + zk, 8 + zk]))
            take_foreign(0, zk)
            pl.when((k < 3) & mine(k))(lambda: attend([zk, 4 + zk, 8 + zk, own]))
            pl.when((k < 3) & ~mine(k))(lambda: attend([zk, 4 + zk, 8 + zk]))

        two = (line == 2) & live & (k > 0)
        pl.when(two & mine(k))(lambda: attend([zk, 4 + before, own]))
        pl.when(two & ~mine(k))(lambda: attend([zk, 4 + before]))
        pl.when((line == 1) & mine(k))(lambda: attend([zk, own]))
        lone = (line == 1) & live & ~mine(k) | (line == 2) & ((k == 0) | (k == 4)) | (line == 0) & mine(k) | (line == 3) & (k == 3)
        pl.when(lone)(lambda: attend([jnp.where(line == 0, own, jnp.where(k == 4, 4 + before, zk))]))

    lax.fori_loop(0, 5, round_, None)

    for n in range(8):
        out = (mix_s[n, :HEAD, :] * (1 / mix_s[n, HEAD : HEAD + 1, :])).astype(BF)
        for m in range(2):
            h = 2 * n + m
            seen_s[:, h * HEAD : (h + 1) * HEAD] = out[:, m * UNIT : (m + 1) * UNIT].T

    def give(c):
        return remote(part_s.at[c, 1 - core], other_s.at[c], part_send.at[c], part_recv.at[c], partner)

    def finish(c):
        give(c).wait_recv()
        at = pl.ds(pl.multiple_of(c * CHUNK, CHUNK), CHUNK)
        y_ref[:, at] = (xs[core, :, at].astype(F32) + (part_s[c, core] + other_s[c])).astype(BF)

    def project_o(c, _):
        get_o(c).wait()
        part_s[c] = _dot(seen_s[...], wos[c]).reshape(2, OWN, CHUNK)
        give(c).start()
        pl.when(c >= 2)(lambda: finish(c - 2))

    lax.fori_loop(0, 8, project_o, None)
    finish(6)
    finish(7)

    for r in range(OWN // PIECE):
        swap(core, r).wait_send()
    lax.fori_loop(0, 8, lambda c, _: give(c).wait_send(), None)
    sent = lambda copy: copy.wait_send()

    def drain(zj, _):
        for kind in range(2):
            pl.when((line < 3) | (zj <= z))(lambda kind=kind: forward_own(kind, zj, sent))
            for lj in range(2):
                forward_foreign(kind, lj, zj, sent)

    lax.fori_loop(0, 4, drain, None)


def solution(mesh):
    def step(x, gain, wq, wk, wv, wo):
        half = HEAD // 2
        freq = THETA ** (-jnp.arange(half, dtype=F32) / half)
        freq = jnp.concatenate([freq, freq])[None]
        hbm, vmem = pl.BlockSpec(memory_space=pl.ANY), pl.BlockSpec(memory_space=pltpu.VMEM)
        dma = pltpu.SemaphoreType.DMA
        return pl.pallas_call(
            kernel,
            out_shape=jax.ShapeDtypeStruct((OWN, D), BF),
            in_specs=[hbm, vmem, hbm, hbm, hbm, hbm, vmem],
            out_specs=vmem,
            scratch_shapes=[
                pltpu.VMEM((2, OWN, D), BF),
                pltpu.VMEM((2, OWN, D), BF),
                pltpu.VMEM((UNIT, HEAD), F32),
                pltpu.VMEM((UNIT, HEAD), F32),
                pltpu.VMEM((D, 512), BF),
                pltpu.VMEM((3, D, CHUNK), BF),
                pltpu.VMEM((8, 2048, CHUNK), BF),
                pltpu.VMEM((16, 2, UNIT, HEAD), BF),
                pltpu.VMEM((16, 2, HEAD, UNIT), BF),
                pltpu.VMEM((8, HEAD, 2 * UNIT), BF),
                pltpu.VMEM((8, 1, 2 * UNIT), F32),
                pltpu.VMEM((8, HEAD + 8, 2 * UNIT), F32),
                pltpu.VMEM((UNIT, 2048), BF),
                pltpu.VMEM((8, 2, OWN, CHUNK), F32),
                pltpu.VMEM((8, OWN, CHUNK), F32),
                dma((OWN // PIECE,)), dma((2,)), dma((4,)), dma((8,)), dma((OWN // PIECE,)), dma((OWN // PIECE,)), dma((8,)), dma((8,)), dma((2, 4, 16)), dma((2, 16)),
            ],
            compiler_params=pltpu.CompilerParams(collective_id=0, has_side_effects=True, vmem_limit_bytes=67043328),
        )(x, gain, wq, wk, wv, wo, freq)

    tokens, whole = P(("dp", "sp"), None), P(None, None)
    return jax.shard_map(
        step,
        mesh=mesh,
        in_specs=(tokens, P(None), whole, whole, whole, whole),
        out_specs=tokens,
        check_vma=False,
    )
```

```python
import jax
import jax.numpy as jnp
from jax import lax
from jax.experimental import pallas as pl
from jax.experimental.pallas import tpu as pltpu
from jax.sharding import PartitionSpec as P

scope = jax.named_scope
HEAD = 128
THETA = 10000
LOG2E = 1.4426950408889634
NEG = -1e30
HIDDEN = -2e30
D = 4096
OWN = 128
PIECE = 32
UNIT = 256
LINE = 4 * UNIT
CHUNK = 512
STRIP = 512
STRIPS = 4 * UNIT // STRIP
E = HEAD**-0.5 * LOG2E
BF, F32 = jnp.bfloat16, jnp.float32


def _dot(a, b):
    return lax.dot_general(a, b, (((1,), (0,)), ((), ())), preferred_element_type=F32)


def kernel(x_hbm, gain_ref, wq_hbm, wk_hbm, wv_hbm, wo_hbm, freq_ref, y_ref,
           xs, a_s, cos_s, sin_s, wkv, wqs, wos, kv, stage, qt, q_stage, vt, top_s, mix_s, seen_s, o_stage, part_s, other_s,
           x_sem, k_sem, wq_sem, wo_sem, swap_send, swap_recv, plane_send, block_recv, z_send, relay_send, hand_send, hand_recv,
           q_send, q_recv, out_send, out_recv, part_send, part_recv):
    me = lax.axis_index("sp")
    core, chip = lax.rem(me, 2), lax.div(me, 2)
    z, line = lax.rem(chip, 4), lax.div(chip, 4)
    y, x = lax.rem(line, 2), lax.div(line, 2)
    partner = me + 1 - 2 * core

    def in_plane(l):
        return me + (lax.div(l, 2) - x) * 16 + (lax.rem(l, 2) - y) * 8

    def mate(j):
        dx, dy = 1 - lax.div(j, 2), lax.rem(j + 1, 2)
        return lax.rem(x + dx, 2) * 2 + lax.rem(y + dy, 2)

    def get_x(r):
        at = pl.ds(r * PIECE, PIECE)
        return pltpu.make_async_copy(x_hbm.at[at], xs.at[core, at], x_sem.at[r])

    def get_kv(w):
        return pltpu.make_async_copy(w, wkv, k_sem)

    def get_q(j):
        at = pl.multiple_of(mate(j) * 1024 + core * 512, CHUNK)
        return pltpu.make_async_copy(wq_hbm.at[:, pl.ds(at, CHUNK)], wqs.at[lax.rem(j, 3)], wq_sem.at[j])

    def get_o(h):
        return pltpu.make_async_copy(wo_hbm.at[pl.ds(pl.multiple_of(h * 1024 + core * 512, CHUNK), CHUNK)], wos.at[h], wo_sem.at[h])

    for r in range(OWN // PIECE):
        get_x(r).start()
    pl.when(core == 0)(lambda: get_kv(wk_hbm).start())
    pl.when(core == 1)(lambda: get_kv(wv_hbm).start())

    kv[:, 12:] = jnp.zeros((2, 4, UNIT, HEAD), BF)

    barrier = pltpu.get_barrier_semaphore()

    def greet(device):
        pl.semaphore_signal(barrier, inc=1, device_id={"sp": device}, device_id_type=pl.DeviceIdType.MESH)

    greet(partner)
    for j in range(3):
        greet(in_plane(mate(j)))
    pl.when(z > 0)(lambda: greet(me - 2))
    pl.when(z < 3)(lambda: greet(me + 2))
    greet(jnp.where(z < 2, me + 4, me - 4))
    with scope("barrier"):
        pl.semaphore_wait(barrier, jnp.where((z > 0) & (z < 3), 7, 6))

    def remote(src, dst, send, recv, device):
        return pltpu.make_async_remote_copy(src_ref=src, dst_ref=dst, send_sem=send, recv_sem=recv, device_id={"sp": device},
                                            device_id_type=pl.DeviceIdType.MESH)

    def swap(which, r):
        at = pl.ds(r * PIECE, PIECE)
        return remote(xs.at[which, at], xs.at[which, at], swap_send.at[r], swap_recv.at[r], partner)

    with scope("x_in"):
        for r in range(OWN // PIECE):
            get_x(r).wait()
            swap(core, r).start()
    for j in range(3):
        get_q(j).start()

    place = chip * UNIT + lax.broadcasted_iota(jnp.int32, (UNIT, HEAD), 0)
    angle = place.astype(F32) * freq_ref[...]
    first_half = lax.broadcasted_iota(jnp.int32, (UNIT, HEAD), 1) < HEAD // 2
    cos_s[...] = jnp.cos(angle)
    sin = jnp.sin(angle)
    sin_s[...] = jnp.where(first_half, -sin, sin)

    def norm(which, r):
        at = pl.ds(r * PIECE, PIECE)
        wide = xs[which, at, :].astype(F32)
        scale = lax.rsqrt(jnp.mean(wide * wide, -1, keepdims=True) + 1e-6)
        a_s[which, at, :] = (wide * scale * gain_ref[...].astype(F32).reshape(1, D)).astype(BF)

    with scope("norm"):
        for r in range(OWN // PIECE):
            norm(core, r)
    with scope("swap"):
        for r in range(OWN // PIECE):
            swap(1 - core, r).wait_recv()
            norm(1 - core, r)

    def turned(t):
        t = t.astype(F32)
        return (t * cos_s[...] + pltpu.roll(t, HEAD // 2, 1) * sin_s[...]).astype(BF)

    def block(b):
        return kv.at[core, b]

    def to_mate(j):
        l = mate(j)
        return remote(stage.at[l], block(4 * line + z), plane_send.at[j], block_recv.at[4 * line + z], in_plane(l))

    def arrived(b):
        remote(block(b), block(b), z_send.at[0, 0], block_recv.at[b], partner).wait_recv()

    STEPS = (1, 2, -1, -2)

    def along_z(l, act):
        for i, step in enumerate(STEPS):
            b = 4 * l + z
            copy = remote(block(b), block(b), z_send.at[i, l], block_recv.at[b], me + 2 * step)
            there = z + step
            yes = (there >= 0) & (there < 4)
            if step < 0:
                yes = yes & (l < 3)
            pl.when(yes)(lambda copy=copy: act(copy))

    def relay(l, act):
        up = remote(block(4 * l), block(4 * l), relay_send.at[l], block_recv.at[4 * l], me + 2)
        down = remote(block(4 * l + 3), block(4 * l + 3), relay_send.at[l], block_recv.at[4 * l + 3], me - 2)
        pl.when(z == 2)(lambda: act(up))
        pl.when((z == 1) & (l < 3))(lambda: act(down))

    def hand(b):
        return remote(block(b), block(b), hand_send.at[b], hand_recv.at[b], partner)

    start = lambda copy: copy.start()
    sent = lambda copy: copy.wait_send()

    with scope("kvw"):
        get_kv(wk_hbm).wait()
    t = _dot(a_s[...].reshape(UNIT, D), wkv[...]).astype(BF)
    for h in range(4):
        own = t[:, h * HEAD : (h + 1) * HEAD]
        stage[h] = jnp.where(core == 0, turned(own), own)
    for j in range(3):
        to_mate(j).start()
    kv[core, 4 * line + z] = stage[line]
    along_z(line, start)
    hand(4 * line + z).start()

    def q_copy(j):
        return remote(q_stage.at[j], qt.at[line], q_send.at[j], q_recv.at[line], in_plane(mate(j)))

    def project_q(j, _):
        get_q(j).wait()
        q = _dot(a_s[...].reshape(UNIT, D), wqs[lax.rem(j, 3)]).astype(BF)
        for n in range(4):
            q_stage[j, :, n * UNIT : (n + 1) * UNIT] = turned(q[:, n * HEAD : (n + 1) * HEAD]).T
        pl.when(j < 3)(lambda: q_copy(j).start())

        @pl.when(j == 0)
        def _():
            get_q(3).start()

        @pl.when(j == 2)
        def _():
            with scope("plane"):
                def take(l, _):
                    @pl.when(l != line)
                    def _():
                        arrived(4 * l + z)
                        along_z(l, start)
                        hand(4 * l + z).start()

                lax.fori_loop(0, 4, take, None)

    with scope("q_proj"):
        lax.fori_loop(0, 4, project_q, None)
    qt[line] = q_stage[3]
    for h in range(4):
        get_o(h).start()

    for n in range(4 * STRIPS):
        top_s[n] = jnp.full((1, STRIP), NEG, F32)
        mix_s[n] = jnp.zeros((HEAD + 8, STRIP), F32)

    def used(l, place):
        return (place != z) & ((l < 3) | (place < z))

    def take_z(l):
        with scope("take_z"):
            for place in (0, 3, 1, 2):
                @pl.when(used(l, place))
                def _():
                    arrived(4 * l + place)
                    if place == 0:
                        pl.when(z == 2)(lambda: relay(l, start))
                    if place == 3:
                        pl.when(z == 1)(lambda: relay(l, start))
                    hand(4 * l + place).start()

    def attend(l, g, masked):
        with scope("attend#m=%d" % masked):
            keys = kv[0, pl.ds(4 * g, 4)].reshape(LINE, HEAD)
            values = jnp.concatenate([vt[...], jnp.ones((8, LINE), BF)], 0)
            scores = [_dot(keys, qt[l, :, n * STRIP : (n + 1) * STRIP]) for n in range(STRIPS)]
            weights, keeps = [], []
            for n, s in enumerate(scores):
                if masked:
                    key = lax.broadcasted_iota(jnp.int32, s.shape, 0)
                    query = z * UNIT + lax.rem(lax.broadcasted_iota(jnp.int32, s.shape, 1), UNIT)
                    s = jnp.where(query >= key, s, HIDDEN)
                old = top_s[STRIPS * l + n]
                top = jnp.maximum(old, s.max(axis=0, keepdims=True))
                top_s[STRIPS * l + n] = top
                keeps.append(jnp.exp2((old - top) * E))
                weights.append(jnp.exp2((s - top) * E).astype(BF))
            for n, p in enumerate(weights):
                mix_s[STRIPS * l + n] = mix_s[STRIPS * l + n] * keeps[n] + _dot(values, p)

    def out_copy(l):
        return remote(o_stage.at[l], seen_s.at[line], out_send.at[l], out_recv.at[line], in_plane(l))

    def complete(l):
        with scope("complete"):
            per = STRIP // UNIT
            for n in range(STRIPS):
                out = (mix_s[STRIPS * l + n, :HEAD, :] * (1 / mix_s[STRIPS * l + n, HEAD : HEAD + 1, :])).astype(BF)
                for m in range(per):
                    h = per * n + m
                    o_stage[l, :, h * HEAD : (h + 1) * HEAD] = out[:, m * UNIT : (m + 1) * UNIT].T
            pl.when(l != line)(lambda: out_copy(l).start())

            @pl.when(l == line)
            def _():
                seen_s[line] = o_stage[l]

    def meet(g, _):
        with scope("hand_wait"):
            for place in range(4):
                @pl.when((g < 3) | (place <= z))
                def _():
                    b = 4 * g + place
                    remote(kv.at[1 - core, b], kv.at[1 - core, b], hand_send.at[b], hand_recv.at[b], partner).wait_recv()
        for i in range(4):
            vt[:, i * UNIT : (i + 1) * UNIT] = kv[1, 4 * g + i].T

        def row(i, _):
            l = jnp.where(g == 0, mate(lax.rem(i + 3, 4)), i)

            @pl.when((g == 0) & (l != line))
            def _():
                with scope("q_wait"):
                    remote(qt.at[l], qt.at[l], q_send.at[0], q_recv.at[l], partner).wait_recv()

            @pl.when(l == g)
            def _():
                attend(l, g, True)
                complete(l)

            pl.when(l > g)(lambda: attend(l, g, False))
            pl.when((i == 1) & (g < 3))(lambda: take_z(g + 1))

        lax.fori_loop(0, 4, row, None)

    take_z(0)
    lax.fori_loop(0, 4, meet, None)

    def give(c):
        return remote(part_s.at[c, 1 - core], other_s.at[c], part_send.at[c], part_recv.at[c], partner)

    def product(c, hs):
        at = pl.ds(pl.multiple_of(c * CHUNK, CHUNK), CHUNK)
        seen = jnp.concatenate([seen_s[h] for h in hs], 1)
        return _dot(seen, jnp.concatenate([wos[h, :, at] for h in hs], 0)).reshape(2, OWN, CHUNK)

    def finish(c):
        give(c).wait_recv()
        at = pl.ds(pl.multiple_of(c * CHUNK, CHUNK), CHUNK)
        y_ref[:, at] = (xs[core, :, at].astype(F32) + (part_s[c, core] + other_s[c])).astype(BF)

    def seen_wait(l):
        with scope("seen_wait"):
            remote(seen_s.at[l], seen_s.at[l], out_send.at[0], out_recv.at[l], partner).wait_recv()

    for h in range(4):
        get_o(h).wait()
    seen_wait(mate(1))
    early, late = (line, mate(1)), (mate(2), mate(0))

    def project_early(c, _):
        part_s[c] = product(c, early)

    def project_late(c, _):
        part_s[c] = part_s[c] + product(c, late)
        give(c).start()
        pl.when(c >= 2)(lambda: finish(c - 2))

    with scope("o_early"):
        lax.fori_loop(0, 8, project_early, None)
    seen_wait(mate(2))
    seen_wait(mate(0))
    with scope("o_late"):
        lax.fori_loop(0, 8, project_late, None)
    with scope("finish"):
        finish(6)
        finish(7)

    for r in range(OWN // PIECE):
        swap(core, r).wait_send()
    for j in range(3):
        to_mate(j).wait_send()
        q_copy(j).wait_send()

    def drain(l, _):
        along_z(l, sent)
        relay(l, sent)
        pl.when(l != line)(lambda: out_copy(l).wait_send())
        for place in range(4):
            pl.when((l < 3) | (place <= z))(lambda place=place: hand(4 * l + place).wait_send())

    lax.fori_loop(0, 4, drain, None)
    lax.fori_loop(0, 8, lambda c, _: give(c).wait_send(), None)


def solution(mesh):
    def step(x, gain, wq, wk, wv, wo):
        half = HEAD // 2
        freq = THETA ** (-jnp.arange(half, dtype=F32) / half)
        freq = jnp.concatenate([freq, freq])[None]
        hbm, vmem = pl.BlockSpec(memory_space=pl.ANY), pl.BlockSpec(memory_space=pltpu.VMEM)
        dma = lambda *shape: pltpu.SemaphoreType.DMA(shape)
        return pl.pallas_call(
            kernel,
            out_shape=jax.ShapeDtypeStruct((OWN, D), BF),
            in_specs=[hbm, vmem, hbm, hbm, hbm, hbm, vmem],
            out_specs=vmem,
            scratch_shapes=[
                pltpu.VMEM((2, OWN, D), BF),
                pltpu.VMEM((2, OWN, D), BF),
                pltpu.VMEM((UNIT, HEAD), F32),
                pltpu.VMEM((UNIT, HEAD), F32),
                pltpu.VMEM((D, 512), BF),
                pltpu.VMEM((3, D, CHUNK), BF),
                pltpu.VMEM((4, CHUNK, D), BF),
                pltpu.VMEM((2, 16, UNIT, HEAD), BF),
                pltpu.VMEM((4, UNIT, HEAD), BF),
                pltpu.VMEM((4, HEAD, 4 * UNIT), BF),
                pltpu.VMEM((4, HEAD, 4 * UNIT), BF),
                pltpu.VMEM((HEAD, LINE), BF),
                pltpu.VMEM((4 * STRIPS, 1, STRIP), F32),
                pltpu.VMEM((4 * STRIPS, HEAD + 8, STRIP), F32),
                pltpu.VMEM((4, UNIT, 4 * HEAD), BF),
                pltpu.VMEM((4, UNIT, 4 * HEAD), BF),
                pltpu.VMEM((8, 2, OWN, CHUNK), F32),
                pltpu.VMEM((8, OWN, CHUNK), F32),
                dma(OWN // PIECE), pltpu.SemaphoreType.DMA, dma(4), dma(4), dma(OWN // PIECE), dma(OWN // PIECE),
                dma(3), dma(16), dma(4, 4), dma(4), dma(16), dma(16),
                dma(3), dma(4), dma(4), dma(4), dma(8), dma(8),
            ],
            compiler_params=pltpu.CompilerParams(collective_id=0, has_side_effects=True, vmem_limit_bytes=67043328),
        )(x, gain, wq, wk, wv, wo, freq)

    tokens, whole = P(("dp", "sp"), None), P(None, None)
    return jax.shard_map(
        step,
        mesh=mesh,
        in_specs=(tokens, P(None), whole, whole, whole, whole),
        out_specs=tokens,
        check_vma=False,
    )
```

```python
import jax
import jax.numpy as jnp
from jax import lax
from jax.experimental import pallas as pl
from jax.experimental.pallas import tpu as pltpu
from jax.sharding import PartitionSpec as P

scope = jax.named_scope
HEAD = 128
THETA = 10000
LOG2E = 1.4426950408889634
NEG = -1e30
HIDDEN = -2e30
D = 4096
OWN = 128
PIECE = 32
UNIT = 256
LINE = 4 * UNIT
CHUNK = 512
STRIP = 512
STRIPS = 4 * UNIT // STRIP
E = HEAD**-0.5 * LOG2E
BF, F32 = jnp.bfloat16, jnp.float32


def _dot(a, b):
    return lax.dot_general(a, b, (((1,), (0,)), ((), ())), preferred_element_type=F32)


def kernel(x_hbm, gain_ref, wq_hbm, wk_hbm, wv_hbm, wo_hbm, freq_ref, y_hbm,
           xs, a_s, cos_s, sin_s, wkv, wqs, wos, kv, stage, qt, q_stage, vt, top_s, mix_s, seen_s, o_stage, part_s, other_s, y_s,
           x_sem, k_sem, wq_sem, wo_sem, swap_send, swap_recv, plane_send, block_recv, z_send, relay_send, hand_send, hand_recv,
           q_send, q_recv, out_send, out_recv, part_send, part_recv, y_sem):
    me = lax.axis_index("sp")
    core, chip = lax.rem(me, 2), lax.div(me, 2)
    z, line = lax.rem(chip, 4), lax.div(chip, 4)
    y, x = lax.rem(line, 2), lax.div(line, 2)
    partner = me + 1 - 2 * core

    def in_plane(l):
        return me + (lax.div(l, 2) - x) * 16 + (lax.rem(l, 2) - y) * 8

    def mate(j):
        dx, dy = 1 - lax.div(j, 2), lax.rem(j + 1, 2)
        return lax.rem(x + dx, 2) * 2 + lax.rem(y + dy, 2)

    def get_x(r):
        at = pl.ds(r * PIECE, PIECE)
        return pltpu.make_async_copy(x_hbm.at[at], xs.at[core, at], x_sem.at[r])

    def get_kv(w):
        return pltpu.make_async_copy(w, wkv, k_sem)

    def get_q(j):
        at = pl.multiple_of(mate(j) * 1024 + core * 512, CHUNK)
        return pltpu.make_async_copy(wq_hbm.at[:, pl.ds(at, CHUNK)], wqs.at[lax.rem(j, 3)], wq_sem.at[j])

    def get_o(h):
        return pltpu.make_async_copy(wo_hbm.at[pl.ds(pl.multiple_of(h * 1024 + core * 512, CHUNK), CHUNK)], wos.at[h], wo_sem.at[h])

    for r in range(OWN // PIECE):
        get_x(r).start()
    pl.when(core == 0)(lambda: get_kv(wk_hbm).start())
    pl.when(core == 1)(lambda: get_kv(wv_hbm).start())

    kv[:, 12:] = jnp.zeros((2, 4, UNIT, HEAD), BF)

    barrier = pltpu.get_barrier_semaphore()

    def greet(device):
        pl.semaphore_signal(barrier, inc=1, device_id={"sp": device}, device_id_type=pl.DeviceIdType.MESH)

    greet(partner)
    for j in range(3):
        greet(in_plane(mate(j)))
    pl.when(z > 0)(lambda: greet(me - 2))
    pl.when(z < 3)(lambda: greet(me + 2))
    greet(jnp.where(z < 2, me + 4, me - 4))
    with scope("barrier"):
        pl.semaphore_wait(barrier, jnp.where((z > 0) & (z < 3), 7, 6))

    def remote(src, dst, send, recv, device):
        return pltpu.make_async_remote_copy(src_ref=src, dst_ref=dst, send_sem=send, recv_sem=recv, device_id={"sp": device},
                                            device_id_type=pl.DeviceIdType.MESH)

    def swap(which, r):
        at = pl.ds(r * PIECE, PIECE)
        return remote(xs.at[which, at], xs.at[which, at], swap_send.at[r], swap_recv.at[r], partner)

    with scope("x_in"):
        for r in range(OWN // PIECE):
            get_x(r).wait()
            swap(core, r).start()
    for j in range(3):
        get_q(j).start()

    place = chip * UNIT + lax.broadcasted_iota(jnp.int32, (UNIT, HEAD), 0)
    angle = place.astype(F32) * freq_ref[...]
    first_half = lax.broadcasted_iota(jnp.int32, (UNIT, HEAD), 1) < HEAD // 2
    cos_s[...] = jnp.cos(angle)
    sin = jnp.sin(angle)
    sin_s[...] = jnp.where(first_half, -sin, sin)

    def norm(which, r):
        at = pl.ds(r * PIECE, PIECE)
        wide = xs[which, at, :].astype(F32)
        scale = lax.rsqrt(jnp.mean(wide * wide, -1, keepdims=True) + 1e-6)
        a_s[which, at, :] = (wide * scale * gain_ref[...].astype(F32).reshape(1, D)).astype(BF)

    with scope("norm"):
        for r in range(OWN // PIECE):
            norm(core, r)
    with scope("swap"):
        for r in range(OWN // PIECE):
            swap(1 - core, r).wait_recv()
            norm(1 - core, r)

    def turned(t):
        t = t.astype(F32)
        return (t * cos_s[...] + pltpu.roll(t, HEAD // 2, 1) * sin_s[...]).astype(BF)

    def block(b):
        return kv.at[core, b]

    def to_mate(j):
        l = mate(j)
        return remote(stage.at[l], block(4 * line + z), plane_send.at[j], block_recv.at[4 * line + z], in_plane(l))

    def arrived(b):
        remote(block(b), block(b), z_send.at[0, 0], block_recv.at[b], partner).wait_recv()

    STEPS = (1, 2, -1, -2)

    def along_z(l, act):
        for i, step in enumerate(STEPS):
            b = 4 * l + z
            copy = remote(block(b), block(b), z_send.at[i, l], block_recv.at[b], me + 2 * step)
            there = z + step
            yes = (there >= 0) & (there < 4)
            if step < 0:
                yes = yes & (l < 3)
            pl.when(yes)(lambda copy=copy: act(copy))

    def relay(l, act):
        up = remote(block(4 * l), block(4 * l), relay_send.at[l], block_recv.at[4 * l], me + 2)
        down = remote(block(4 * l + 3), block(4 * l + 3), relay_send.at[l], block_recv.at[4 * l + 3], me - 2)
        pl.when(z == 2)(lambda: act(up))
        pl.when((z == 1) & (l < 3))(lambda: act(down))

    def hand(b):
        return remote(block(b), block(b), hand_send.at[b], hand_recv.at[b], partner)

    start = lambda copy: copy.start()
    sent = lambda copy: copy.wait_send()

    with scope("kvw"):
        get_kv(wk_hbm).wait()
    t = _dot(a_s[...].reshape(UNIT, D), wkv[...]).astype(BF)
    for h in range(4):
        own = t[:, h * HEAD : (h + 1) * HEAD]
        stage[h] = jnp.where(core == 0, turned(own), own)
    for j in range(3):
        to_mate(j).start()
    kv[core, 4 * line + z] = stage[line]
    along_z(line, start)
    hand(4 * line + z).start()

    def q_copy(j):
        return remote(q_stage.at[j], qt.at[line], q_send.at[j], q_recv.at[line], in_plane(mate(j)))

    def project_q(j, _):
        get_q(j).wait()
        q = _dot(a_s[...].reshape(UNIT, D), wqs[lax.rem(j, 3)]).astype(BF)
        for n in range(4):
            q_stage[j, :, n * UNIT : (n + 1) * UNIT] = turned(q[:, n * HEAD : (n + 1) * HEAD]).T
        pl.when(j < 3)(lambda: q_copy(j).start())

        @pl.when(j == 0)
        def _():
            get_q(3).start()

        @pl.when(j == 2)
        def _():
            with scope("plane"):
                def take(l, _):
                    @pl.when(l != line)
                    def _():
                        arrived(4 * l + z)
                        along_z(l, start)
                        hand(4 * l + z).start()

                lax.fori_loop(0, 4, take, None)

    with scope("q_proj"):
        lax.fori_loop(0, 4, project_q, None)
    qt[line] = q_stage[3]
    for h in range(4):
        get_o(h).start()

    for n in range(4 * STRIPS):
        top_s[n] = jnp.full((1, STRIP), NEG, F32)
        mix_s[n] = jnp.zeros((HEAD + 8, STRIP), F32)

    def used(l, place):
        return (place != z) & ((l < 3) | (place < z))

    def take_z(l):
        with scope("take_z"):
            for place in (0, 3, 1, 2):
                @pl.when(used(l, place))
                def _():
                    arrived(4 * l + place)
                    if place == 0:
                        pl.when(z == 2)(lambda: relay(l, start))
                    if place == 3:
                        pl.when(z == 1)(lambda: relay(l, start))
                    hand(4 * l + place).start()

    def attend(l, g, masked):
        with scope("attend#m=%d" % masked):
            keys = kv[0, pl.ds(4 * g, 4)].reshape(LINE, HEAD)
            values = jnp.concatenate([vt[g], jnp.ones((8, LINE), BF)], 0)
            scores = [_dot(keys, qt[l, :, n * STRIP : (n + 1) * STRIP]) for n in range(STRIPS)]
            weights, keeps = [], []
            for n, s in enumerate(scores):
                if masked:
                    key = lax.broadcasted_iota(jnp.int32, s.shape, 0)
                    query = z * UNIT + lax.rem(lax.broadcasted_iota(jnp.int32, s.shape, 1), UNIT)
                    s = jnp.where(query >= key, s, HIDDEN)
                old = top_s[STRIPS * l + n]
                top = jnp.maximum(old, s.max(axis=0, keepdims=True))
                top_s[STRIPS * l + n] = top
                keeps.append(jnp.exp2((old - top) * E))
                weights.append(jnp.exp2((s - top) * E).astype(BF))
            for n, p in enumerate(weights):
                mix_s[STRIPS * l + n] = mix_s[STRIPS * l + n] * keeps[n] + _dot(values, p)

    def out_copy(l):
        return remote(o_stage.at[l], seen_s.at[line], out_send.at[l], out_recv.at[line], in_plane(l))

    def complete(l):
        with scope("complete"):
            per = STRIP // UNIT
            for n in range(STRIPS):
                out = (mix_s[STRIPS * l + n, :HEAD, :] * (1 / mix_s[STRIPS * l + n, HEAD : HEAD + 1, :])).astype(BF)
                for m in range(per):
                    h = per * n + m
                    o_stage[l, :, h * HEAD : (h + 1) * HEAD] = out[:, m * UNIT : (m + 1) * UNIT].T
            pl.when(l != line)(lambda: out_copy(l).start())

            @pl.when(l == line)
            def _():
                seen_s[line] = o_stage[l]

    def ready(g):
        take_z(g)
        with scope("hand_wait"):
            for place in range(4):
                @pl.when((g < 3) | (place <= z))
                def _():
                    b = 4 * g + place
                    remote(kv.at[1 - core, b], kv.at[1 - core, b], hand_send.at[b], hand_recv.at[b], partner).wait_recv()
        for i in range(4):
            vt[g, :, i * UNIT : (i + 1) * UNIT] = kv[1, 4 * g + i].T

    takes = (0, 1, jnp.where(line < 2, 2, 4), jnp.where(line == 3, 7, 3 + line))

    def row(j, s):
        l = mate(j)

        def meet(g, s):
            for i in range(4):
                pl.when(s == takes[i])(lambda i=i: ready(i))

            @pl.when((g == 0) & (l != line))
            def _():
                with scope("q_wait"):
                    remote(qt.at[l], qt.at[l], q_send.at[0], q_recv.at[l], partner).wait_recv()

            pl.when(l == g)(lambda: attend(l, g, True))
            pl.when(l > g)(lambda: attend(l, g, False))
            return s + 1

        s = lax.fori_loop(0, l + 1, meet, s)
        complete(l)
        return s

    lax.fori_loop(0, 4, row, 0)

    def give(c):
        return remote(part_s.at[c, 1 - core], other_s.at[c], part_send.at[c], part_recv.at[c], partner)

    def product(c, hs):
        at = pl.ds(pl.multiple_of(c * CHUNK, CHUNK), CHUNK)
        seen = jnp.concatenate([seen_s[h] for h in hs], 1)
        return _dot(seen, jnp.concatenate([wos[h, :, at] for h in hs], 0)).reshape(2, OWN, CHUNK)

    def put(c):
        return pltpu.make_async_copy(y_s.at[c], y_hbm.at[:, pl.ds(pl.multiple_of(c * CHUNK, CHUNK), CHUNK)], y_sem.at[c])

    def finish(c):
        give(c).wait_recv()
        at = pl.ds(pl.multiple_of(c * CHUNK, CHUNK), CHUNK)
        y_s[c] = (xs[core, :, at].astype(F32) + (part_s[c, core] + other_s[c])).astype(BF)
        put(c).start()

    def seen_wait(l):
        with scope("seen_wait"):
            remote(seen_s.at[l], seen_s.at[l], out_send.at[0], out_recv.at[l], partner).wait_recv()

    for h in range(4):
        get_o(h).wait()
    seen_wait(mate(1))
    seen_wait(mate(0))
    early, late = (mate(0), mate(1), line), (mate(2),)

    def project_early(c, _):
        part_s[c] = product(c, early)

    def project_late(c, _):
        part_s[c] = part_s[c] + product(c, late)
        give(c).start()
        pl.when(c >= 2)(lambda: finish(c - 2))

    with scope("o_early"):
        lax.fori_loop(0, 8, project_early, None)
    seen_wait(mate(2))
    with scope("o_late"):
        lax.fori_loop(0, 8, project_late, None)
    with scope("finish"):
        finish(6)
        finish(7)

    for r in range(OWN // PIECE):
        swap(core, r).wait_send()
    for j in range(3):
        to_mate(j).wait_send()
        q_copy(j).wait_send()

    def drain(l, _):
        along_z(l, sent)
        relay(l, sent)
        pl.when(l != line)(lambda: out_copy(l).wait_send())
        for place in range(4):
            pl.when((l < 3) | (place <= z))(lambda place=place: hand(4 * l + place).wait_send())

    lax.fori_loop(0, 4, drain, None)

    def drain_chunk(c, _):
        give(c).wait_send()
        put(c).wait()

    lax.fori_loop(0, 8, drain_chunk, None)


def solution(mesh):
    def step(x, gain, wq, wk, wv, wo):
        half = HEAD // 2
        freq = THETA ** (-jnp.arange(half, dtype=F32) / half)
        freq = jnp.concatenate([freq, freq])[None]
        hbm, vmem = pl.BlockSpec(memory_space=pl.ANY), pl.BlockSpec(memory_space=pltpu.VMEM)
        dma = lambda *shape: pltpu.SemaphoreType.DMA(shape)
        return pl.pallas_call(
            kernel,
            out_shape=jax.ShapeDtypeStruct((OWN, D), BF),
            in_specs=[hbm, vmem, hbm, hbm, hbm, hbm, vmem],
            out_specs=hbm,
            scratch_shapes=[
                pltpu.VMEM((2, OWN, D), BF),
                pltpu.VMEM((2, OWN, D), BF),
                pltpu.VMEM((UNIT, HEAD), F32),
                pltpu.VMEM((UNIT, HEAD), F32),
                pltpu.VMEM((D, 512), BF),
                pltpu.VMEM((3, D, CHUNK), BF),
                pltpu.VMEM((4, CHUNK, D), BF),
                pltpu.VMEM((2, 16, UNIT, HEAD), BF),
                pltpu.VMEM((4, UNIT, HEAD), BF),
                pltpu.VMEM((4, HEAD, 4 * UNIT), BF),
                pltpu.VMEM((4, HEAD, 4 * UNIT), BF),
                pltpu.VMEM((4, HEAD, LINE), BF),
                pltpu.VMEM((4 * STRIPS, 1, STRIP), F32),
                pltpu.VMEM((4 * STRIPS, HEAD + 8, STRIP), F32),
                pltpu.VMEM((4, UNIT, 4 * HEAD), BF),
                pltpu.VMEM((4, UNIT, 4 * HEAD), BF),
                pltpu.VMEM((8, 2, OWN, CHUNK), F32),
                pltpu.VMEM((8, OWN, CHUNK), F32),
                pltpu.VMEM((8, OWN, CHUNK), BF),
                dma(OWN // PIECE), pltpu.SemaphoreType.DMA, dma(4), dma(4), dma(OWN // PIECE), dma(OWN // PIECE),
                dma(3), dma(16), dma(4, 4), dma(4), dma(16), dma(16),
                dma(3), dma(4), dma(4), dma(4), dma(8), dma(8), dma(8),
            ],
            compiler_params=pltpu.CompilerParams(collective_id=0, has_side_effects=True, vmem_limit_bytes=67043328),
        )(x, gain, wq, wk, wv, wo, freq)

    tokens, whole = P(("dp", "sp"), None), P(None, None)
    return jax.shard_map(
        step,
        mesh=mesh,
        in_specs=(tokens, P(None), whole, whole, whole, whole),
        out_specs=tokens,
        check_vma=False,
    )
```

```python
import jax
import jax.numpy as jnp
from jax import lax
from jax.experimental import pallas as pl
from jax.experimental.pallas import tpu as pltpu
from jax.sharding import PartitionSpec as P

scope = jax.named_scope
HEAD = 128
THETA = 10000
LOG2E = 1.4426950408889634
NEG = -1e30
HIDDEN = -2e30
D = 4096
OWN = 128
PIECE = 32
UNIT = 256
LINE = 4 * UNIT
CHUNK = 512
STRIP = 512
STRIPS = 4 * UNIT // STRIP
E = HEAD**-0.5 * LOG2E
BF, F32 = jnp.bfloat16, jnp.float32


def _dot(a, b):
    return lax.dot_general(a, b, (((1,), (0,)), ((), ())), preferred_element_type=F32)


def kernel(x_hbm, gain_ref, wq_hbm, wk_hbm, wv_hbm, wo_hbm, freq_ref, y_hbm,
           xs, a_s, cos_s, sin_s, wkv, wqs, wos, kv, stage, qt, q_stage, vt, top_s, mix_s, seen_s, o_stage, part_s, other_s, y_s,
           x_sem, k_sem, wq_sem, wo_sem, swap_send, swap_recv, plane_send, block_recv, z_send, relay_send, hand_send, hand_recv,
           q_send, q_recv, out_send, out_recv, part_send, part_recv, y_sem):
    me = lax.axis_index("sp")
    core, chip = lax.rem(me, 2), lax.div(me, 2)
    z, line = lax.rem(chip, 4), lax.div(chip, 4)
    y, x = lax.rem(line, 2), lax.div(line, 2)
    partner = me + 1 - 2 * core

    def in_plane(l):
        return me + (lax.div(l, 2) - x) * 16 + (lax.rem(l, 2) - y) * 8

    def mate(j):
        dx, dy = 1 - lax.div(j, 2), lax.rem(j + 1, 2)
        return lax.rem(x + dx, 2) * 2 + lax.rem(y + dy, 2)

    def get_x(r):
        at = pl.ds(r * PIECE, PIECE)
        return pltpu.make_async_copy(x_hbm.at[at], xs.at[core, at], x_sem.at[r])

    def get_kv(w):
        return pltpu.make_async_copy(w, wkv, k_sem)

    def get_q(j):
        at = pl.multiple_of(mate(j) * 1024 + core * 512, CHUNK)
        return pltpu.make_async_copy(wq_hbm.at[:, pl.ds(at, CHUNK)], wqs.at[lax.rem(j, 3)], wq_sem.at[j])

    def get_o(h):
        return pltpu.make_async_copy(wo_hbm.at[pl.ds(pl.multiple_of(h * 1024 + core * 512, CHUNK), CHUNK)], wos.at[h], wo_sem.at[h])

    for r in range(OWN // PIECE):
        get_x(r).start()
    pl.when(core == 0)(lambda: get_kv(wk_hbm).start())
    pl.when(core == 1)(lambda: get_kv(wv_hbm).start())

    kv[:, 12:] = jnp.zeros((2, 4, UNIT, HEAD), BF)

    barrier = pltpu.get_barrier_semaphore()

    def greet(device):
        pl.semaphore_signal(barrier, inc=1, device_id={"sp": device}, device_id_type=pl.DeviceIdType.MESH)

    greet(partner)
    for j in range(3):
        greet(in_plane(mate(j)))
    pl.when(z > 0)(lambda: greet(me - 2))
    pl.when(z < 3)(lambda: greet(me + 2))
    greet(jnp.where(z < 2, me + 4, me - 4))
    pl.when(z == 0)(lambda: greet(me + 6))
    pl.when(z == 3)(lambda: greet(me - 6))
    with scope("barrier"):
        pl.semaphore_wait(barrier, 7)

    def remote(src, dst, send, recv, device):
        return pltpu.make_async_remote_copy(src_ref=src, dst_ref=dst, send_sem=send, recv_sem=recv, device_id={"sp": device},
                                            device_id_type=pl.DeviceIdType.MESH)

    def swap(which, r):
        at = pl.ds(r * PIECE, PIECE)
        return remote(xs.at[which, at], xs.at[which, at], swap_send.at[r], swap_recv.at[r], partner)

    with scope("x_in"):
        for r in range(OWN // PIECE):
            get_x(r).wait()
            swap(core, r).start()
    for j in range(3):
        get_q(j).start()

    place = chip * UNIT + lax.broadcasted_iota(jnp.int32, (UNIT, HEAD), 0)
    angle = place.astype(F32) * freq_ref[...]
    first_half = lax.broadcasted_iota(jnp.int32, (UNIT, HEAD), 1) < HEAD // 2
    cos_s[...] = jnp.cos(angle)
    sin = jnp.sin(angle)
    sin_s[...] = jnp.where(first_half, -sin, sin)

    def norm(which, r):
        at = pl.ds(r * PIECE, PIECE)
        wide = xs[which, at, :].astype(F32)
        scale = lax.rsqrt(jnp.mean(wide * wide, -1, keepdims=True) + 1e-6)
        a_s[which, at, :] = (wide * scale * gain_ref[...].astype(F32).reshape(1, D)).astype(BF)

    with scope("norm"):
        for r in range(OWN // PIECE):
            norm(core, r)
    with scope("swap"):
        for r in range(OWN // PIECE):
            swap(1 - core, r).wait_recv()
            norm(1 - core, r)

    def turned(t):
        t = t.astype(F32)
        return (t * cos_s[...] + pltpu.roll(t, HEAD // 2, 1) * sin_s[...]).astype(BF)

    def block(b):
        return kv.at[core, b]

    def to_mate(j):
        l = mate(j)
        return remote(stage.at[l], block(4 * line + z), plane_send.at[j], block_recv.at[4 * line + z], in_plane(l))

    def arrived(b):
        remote(block(b), block(b), z_send.at[0, 0], block_recv.at[b], partner).wait_recv()

    STEPS = (1, -1, 2, -2, 3, -3)

    def direct(l):
        return (l == line) | (l == 0)

    def along_z(l, act):
        for i, step in enumerate(STEPS):
            b = 4 * l + z
            copy = remote(block(b), block(b), z_send.at[i, l], block_recv.at[b], me + 2 * step)
            there = z + step
            yes = (there >= 0) & (there < 4)
            if step < 0:
                yes = yes & (l < 3)
            if abs(step) == 3:
                yes = yes & direct(l)
            pl.when(yes)(lambda copy=copy: act(copy))

    def relay(l, act):
        up = remote(block(4 * l), block(4 * l), relay_send.at[l], block_recv.at[4 * l], me + 2)
        down = remote(block(4 * l + 3), block(4 * l + 3), relay_send.at[l], block_recv.at[4 * l + 3], me - 2)
        pl.when((z == 2) & ~direct(l))(lambda: act(up))
        pl.when((z == 1) & (l < 3) & ~direct(l))(lambda: act(down))

    def hand(b):
        return remote(block(b), block(b), hand_send.at[b], hand_recv.at[b], partner)

    start = lambda copy: copy.start()
    sent = lambda copy: copy.wait_send()

    with scope("kvw"):
        get_kv(wk_hbm).wait()
    t = _dot(a_s[...].reshape(UNIT, D), wkv[...]).astype(BF)
    for h in range(4):
        own = t[:, h * HEAD : (h + 1) * HEAD]
        stage[h] = jnp.where(core == 0, turned(own), own)
    for j in range(3):
        to_mate(j).start()
    kv[core, 4 * line + z] = stage[line]
    along_z(line, start)
    hand(4 * line + z).start()

    def q_copy(j):
        return remote(q_stage.at[j], qt.at[line], q_send.at[j], q_recv.at[line], in_plane(mate(j)))

    def project_q(j, _):
        get_q(j).wait()
        q = _dot(a_s[...].reshape(UNIT, D), wqs[lax.rem(j, 3)]).astype(BF)
        for n in range(4):
            q_stage[j, :, n * UNIT : (n + 1) * UNIT] = turned(q[:, n * HEAD : (n + 1) * HEAD]).T
        pl.when(j < 3)(lambda: q_copy(j).start())

        @pl.when(j == 0)
        def _():
            get_q(3).start()

        @pl.when(j == 2)
        def _():
            with scope("plane"):
                def take(l, _):
                    @pl.when(l != line)
                    def _():
                        arrived(4 * l + z)
                        along_z(l, start)
                        hand(4 * l + z).start()

                lax.fori_loop(0, 4, take, None)

    with scope("q_proj"):
        lax.fori_loop(0, 4, project_q, None)
    qt[line] = q_stage[3]
    for h in range(4):
        get_o(h).start()

    for n in range(4 * STRIPS):
        top_s[n] = jnp.full((1, STRIP), NEG, F32)
        mix_s[n] = jnp.zeros((HEAD + 8, STRIP), F32)

    def used(l, place):
        return (place != z) & ((l < 3) | (place < z))

    def take_z(l):
        with scope("take_z"):
            for place in (0, 3, 1, 2):
                @pl.when(used(l, place))
                def _():
                    arrived(4 * l + place)
                    if place == 0:
                        pl.when(z == 2)(lambda: relay(l, start))
                    if place == 3:
                        pl.when(z == 1)(lambda: relay(l, start))
                    hand(4 * l + place).start()

    def attend(l, g, masked):
        with scope("attend#m=%d" % masked):
            keys = kv[0, pl.ds(4 * g, 4)].reshape(LINE, HEAD)
            values = jnp.concatenate([vt[g], jnp.ones((8, LINE), BF)], 0)
            scores = [_dot(keys, qt[l, :, n * STRIP : (n + 1) * STRIP]) for n in range(STRIPS)]
            weights, keeps = [], []
            for n, s in enumerate(scores):
                if masked:
                    key = lax.broadcasted_iota(jnp.int32, s.shape, 0)
                    query = z * UNIT + lax.rem(lax.broadcasted_iota(jnp.int32, s.shape, 1), UNIT)
                    s = jnp.where(query >= key, s, HIDDEN)
                old = top_s[STRIPS * l + n]
                top = jnp.maximum(old, s.max(axis=0, keepdims=True))
                top_s[STRIPS * l + n] = top
                keeps.append(jnp.exp2((old - top) * E))
                weights.append(jnp.exp2((s - top) * E).astype(BF))
            for n, p in enumerate(weights):
                mix_s[STRIPS * l + n] = mix_s[STRIPS * l + n] * keeps[n] + _dot(values, p)

    def out_copy(l):
        return remote(o_stage.at[l], seen_s.at[line], out_send.at[l], out_recv.at[line], in_plane(l))

    def complete(l):
        with scope("complete"):
            per = STRIP // UNIT
            for n in range(STRIPS):
                out = (mix_s[STRIPS * l + n, :HEAD, :] * (1 / mix_s[STRIPS * l + n, HEAD : HEAD + 1, :])).astype(BF)
                for m in range(per):
                    h = per * n + m
                    o_stage[l, :, h * HEAD : (h + 1) * HEAD] = out[:, m * UNIT : (m + 1) * UNIT].T
            pl.when(l != line)(lambda: out_copy(l).start())

            @pl.when(l == line)
            def _():
                seen_s[line] = o_stage[l]

    def handed(g):
        with scope("hand_wait"):
            for place in range(4):
                @pl.when((g < 3) | (place <= z))
                def _():
                    b = 4 * g + place
                    remote(kv.at[1 - core, b], kv.at[1 - core, b], hand_send.at[b], hand_recv.at[b], partner).wait_recv()
        for i in range(4):
            vt[g, :, i * UNIT : (i + 1) * UNIT] = kv[1, 4 * g + i].T

    def q_wait(l):
        with scope("q_wait"):
            remote(qt.at[l], qt.at[l], q_send.at[0], q_recv.at[l], partner).wait_recv()

    def other(k):
        return jnp.where(line <= k, k + 1, k)

    across = mate(0)
    early = across > line
    take_z(line)
    handed(line)
    attend(line, line, True)

    @pl.when(early)
    def _():
        q_wait(across)
        attend(across, line, False)

    takes = (0, jnp.where((line == 0) | (line == 3), 1, 0), 4)
    needs = (jnp.where(line == 0, 1, 0), jnp.where((line == 0) | (line == 3), 2, 1), jnp.where(line == 2, 6, 5))

    def row(i, s):
        j = jnp.where((line == 0) & (i < 2), 1 - i, i)
        l = mate(j)
        pl.when((l != line) & ~((j == 0) & early))(lambda: q_wait(l))

        def meet(g, s):
            done = (g == line) & ((l == line) | (j == 0))

            @pl.when(~done)
            def _():
                for k in range(3):
                    pl.when(s == takes[k])(lambda k=k: take_z(other(k)))
                for k in range(3):
                    pl.when(s == needs[k])(lambda k=k: handed(other(k)))
                pl.when(l == g)(lambda: attend(l, g, True))
                pl.when(l > g)(lambda: attend(l, g, False))

            return jnp.where(done, s, s + 1)

        s = lax.fori_loop(0, l + 1, meet, s)
        complete(l)
        return s

    lax.fori_loop(0, 4, row, 0)

    def give(c):
        return remote(part_s.at[c, 1 - core], other_s.at[c], part_send.at[c], part_recv.at[c], partner)

    def product(c):
        at = pl.ds(pl.multiple_of(c * CHUNK, CHUNK), CHUNK)
        seen = jnp.concatenate([seen_s[h] for h in range(4)], 1)
        return _dot(seen, wos[:, :, at].reshape(2048, CHUNK)).reshape(2, OWN, CHUNK)

    def put(c):
        return pltpu.make_async_copy(y_s.at[c], y_hbm.at[:, pl.ds(pl.multiple_of(c * CHUNK, CHUNK), CHUNK)], y_sem.at[c])

    def finish(c):
        give(c).wait_recv()
        at = pl.ds(pl.multiple_of(c * CHUNK, CHUNK), CHUNK)
        y_s[c] = (xs[core, :, at].astype(F32) + (part_s[c, core] + other_s[c])).astype(BF)
        put(c).start()

    def seen_wait(l):
        with scope("seen_wait"):
            remote(seen_s.at[l], seen_s.at[l], out_send.at[0], out_recv.at[l], partner).wait_recv()

    for h in range(4):
        get_o(h).wait()
    for j in range(3):
        seen_wait(mate(j))

    def project_o(c, _):
        both = [product(2 * c + i) for i in range(2)]
        for i in range(2):
            part_s[2 * c + i] = both[i]
        for i in range(2):
            give(2 * c + i).start()

        @pl.when(c > 0)
        def _():
            finish(2 * c - 2)
            finish(2 * c - 1)

    with scope("o_proj"):
        lax.fori_loop(0, 4, project_o, None)
    with scope("finish"):
        finish(6)
        finish(7)

    for r in range(OWN // PIECE):
        swap(core, r).wait_send()
    for j in range(3):
        to_mate(j).wait_send()
        q_copy(j).wait_send()

    def drain(l, _):
        along_z(l, sent)
        relay(l, sent)
        pl.when(l != line)(lambda: out_copy(l).wait_send())
        for place in range(4):
            pl.when((l < 3) | (place <= z))(lambda place=place: hand(4 * l + place).wait_send())

    lax.fori_loop(0, 4, drain, None)

    def drain_chunk(c, _):
        give(c).wait_send()
        put(c).wait()

    lax.fori_loop(0, 8, drain_chunk, None)


def solution(mesh):
    def step(x, gain, wq, wk, wv, wo):
        half = HEAD // 2
        freq = THETA ** (-jnp.arange(half, dtype=F32) / half)
        freq = jnp.concatenate([freq, freq])[None]
        hbm, vmem = pl.BlockSpec(memory_space=pl.ANY), pl.BlockSpec(memory_space=pltpu.VMEM)
        dma = lambda *shape: pltpu.SemaphoreType.DMA(shape)
        return pl.pallas_call(
            kernel,
            out_shape=jax.ShapeDtypeStruct((OWN, D), BF),
            in_specs=[hbm, vmem, hbm, hbm, hbm, hbm, vmem],
            out_specs=hbm,
            scratch_shapes=[
                pltpu.VMEM((2, OWN, D), BF),
                pltpu.VMEM((2, OWN, D), BF),
                pltpu.VMEM((UNIT, HEAD), F32),
                pltpu.VMEM((UNIT, HEAD), F32),
                pltpu.VMEM((D, 512), BF),
                pltpu.VMEM((3, D, CHUNK), BF),
                pltpu.VMEM((4, CHUNK, D), BF),
                pltpu.VMEM((2, 16, UNIT, HEAD), BF),
                pltpu.VMEM((4, UNIT, HEAD), BF),
                pltpu.VMEM((4, HEAD, 4 * UNIT), BF),
                pltpu.VMEM((4, HEAD, 4 * UNIT), BF),
                pltpu.VMEM((4, HEAD, LINE), BF),
                pltpu.VMEM((4 * STRIPS, 1, STRIP), F32),
                pltpu.VMEM((4 * STRIPS, HEAD + 8, STRIP), F32),
                pltpu.VMEM((4, UNIT, 4 * HEAD), BF),
                pltpu.VMEM((4, UNIT, 4 * HEAD), BF),
                pltpu.VMEM((8, 2, OWN, CHUNK), F32),
                pltpu.VMEM((8, OWN, CHUNK), F32),
                pltpu.VMEM((8, OWN, CHUNK), BF),
                dma(OWN // PIECE), pltpu.SemaphoreType.DMA, dma(4), dma(4), dma(OWN // PIECE), dma(OWN // PIECE),
                dma(3), dma(16), dma(6, 4), dma(4), dma(16), dma(16),
                dma(3), dma(4), dma(4), dma(4), dma(8), dma(8), dma(8),
            ],
            compiler_params=pltpu.CompilerParams(collective_id=0, has_side_effects=True, vmem_limit_bytes=67043328),
        )(x, gain, wq, wk, wv, wo, freq)

    tokens, whole = P(("dp", "sp"), None), P(None, None)
    return jax.shard_map(
        step,
        mesh=mesh,
        in_specs=(tokens, P(None), whole, whole, whole, whole),
        out_specs=tokens,
        check_vma=False,
    )
```

```python
import jax
import jax.numpy as jnp
from jax import lax
from jax.experimental import pallas as pl
from jax.experimental.pallas import tpu as pltpu
from jax.sharding import PartitionSpec as P

scope = jax.named_scope
HEAD = 128
THETA = 10000
LOG2E = 1.4426950408889634
NEG = -1e30
HIDDEN = -2e30
D = 4096
OWN = 128
PIECE = 32
UNIT = 256
LINE = 4 * UNIT
CHUNK = 512
STRIP = 512
STRIPS = 4 * UNIT // STRIP
E = HEAD**-0.5 * LOG2E
BF, F32 = jnp.bfloat16, jnp.float32


def _dot(a, b):
    return lax.dot_general(a, b, (((1,), (0,)), ((), ())), preferred_element_type=F32)


def kernel(x_hbm, gain_ref, wq_hbm, wk_hbm, wv_hbm, wo_hbm, freq_ref, y_hbm,
           xs, a_s, cos_s, sin_s, wkv, wqs, wos, kv, stage, qt, q_stage, vt, top_s, mix_s, seen_s, o_stage, part_s, other_s, y_s,
           x_sem, k_sem, wq_sem, wo_sem, swap_send, swap_recv, plane_send, block_recv, z_send, relay_send, hand_send, hand_recv,
           q_send, q_recv, out_send, out_recv, part_send, part_recv, y_sem):
    me = lax.axis_index("sp")
    core, chip = lax.rem(me, 2), lax.div(me, 2)
    z, line = lax.rem(chip, 4), lax.div(chip, 4)
    y, x = lax.rem(line, 2), lax.div(line, 2)
    partner = me + 1 - 2 * core

    def in_plane(l):
        return me + (lax.div(l, 2) - x) * 16 + (lax.rem(l, 2) - y) * 8

    def mate(j):
        dx, dy = 1 - lax.div(j, 2), lax.rem(j + 1, 2)
        return lax.rem(x + dx, 2) * 2 + lax.rem(y + dy, 2)

    def get_x(r):
        at = pl.ds(r * PIECE, PIECE)
        return pltpu.make_async_copy(x_hbm.at[at], xs.at[core, at], x_sem.at[r])

    def get_kv(w):
        return pltpu.make_async_copy(w, wkv, k_sem)

    def get_q(j):
        at = pl.multiple_of(mate(j) * 1024 + core * 512, CHUNK)
        return pltpu.make_async_copy(wq_hbm.at[:, pl.ds(at, CHUNK)], wqs.at[lax.rem(j, 3)], wq_sem.at[j])

    def get_o(h):
        return pltpu.make_async_copy(wo_hbm.at[pl.ds(pl.multiple_of(h * 1024 + core * 512, CHUNK), CHUNK)], wos.at[h], wo_sem.at[h])

    for r in range(OWN // PIECE):
        get_x(r).start()
    pl.when(core == 0)(lambda: get_kv(wk_hbm).start())
    pl.when(core == 1)(lambda: get_kv(wv_hbm).start())

    kv[:, 12:] = jnp.zeros((2, 4, UNIT, HEAD), BF)

    barrier = pltpu.get_barrier_semaphore()

    def greet(device):
        pl.semaphore_signal(barrier, inc=1, device_id={"sp": device}, device_id_type=pl.DeviceIdType.MESH)

    greet(partner)
    for j in range(3):
        greet(in_plane(mate(j)))
    pl.when(z > 0)(lambda: greet(me - 2))
    pl.when(z < 3)(lambda: greet(me + 2))
    greet(jnp.where(z < 2, me + 4, me - 4))
    pl.when(z == 0)(lambda: greet(me + 6))
    pl.when(z == 3)(lambda: greet(me - 6))
    with scope("barrier"):
        pl.semaphore_wait(barrier, 7)

    def remote(src, dst, send, recv, device):
        return pltpu.make_async_remote_copy(src_ref=src, dst_ref=dst, send_sem=send, recv_sem=recv, device_id={"sp": device},
                                            device_id_type=pl.DeviceIdType.MESH)

    def swap(which, r):
        at = pl.ds(r * PIECE, PIECE)
        return remote(xs.at[which, at], xs.at[which, at], swap_send.at[r], swap_recv.at[r], partner)

    with scope("x_in"):
        for r in range(OWN // PIECE):
            get_x(r).wait()
            swap(core, r).start()
    for j in range(3):
        get_q(j).start()

    place = chip * UNIT + lax.broadcasted_iota(jnp.int32, (UNIT, HEAD), 0)
    angle = place.astype(F32) * freq_ref[...]
    first_half = lax.broadcasted_iota(jnp.int32, (UNIT, HEAD), 1) < HEAD // 2
    cos_s[...] = jnp.cos(angle)
    sin = jnp.sin(angle)
    sin_s[...] = jnp.where(first_half, -sin, sin)

    def norm(which, r):
        at = pl.ds(r * PIECE, PIECE)
        wide = xs[which, at, :].astype(F32)
        scale = lax.rsqrt(jnp.mean(wide * wide, -1, keepdims=True) + 1e-6)
        a_s[which, at, :] = (wide * scale * gain_ref[...].astype(F32).reshape(1, D)).astype(BF)

    with scope("norm"):
        for r in range(OWN // PIECE):
            norm(core, r)
    with scope("swap"):
        for r in range(OWN // PIECE):
            swap(1 - core, r).wait_recv()
            norm(1 - core, r)

    def turned(t):
        t = t.astype(F32)
        return (t * cos_s[...] + pltpu.roll(t, HEAD // 2, 1) * sin_s[...]).astype(BF)

    def block(b):
        return kv.at[core, b]

    def to_mate(j):
        l = mate(j)
        return remote(stage.at[l], block(4 * line + z), plane_send.at[j], block_recv.at[4 * line + z], in_plane(l))

    def arrived(b):
        remote(block(b), block(b), z_send.at[0, 0], block_recv.at[b], partner).wait_recv()

    STEPS = (3, -3, 2, -2, 1, -1)

    def direct(l):
        return (l == line) | (l == 0)

    def along_z(l, act):
        for i, step in enumerate(STEPS):
            b = 4 * l + z
            copy = remote(block(b), block(b), z_send.at[i, l], block_recv.at[b], me + 2 * step)
            there = z + step
            yes = (there >= 0) & (there < 4)
            if step < 0:
                yes = yes & (l < 3)
            if abs(step) == 3:
                yes = yes & direct(l)
            pl.when(yes)(lambda copy=copy: act(copy))

    def relay(l, act):
        up = remote(block(4 * l), block(4 * l), relay_send.at[l], block_recv.at[4 * l], me + 2)
        down = remote(block(4 * l + 3), block(4 * l + 3), relay_send.at[l], block_recv.at[4 * l + 3], me - 2)
        pl.when((z == 2) & ~direct(l))(lambda: act(up))
        pl.when((z == 1) & (l < 3) & ~direct(l))(lambda: act(down))

    def hand(b):
        return remote(block(b), block(b), hand_send.at[b], hand_recv.at[b], partner)

    start = lambda copy: copy.start()
    sent = lambda copy: copy.wait_send()

    with scope("kvw"):
        get_kv(wk_hbm).wait()
    t = _dot(a_s[...].reshape(UNIT, D), wkv[...]).astype(BF)
    for h in range(4):
        own = t[:, h * HEAD : (h + 1) * HEAD]
        stage[h] = jnp.where(core == 0, turned(own), own)
    for j in range(3):
        to_mate(j).start()
    kv[core, 4 * line + z] = stage[line]
    along_z(line, start)
    hand(4 * line + z).start()

    def q_copy(j):
        return remote(q_stage.at[j], qt.at[line], q_send.at[j], q_recv.at[line], in_plane(mate(j)))

    def project_q(j, _):
        get_q(j).wait()
        q = _dot(a_s[...].reshape(UNIT, D), wqs[lax.rem(j, 3)]).astype(BF)
        for n in range(4):
            q_stage[j, :, n * UNIT : (n + 1) * UNIT] = turned(q[:, n * HEAD : (n + 1) * HEAD]).T
        pl.when(j < 3)(lambda: q_copy(j).start())

        @pl.when(j == 0)
        def _():
            get_q(3).start()

        @pl.when(j == 2)
        def _():
            with scope("plane"):
                def take(l, _):
                    @pl.when(l != line)
                    def _():
                        arrived(4 * l + z)
                        along_z(l, start)
                        hand(4 * l + z).start()

                lax.fori_loop(0, 4, take, None)

    with scope("q_proj"):
        lax.fori_loop(0, 4, project_q, None)
    qt[line] = q_stage[3]
    for h in range(4):
        get_o(h).start()

    for n in range(4 * STRIPS):
        top_s[n] = jnp.full((1, STRIP), NEG, F32)
        mix_s[n] = jnp.zeros((HEAD + 8, STRIP), F32)

    def used(l, place):
        return (place != z) & ((l < 3) | (place < z))

    def relayed(l, place):
        return used(l, place) & ~direct(l) & ({0: z == 2, 3: z == 1}.get(place, z < 0))

    def take_relay(l):
        with scope("take_relay"):
            for place in (0, 3):
                @pl.when(relayed(l, place))
                def _():
                    arrived(4 * l + place)
                    relay(l, start)
                    hand(4 * l + place).start()

    def take_z(l):
        with scope("take_z"):
            for place in (0, 3, 1, 2):
                @pl.when(used(l, place) & ~relayed(l, place))
                def _():
                    arrived(4 * l + place)
                    hand(4 * l + place).start()

    def attend(l, g, masked):
        with scope("attend#m=%d" % masked):
            keys = kv[0, pl.ds(4 * g, 4)].reshape(LINE, HEAD)
            values = jnp.concatenate([vt[g], jnp.ones((8, LINE), BF)], 0)
            scores = [_dot(keys, qt[l, :, n * STRIP : (n + 1) * STRIP]) for n in range(STRIPS)]
            weights, keeps = [], []
            for n, s in enumerate(scores):
                if masked:
                    key = lax.broadcasted_iota(jnp.int32, s.shape, 0)
                    query = z * UNIT + lax.rem(lax.broadcasted_iota(jnp.int32, s.shape, 1), UNIT)
                    s = jnp.where(query >= key, s, HIDDEN)
                old = top_s[STRIPS * l + n]
                top = jnp.maximum(old, s.max(axis=0, keepdims=True))
                top_s[STRIPS * l + n] = top
                keeps.append(jnp.exp2((old - top) * E))
                weights.append(jnp.exp2((s - top) * E).astype(BF))
            for n, p in enumerate(weights):
                mix_s[STRIPS * l + n] = mix_s[STRIPS * l + n] * keeps[n] + _dot(values, p)

    def out_copy(l):
        return remote(o_stage.at[l], seen_s.at[line], out_send.at[l], out_recv.at[line], in_plane(l))

    def complete(l):
        with scope("complete"):
            per = STRIP // UNIT
            for n in range(STRIPS):
                out = (mix_s[STRIPS * l + n, :HEAD, :] * (1 / mix_s[STRIPS * l + n, HEAD : HEAD + 1, :])).astype(BF)
                for m in range(per):
                    h = per * n + m
                    o_stage[l, :, h * HEAD : (h + 1) * HEAD] = out[:, m * UNIT : (m + 1) * UNIT].T
            pl.when(l != line)(lambda: out_copy(l).start())

            @pl.when(l == line)
            def _():
                seen_s[line] = o_stage[l]

    def handed(g):
        with scope("hand_wait"):
            for place in range(4):
                @pl.when((g < 3) | (place <= z))
                def _():
                    b = 4 * g + place
                    remote(kv.at[1 - core, b], kv.at[1 - core, b], hand_send.at[b], hand_recv.at[b], partner).wait_recv()
        for i in range(4):
            vt[g, :, i * UNIT : (i + 1) * UNIT] = kv[1, 4 * g + i].T

    def q_wait(l):
        with scope("q_wait"):
            remote(qt.at[l], qt.at[l], q_send.at[0], q_recv.at[l], partner).wait_recv()

    def other(k):
        return jnp.where(line <= k, k + 1, k)

    across = mate(0)
    early = across > line
    take_z(line)
    handed(line)
    attend(line, line, True)

    @pl.when(early)
    def _():
        q_wait(across)
        attend(across, line, False)

    takes = (0, jnp.where(line == 3, 1, 0), jnp.where(line == 0, 1, 4))
    needs = (0, jnp.where(line == 3, 2, 1), jnp.where(line == 0, 2, 5))

    def row(i, s):
        j = jnp.where((line == 2) & (i > 0) & (i < 3), 3 - i, i)
        l = mate(j)
        pl.when((l != line) & ~((j == 0) & early))(lambda: q_wait(l))

        def meet(g, s):
            done = (g == line) & ((l == line) | (j == 0))

            @pl.when(~done)
            def _():
                @pl.when(s == 0)
                def _():
                    take_relay(other(0))
                    take_relay(other(1))

                pl.when(s == jnp.where(line == 0, 1, 2))(lambda: take_relay(other(2)))
                for k in range(3):
                    pl.when(s == takes[k])(lambda k=k: take_z(other(k)))
                for k in range(3):
                    pl.when(s == needs[k])(lambda k=k: handed(other(k)))
                pl.when(l == g)(lambda: attend(l, g, True))
                pl.when(l > g)(lambda: attend(l, g, False))

            return jnp.where(done, s, s + 1)

        s = lax.fori_loop(0, l + 1, meet, s)
        complete(l)
        return s

    lax.fori_loop(0, 4, row, 0)

    def give(c):
        return remote(part_s.at[c, 1 - core], other_s.at[c], part_send.at[c], part_recv.at[c], partner)

    def product(c, hs):
        at = pl.ds(pl.multiple_of(c * CHUNK, CHUNK), CHUNK)
        seen = jnp.concatenate([seen_s[h] for h in hs], 1)
        return _dot(seen, jnp.concatenate([wos[h, :, at] for h in hs], 0)).reshape(2, OWN, CHUNK)

    def put(c):
        return pltpu.make_async_copy(y_s.at[c], y_hbm.at[:, pl.ds(pl.multiple_of(c * CHUNK, CHUNK), CHUNK)], y_sem.at[c])

    def finish(c):
        give(c).wait_recv()
        at = pl.ds(pl.multiple_of(c * CHUNK, CHUNK), CHUNK)
        y_s[c] = (xs[core, :, at].astype(F32) + (part_s[c, core] + other_s[c])).astype(BF)
        put(c).start()

    def seen_wait(l):
        with scope("seen_wait"):
            remote(seen_s.at[l], seen_s.at[l], out_send.at[0], out_recv.at[l], partner).wait_recv()

    for h in range(4):
        get_o(h).wait()
    seen_wait(mate(0))

    def project_early(c, _):
        both = [product(2 * c + i, (line, mate(0))) for i in range(2)]
        for i in range(2):
            part_s[2 * c + i] = both[i]

    with scope("o_early"):
        lax.fori_loop(0, 4, project_early, None)
    seen_wait(mate(1))
    seen_wait(mate(2))

    def project_late(c, _):
        both = [part_s[2 * c + i] + product(2 * c + i, (mate(1), mate(2))) for i in range(2)]
        for i in range(2):
            part_s[2 * c + i] = both[i]
        for i in range(2):
            give(2 * c + i).start()

        @pl.when(c > 1)
        def _():
            finish(2 * c - 4)
            finish(2 * c - 3)

    with scope("o_late"):
        lax.fori_loop(0, 4, project_late, None)
    with scope("finish"):
        for c in range(4, 8):
            finish(c)

    for r in range(OWN // PIECE):
        swap(core, r).wait_send()
    for j in range(3):
        to_mate(j).wait_send()
        q_copy(j).wait_send()

    def drain(l, _):
        along_z(l, sent)
        relay(l, sent)
        pl.when(l != line)(lambda: out_copy(l).wait_send())
        for place in range(4):
            pl.when((l < 3) | (place <= z))(lambda place=place: hand(4 * l + place).wait_send())

    lax.fori_loop(0, 4, drain, None)

    def drain_chunk(c, _):
        give(c).wait_send()
        put(c).wait()

    lax.fori_loop(0, 8, drain_chunk, None)


def solution(mesh):
    def step(x, gain, wq, wk, wv, wo):
        half = HEAD // 2
        freq = THETA ** (-jnp.arange(half, dtype=F32) / half)
        freq = jnp.concatenate([freq, freq])[None]
        hbm, vmem = pl.BlockSpec(memory_space=pl.ANY), pl.BlockSpec(memory_space=pltpu.VMEM)
        dma = lambda *shape: pltpu.SemaphoreType.DMA(shape)
        return pl.pallas_call(
            kernel,
            out_shape=jax.ShapeDtypeStruct((OWN, D), BF),
            in_specs=[hbm, vmem, hbm, hbm, hbm, hbm, vmem],
            out_specs=hbm,
            scratch_shapes=[
                pltpu.VMEM((2, OWN, D), BF),
                pltpu.VMEM((2, OWN, D), BF),
                pltpu.VMEM((UNIT, HEAD), F32),
                pltpu.VMEM((UNIT, HEAD), F32),
                pltpu.VMEM((D, 512), BF),
                pltpu.VMEM((3, D, CHUNK), BF),
                pltpu.VMEM((4, CHUNK, D), BF),
                pltpu.VMEM((2, 16, UNIT, HEAD), BF),
                pltpu.VMEM((4, UNIT, HEAD), BF),
                pltpu.VMEM((4, HEAD, 4 * UNIT), BF),
                pltpu.VMEM((4, HEAD, 4 * UNIT), BF),
                pltpu.VMEM((4, HEAD, LINE), BF),
                pltpu.VMEM((4 * STRIPS, 1, STRIP), F32),
                pltpu.VMEM((4 * STRIPS, HEAD + 8, STRIP), F32),
                pltpu.VMEM((4, UNIT, 4 * HEAD), BF),
                pltpu.VMEM((4, UNIT, 4 * HEAD), BF),
                pltpu.VMEM((8, 2, OWN, CHUNK), F32),
                pltpu.VMEM((8, OWN, CHUNK), F32),
                pltpu.VMEM((8, OWN, CHUNK), BF),
                dma(OWN // PIECE), pltpu.SemaphoreType.DMA, dma(4), dma(4), dma(OWN // PIECE), dma(OWN // PIECE),
                dma(3), dma(16), dma(6, 4), dma(4), dma(16), dma(16),
                dma(3), dma(4), dma(4), dma(4), dma(8), dma(8), dma(8),
            ],
            compiler_params=pltpu.CompilerParams(collective_id=0, has_side_effects=True, vmem_limit_bytes=67043328),
        )(x, gain, wq, wk, wv, wo, freq)

    tokens, whole = P(("dp", "sp"), None), P(None, None)
    return jax.shard_map(
        step,
        mesh=mesh,
        in_specs=(tokens, P(None), whole, whole, whole, whole),
        out_specs=tokens,
        check_vma=False,
    )
```

```python
import jax
import jax.numpy as jnp
from jax import lax
from jax.experimental import pallas as pl
from jax.experimental.pallas import tpu as pltpu
from jax.sharding import PartitionSpec as P

scope = jax.named_scope
HEAD = 128
THETA = 10000
LOG2E = 1.4426950408889634
NEG = -1e30
HIDDEN = -2e30
D = 4096
OWN = 128
PIECE = 32
UNIT = 256
LINE = 4 * UNIT
CHUNK = 512
STRIP = 512
E = HEAD**-0.5 * LOG2E
BF, F32 = jnp.bfloat16, jnp.float32


def _dot(a, b):
    return lax.dot_general(a, b, (((1,), (0,)), ((), ())), preferred_element_type=F32)


def kernel(x_hbm, gain_ref, wq_hbm, wk_hbm, wv_hbm, wo_hbm, freq_ref, y_hbm,
           xs, a_s, cos_s, sin_s, wkv, wqs, wos, kv, stage, qt, q_stage, vt, top_a, top_b, mix_a, mix_b, s_a, s_b, m_a, m_b, p_a, p_b, k_a, k_b, seen_s, o_stage, part_s, other_s,
           x_sem, k_sem, wq_sem, wo_sem, swap_send, swap_recv, plane_send, block_recv, z_send, relay_send, hand_send, hand_recv,
           q_send, q_recv, out_send, out_recv, part_send, part_recv, y_sem):
    me = lax.axis_index("sp")
    core, chip = lax.rem(me, 2), lax.div(me, 2)
    z, line = lax.rem(chip, 4), lax.div(chip, 4)
    y, x = lax.rem(line, 2), lax.div(line, 2)
    partner = me + 1 - 2 * core

    def in_plane(l):
        return me + (lax.div(l, 2) - x) * 16 + (lax.rem(l, 2) - y) * 8

    def mate(j):
        dx, dy = 1 - lax.div(j, 2), lax.rem(j + 1, 2)
        return lax.rem(x + dx, 2) * 2 + lax.rem(y + dy, 2)

    def get_x(r):
        at = pl.ds(r * PIECE, PIECE)
        return pltpu.make_async_copy(x_hbm.at[at], xs.at[core, at], x_sem.at[r])

    def get_kv(w):
        return pltpu.make_async_copy(w, wkv, k_sem)

    def get_q(j):
        at = pl.multiple_of(mate(j) * 1024 + core * 512, CHUNK)
        return pltpu.make_async_copy(wq_hbm.at[:, pl.ds(at, CHUNK)], wqs.at[lax.rem(j, 3)], wq_sem.at[j])

    def get_o(h):
        return pltpu.make_async_copy(wo_hbm.at[pl.ds(pl.multiple_of(h * 1024 + core * 512, CHUNK), CHUNK)], wos.at[h], wo_sem.at[h])

    for r in range(OWN // PIECE):
        get_x(r).start()
    pl.when(core == 0)(lambda: get_kv(wk_hbm).start())
    pl.when(core == 1)(lambda: get_kv(wv_hbm).start())

    kv[:, 12:] = jnp.zeros((2, 4, UNIT, HEAD), BF)

    barrier = pltpu.get_barrier_semaphore()

    def greet(device):
        pl.semaphore_signal(barrier, inc=1, device_id={"sp": device}, device_id_type=pl.DeviceIdType.MESH)

    greet(partner)
    for j in range(3):
        greet(in_plane(mate(j)))
    pl.when(z > 0)(lambda: greet(me - 2))
    pl.when(z < 3)(lambda: greet(me + 2))
    greet(jnp.where(z < 2, me + 4, me - 4))
    pl.when(z == 0)(lambda: greet(me + 6))
    pl.when(z == 3)(lambda: greet(me - 6))
    with scope("barrier"):
        pl.semaphore_wait(barrier, 7)

    def remote(src, dst, send, recv, device):
        return pltpu.make_async_remote_copy(src_ref=src, dst_ref=dst, send_sem=send, recv_sem=recv, device_id={"sp": device},
                                            device_id_type=pl.DeviceIdType.MESH)

    def swap(which, r):
        at = pl.ds(r * PIECE, PIECE)
        return remote(xs.at[which, at], xs.at[which, at], swap_send.at[r], swap_recv.at[r], partner)

    with scope("x_in"):
        for r in range(OWN // PIECE):
            get_x(r).wait()
            swap(core, r).start()
    for j in range(3):
        get_q(j).start()

    place = chip * UNIT + lax.broadcasted_iota(jnp.int32, (UNIT, HEAD), 0)
    angle = place.astype(F32) * freq_ref[...]
    first_half = lax.broadcasted_iota(jnp.int32, (UNIT, HEAD), 1) < HEAD // 2
    cos_s[...] = jnp.cos(angle)
    sin = jnp.sin(angle)
    sin_s[...] = jnp.where(first_half, -sin, sin)

    def norm(which, r):
        at = pl.ds(r * PIECE, PIECE)
        wide = xs[which, at, :].astype(F32)
        scale = lax.rsqrt(jnp.mean(wide * wide, -1, keepdims=True) + 1e-6)
        a_s[which, at, :] = (wide * scale * gain_ref[...].astype(F32).reshape(1, D)).astype(BF)

    with scope("norm"):
        for r in range(OWN // PIECE):
            norm(core, r)
    with scope("swap"):
        for r in range(OWN // PIECE):
            swap(1 - core, r).wait_recv()
            norm(1 - core, r)

    def turned(t):
        t = t.astype(F32)
        return (t * cos_s[...] + pltpu.roll(t, HEAD // 2, 1) * sin_s[...]).astype(BF)

    def block(b):
        return kv.at[core, b]

    def to_mate(j):
        l = mate(j)
        return remote(stage.at[l], block(4 * line + z), plane_send.at[j], block_recv.at[4 * line + z], in_plane(l))

    def arrived(b):
        remote(block(b), block(b), z_send.at[0, 0], block_recv.at[b], partner).wait_recv()

    STEPS = (3, -3, 2, -2, 1, -1)

    def direct(l):
        return (l == line) | (l == 0)

    def along_z(l, act):
        for i, step in enumerate(STEPS):
            b = 4 * l + z
            copy = remote(block(b), block(b), z_send.at[i, l], block_recv.at[b], me + 2 * step)
            there = z + step
            yes = (there >= 0) & (there < 4)
            if step < 0:
                yes = yes & (l < 3)
            if abs(step) == 3:
                yes = yes & direct(l)
            pl.when(yes)(lambda copy=copy: act(copy))

    def relay(l, act):
        up = remote(block(4 * l), block(4 * l), relay_send.at[l], block_recv.at[4 * l], me + 2)
        down = remote(block(4 * l + 3), block(4 * l + 3), relay_send.at[l], block_recv.at[4 * l + 3], me - 2)
        pl.when((z == 2) & ~direct(l))(lambda: act(up))
        pl.when((z == 1) & (l < 3) & ~direct(l))(lambda: act(down))

    def hand(b):
        return remote(block(b), block(b), hand_send.at[b], hand_recv.at[b], partner)

    start = lambda copy: copy.start()
    sent = lambda copy: copy.wait_send()

    with scope("kvw"):
        get_kv(wk_hbm).wait()
    t = _dot(a_s[...].reshape(UNIT, D), wkv[...]).astype(BF)
    for h in range(4):
        own = t[:, h * HEAD : (h + 1) * HEAD]
        stage[h] = jnp.where(core == 0, turned(own), own)
    for j in range(3):
        to_mate(j).start()
    kv[core, 4 * line + z] = stage[line]
    along_z(line, start)
    hand(4 * line + z).start()

    def q_copy(j):
        return remote(q_stage.at[j], qt.at[line], q_send.at[j], q_recv.at[line], in_plane(mate(j)))

    def project_q(j, _):
        get_q(j).wait()
        q = _dot(a_s[...].reshape(UNIT, D), wqs[lax.rem(j, 3)]).astype(BF)
        for n in range(4):
            q_stage[j, :, n * UNIT : (n + 1) * UNIT] = turned(q[:, n * HEAD : (n + 1) * HEAD]).T
        pl.when(j < 3)(lambda: q_copy(j).start())

        @pl.when(j == 0)
        def _():
            get_q(3).start()

        @pl.when(j == 2)
        def _():
            with scope("plane"):
                def take(l, _):
                    @pl.when(l != line)
                    def _():
                        arrived(4 * l + z)
                        along_z(l, start)
                        hand(4 * l + z).start()

                lax.fori_loop(0, 4, take, None)

    with scope("q_proj"):
        lax.fori_loop(0, 4, project_q, None)
    qt[line] = q_stage[3]
    for h in range(4):
        get_o(h).start()

    top_s, mix_s, score_s, most_s, weight_s, keep_s = (top_a, top_b), (mix_a, mix_b), (s_a, s_b), (m_a, m_b), (p_a, p_b), (k_a, k_b)
    for n in range(2):
        top_s[n][...] = jnp.full((4, 1, STRIP), NEG, F32)
        mix_s[n][...] = jnp.zeros((4, HEAD + 8, STRIP), F32)

    def used(l, place):
        return (place != z) & ((l < 3) | (place < z))

    def relayed(l, place):
        return used(l, place) & ~direct(l) & ({0: z == 2, 3: z == 1}.get(place, z < 0))

    def take_relay(l):
        with scope("take_relay"):
            for place in (0, 3):
                @pl.when(relayed(l, place))
                def _():
                    arrived(4 * l + place)
                    relay(l, start)
                    hand(4 * l + place).start()

    def take_z(l):
        with scope("take_z"):
            for place in (0, 3, 1, 2):
                @pl.when(used(l, place) & ~relayed(l, place))
                def _():
                    arrived(4 * l + place)
                    hand(4 * l + place).start()

    def scores(l, g, n, masked):
        t = _dot(kv[0, pl.ds(4 * g, 4)].reshape(LINE, HEAD), qt[l, :, n * STRIP : (n + 1) * STRIP])
        if masked:
            key = lax.broadcasted_iota(jnp.int32, t.shape, 0)
            query = z * UNIT + lax.rem(lax.broadcasted_iota(jnp.int32, t.shape, 1), UNIT)
            t = jnp.where(query >= key, t, HIDDEN)
        score_s[n][...] = t
        most_s[n][...] = t.max(axis=0, keepdims=True)

    def weights(l, n):
        old = top_s[n][l]
        top = jnp.maximum(old, most_s[n][...])
        top_s[n][l] = top
        keep_s[n][...] = jnp.exp2((old - top) * E)
        weight_s[n][...] = jnp.exp2((score_s[n][...] - top) * E).astype(BF)

    def values(l, g, n):
        v = jnp.concatenate([vt[g], jnp.ones((8, LINE), BF)], 0)
        mix_s[n][l] = mix_s[n][l] * keep_s[n][...] + _dot(v, weight_s[n][...])

    def attend(l, g, masked):
        with scope("attend_alone"):
            for n in range(2):
                scores(l, g, n, masked)
            for n in range(2):
                weights(l, n)
            for n in range(2):
                values(l, g, n)

    def attend_next(l, g, masked, l0, g0):
        with scope("attend#m=%d" % masked):
            scores(l, g, 0, masked)
            weights(l0, 1)
            values(l0, g0, 0)
            scores(l, g, 1, masked)
            weights(l, 0)
            values(l0, g0, 1)

    def out_copy(l):
        return remote(o_stage.at[l], seen_s.at[line], out_send.at[l], out_recv.at[line], in_plane(l))

    def complete(l):
        with scope("complete"):
            for n in range(2):
                out = (mix_s[n][l, :HEAD, :] * (1 / mix_s[n][l, HEAD : HEAD + 1, :])).astype(BF)
                for m in range(2):
                    h = 2 * n + m
                    o_stage[l, :, h * HEAD : (h + 1) * HEAD] = out[:, m * UNIT : (m + 1) * UNIT].T
            pl.when(l != line)(lambda: out_copy(l).start())

            @pl.when(l == line)
            def _():
                seen_s[line] = o_stage[l]

    def handed(g):
        with scope("hand_wait"):
            for place in range(4):
                @pl.when((g < 3) | (place <= z))
                def _():
                    b = 4 * g + place
                    remote(kv.at[1 - core, b], kv.at[1 - core, b], hand_send.at[b], hand_recv.at[b], partner).wait_recv()
        for i in range(4):
            vt[g, :, i * UNIT : (i + 1) * UNIT] = kv[1, 4 * g + i].T

    def q_wait(l):
        with scope("q_wait"):
            remote(qt.at[l], qt.at[l], q_send.at[0], q_recv.at[l], partner).wait_recv()

    def other(k):
        return jnp.where(line <= k, k + 1, k)

    across = mate(0)
    early = across > line
    take_z(line)
    handed(line)
    attend(line, line, True)

    @pl.when(early)
    def _():
        q_wait(across)
        attend(across, line, False)

    take_relay(other(0))
    take_relay(other(1))

    @pl.when(line == 0)
    def _():
        complete(line)
        q_wait(mate(1))
        attend(mate(1), line, False)

    weight_s[0][...] = jnp.zeros((LINE, STRIP), BF)
    keep_s[0][...] = jnp.ones((1, STRIP), F32)
    score_s[1][...] = jnp.full((LINE, STRIP), HIDDEN, F32)
    most_s[1][...] = jnp.full((1, STRIP), NEG, F32)

    takes = (0, jnp.where(line == 3, 1, 0), jnp.where(line == 0, 1, 4))
    needs = (0, jnp.where(line == 3, 2, 1), jnp.where(line == 0, 2, 5))

    def row(i, carry):
        j = jnp.where((line == 2) & (i > 0) & (i < 3), 3 - i, i)
        l = mate(j)
        met = (j == 0) & early | (line == 0) & (j == 1)
        pl.when((l != line) & ~met)(lambda: q_wait(l))

        def meet(g, carry):
            s, l0, g0 = carry
            done = (g == line) & ((l == line) | met)

            @pl.when(~done)
            def _():
                pl.when(s == jnp.where(line == 0, 0, 2))(lambda: take_relay(other(2)))
                for k in range(3):
                    pl.when(s == takes[k])(lambda k=k: take_z(other(k)))
                for k in range(3):
                    pl.when(s == needs[k])(lambda k=k: handed(other(k)))
                pl.when(l == g)(lambda: attend_next(l, g, True, l0, g0))
                pl.when(l > g)(lambda: attend_next(l, g, False, l0, g0))
                pl.when((s > 0) & (l0 != l))(lambda: complete(l0))

            return jnp.where(done, s, s + 1), jnp.where(done, l0, l), jnp.where(done, g0, g)

        return lax.fori_loop(0, l + 1, meet, carry)

    _, last, g0 = lax.fori_loop(0, 4, row, (0, line, line))
    with scope("attend_last"):
        weights(last, 1)
        for n in range(2):
            values(last, g0, n)
    complete(last)

    def give(c):
        return remote(part_s.at[c, 1 - core], other_s.at[c], part_send.at[c], part_recv.at[c], partner)

    def product(c, hs):
        at = pl.ds(pl.multiple_of(c * CHUNK, CHUNK), CHUNK)
        seen = jnp.concatenate([seen_s[h] for h in hs], 1)
        return _dot(seen, jnp.concatenate([wos[h, :, at] for h in hs], 0)).reshape(2, OWN, CHUNK)

    def put(c):
        at = pl.ds(pl.multiple_of(c * CHUNK, CHUNK), CHUNK)
        return pltpu.make_async_copy(a_s.at[0, :, at], y_hbm.at[:, at], y_sem.at[c])

    def finish(c):
        give(c).wait_recv()
        at = pl.ds(pl.multiple_of(c * CHUNK, CHUNK), CHUNK)
        a_s[0, :, at] = (xs[core, :, at].astype(F32) + (part_s[c, core] + other_s[c])).astype(BF)
        put(c).start()

    def seen_wait(l):
        with scope("seen_wait"):
            remote(seen_s.at[l], seen_s.at[l], out_send.at[0], out_recv.at[l], partner).wait_recv()

    for h in range(4):
        get_o(h).wait()
    seen_wait(mate(0))

    def project_early(c, _):
        both = [product(2 * c + i, (line, mate(0))) for i in range(2)]
        for i in range(2):
            part_s[2 * c + i] = both[i]

    with scope("o_early"):
        lax.fori_loop(0, 4, project_early, None)
    seen_wait(mate(1))
    seen_wait(mate(2))

    def project_late(c, _):
        both = [part_s[2 * c + i] + product(2 * c + i, (mate(1), mate(2))) for i in range(2)]
        for i in range(2):
            part_s[2 * c + i] = both[i]
        for i in range(2):
            give(2 * c + i).start()

        @pl.when(c > 1)
        def _():
            finish(2 * c - 4)
            finish(2 * c - 3)

    with scope("o_late"):
        lax.fori_loop(0, 4, project_late, None)
    with scope("finish"):
        for c in range(4, 8):
            finish(c)

    for r in range(OWN // PIECE):
        swap(core, r).wait_send()
    for j in range(3):
        to_mate(j).wait_send()
        q_copy(j).wait_send()

    def drain(l, _):
        along_z(l, sent)
        relay(l, sent)
        pl.when(l != line)(lambda: out_copy(l).wait_send())
        for place in range(4):
            pl.when((l < 3) | (place <= z))(lambda place=place: hand(4 * l + place).wait_send())

    lax.fori_loop(0, 4, drain, None)

    def drain_chunk(c, _):
        give(c).wait_send()
        put(c).wait()

    lax.fori_loop(0, 8, drain_chunk, None)


def solution(mesh):
    def step(x, gain, wq, wk, wv, wo):
        half = HEAD // 2
        freq = THETA ** (-jnp.arange(half, dtype=F32) / half)
        freq = jnp.concatenate([freq, freq])[None]
        hbm, vmem = pl.BlockSpec(memory_space=pl.ANY), pl.BlockSpec(memory_space=pltpu.VMEM)
        dma = lambda *shape: pltpu.SemaphoreType.DMA(shape)
        return pl.pallas_call(
            kernel,
            out_shape=jax.ShapeDtypeStruct((OWN, D), BF),
            in_specs=[hbm, vmem, hbm, hbm, hbm, hbm, vmem],
            out_specs=hbm,
            scratch_shapes=[
                pltpu.VMEM((2, OWN, D), BF),
                pltpu.VMEM((2, OWN, D), BF),
                pltpu.VMEM((UNIT, HEAD), F32),
                pltpu.VMEM((UNIT, HEAD), F32),
                pltpu.VMEM((D, 512), BF),
                pltpu.VMEM((3, D, CHUNK), BF),
                pltpu.VMEM((4, CHUNK, D), BF),
                pltpu.VMEM((2, 16, UNIT, HEAD), BF),
                pltpu.VMEM((4, UNIT, HEAD), BF),
                pltpu.VMEM((4, HEAD, 4 * UNIT), BF),
                pltpu.VMEM((4, HEAD, 4 * UNIT), BF),
                pltpu.VMEM((4, HEAD, LINE), BF),
                *[pltpu.VMEM((4, 1, STRIP), F32)] * 2,
                *[pltpu.VMEM((4, HEAD + 8, STRIP), F32)] * 2,
                *[pltpu.VMEM((LINE, STRIP), F32)] * 2,
                *[pltpu.VMEM((1, STRIP), F32)] * 2,
                *[pltpu.VMEM((LINE, STRIP), BF)] * 2,
                *[pltpu.VMEM((1, STRIP), F32)] * 2,
                pltpu.VMEM((4, UNIT, 4 * HEAD), BF),
                pltpu.VMEM((4, UNIT, 4 * HEAD), BF),
                pltpu.VMEM((8, 2, OWN, CHUNK), F32),
                pltpu.VMEM((8, OWN, CHUNK), F32),
                dma(OWN // PIECE), pltpu.SemaphoreType.DMA, dma(4), dma(4), dma(OWN // PIECE), dma(OWN // PIECE),
                dma(3), dma(16), dma(6, 4), dma(4), dma(16), dma(16),
                dma(3), dma(4), dma(4), dma(4), dma(8), dma(8), dma(8),
            ],
            compiler_params=pltpu.CompilerParams(collective_id=0, has_side_effects=True, vmem_limit_bytes=67043328),
        )(x, gain, wq, wk, wv, wo, freq)

    tokens, whole = P(("dp", "sp"), None), P(None, None)
    return jax.shard_map(
        step,
        mesh=mesh,
        in_specs=(tokens, P(None), whole, whole, whole, whole),
        out_specs=tokens,
        check_vma=False,
    )
```

```python
import jax
import jax.numpy as jnp
from jax import lax
from jax.experimental import pallas as pl
from jax.experimental.pallas import tpu as pltpu
from jax.sharding import PartitionSpec as P

scope = jax.named_scope
HEAD = 128
LOG2_THETA = 13.287712379549449
LOG2E = 1.4426950408889634
NEG = -1e30
HIDDEN = -2e30
D = 4096
OWN = 128
PIECE = 32
UNIT = 256
LINE = 4 * UNIT
CHUNK = 512
STRIP = 512
E = HEAD**-0.5 * LOG2E
BF, F32 = jnp.bfloat16, jnp.float32


def _dot(a, b):
    return lax.dot_general(a, b, (((1,), (0,)), ((), ())), preferred_element_type=F32)


def kernel(x_hbm, gain_hbm, wq_hbm, wk_hbm, wv_hbm, wo_hbm, y_hbm,
           xs, gain_s, a_s, cos_s, sin_s, wks, wqs, wos, kv, stage, qt, q_stage, vt, top_a, top_b, mix_a, mix_b, s_a, s_b, m_a, m_b, p_a, p_b, k_a, k_b, seen_s, o_stage, part_s, other_s,
           x_sem, gain_sem, k_sem, wq_sem, wo_sem, swap_send, swap_recv, plane_send, block_recv, z_send, relay_send, hand_send, hand_recv,
           q_send, q_recv, out_send, out_recv, part_send, part_recv, y_sem):
    me = lax.axis_index("sp")
    core, chip = lax.rem(me, 2), lax.div(me, 2)
    z, line = lax.rem(chip, 4), lax.div(chip, 4)
    y, x = lax.rem(line, 2), lax.div(line, 2)
    partner = me + 1 - 2 * core

    def in_plane(l):
        return me + (lax.div(l, 2) - x) * 16 + (lax.rem(l, 2) - y) * 8

    def mate(j):
        dx, dy = 1 - lax.div(j, 2), lax.rem(j + 1, 2)
        return lax.rem(x + dx, 2) * 2 + lax.rem(y + dy, 2)

    def get_x(r):
        at = pl.ds(r * PIECE, PIECE)
        return pltpu.make_async_copy(x_hbm.at[at], xs.at[core, at], x_sem.at[r])

    get_k = pltpu.make_async_copy(wk_hbm, wks, k_sem.at[0])
    get_v = pltpu.make_async_copy(wv_hbm, wqs.at[2], k_sem.at[1])

    def get_q(j):
        at = pl.multiple_of(mate(j) * 1024 + core * 512, CHUNK)
        return pltpu.make_async_copy(wq_hbm.at[:, pl.ds(at, CHUNK)], wqs.at[lax.rem(j, 3)], wq_sem.at[j])

    def get_o(h):
        return pltpu.make_async_copy(wo_hbm.at[pl.ds(pl.multiple_of(h * 1024 + core * 512, CHUNK), CHUNK)], wos.at[h], wo_sem.at[h])

    get_gain = pltpu.make_async_copy(gain_hbm, gain_s, gain_sem.at[0])
    get_x(0).start()
    get_gain.start()
    for r in range(1, OWN // PIECE):
        get_x(r).start()

    kv[:, 12:] = jnp.zeros((2, 4, 2, OWN, HEAD), BF)

    barrier = pltpu.get_barrier_semaphore()

    def greet(device):
        pl.semaphore_signal(barrier, inc=1, device_id={"sp": device}, device_id_type=pl.DeviceIdType.MESH)

    greet(partner)
    for j in range(3):
        greet(in_plane(mate(j)))
    pl.when(z > 0)(lambda: greet(me - 2))
    pl.when(z < 3)(lambda: greet(me + 2))
    greet(jnp.where(z < 2, me + 4, me - 4))
    pl.when(z == 0)(lambda: greet(me + 6))
    pl.when(z == 3)(lambda: greet(me - 6))
    def remote(src, dst, send, recv, device):
        return pltpu.make_async_remote_copy(src_ref=src, dst_ref=dst, send_sem=send, recv_sem=recv, device_id={"sp": device},
                                            device_id_type=pl.DeviceIdType.MESH)

    def swap(which, r):
        at = pl.ds(r * PIECE, PIECE)
        return remote(xs.at[which, at], xs.at[which, at], swap_send.at[r], swap_recv.at[r], partner)

    def norm(which, r):
        at = pl.ds(r * PIECE, PIECE)
        wide = xs[which, at, :].astype(F32)
        scale = lax.rsqrt(jnp.mean(wide * wide, -1, keepdims=True) + 1e-6)
        a_s[which, at, :] = (wide * scale * gain_s[...].astype(F32).reshape(1, D)).astype(BF)

    with scope("x_in"):
        for r in range(OWN // PIECE):
            get_x(r).wait()
            if r == 0:
                get_k.start()
                get_v.start()
                get_gain.wait()
            norm(core, r)
    with scope("barrier"):
        pl.semaphore_wait(barrier, 7)
    for r in range(OWN // PIECE):
        swap(core, r).start()

    def turned(t, cos, sin):
        t = t.astype(F32)
        return (t * cos + pltpu.roll(t, HEAD // 2, 1) * sin).astype(BF)

    def block(b):
        return kv.at[core, b]

    def to_mate(j):
        l = mate(j)
        return remote(stage.at[l], block(4 * line + z), plane_send.at[j], block_recv.at[4 * line + z], in_plane(l))

    def arrived(b):
        remote(block(b), block(b), z_send.at[0, 0], block_recv.at[b], partner).wait_recv()

    STEPS = (3, -3, 2, -2, 1, -1)

    def direct(l):
        return (l == line) | (l == 0)

    def along_z(l, act):
        for i, step in enumerate(STEPS):
            b = 4 * l + z
            copy = remote(block(b), block(b), z_send.at[i, l], block_recv.at[b], me + 2 * step)
            there = z + step
            yes = (there >= 0) & (there < 4)
            if step < 0:
                yes = yes & (l < 3)
            if abs(step) == 3:
                yes = yes & direct(l)
            pl.when(yes)(lambda copy=copy: act(copy))

    def relay(l, act):
        up = remote(block(4 * l), block(4 * l), relay_send.at[l], block_recv.at[4 * l], me + 2)
        down = remote(block(4 * l + 3), block(4 * l + 3), relay_send.at[l], block_recv.at[4 * l + 3], me - 2)
        pl.when((z == 2) & ~direct(l))(lambda: act(up))
        pl.when((z == 1) & (l < 3) & ~direct(l))(lambda: act(down))

    def hand(b):
        return remote(block(b), block(b), hand_send.at[b], hand_recv.at[b], partner)

    start = lambda copy: copy.start()
    sent = lambda copy: copy.wait_send()

    place = chip * UNIT + lax.broadcasted_iota(jnp.int32, (UNIT, HEAD), 0)
    element = lax.broadcasted_iota(jnp.int32, (1, HEAD), 1)
    freq = jnp.exp2(lax.rem(element, HEAD // 2).astype(F32) * (-LOG2_THETA * 2 / HEAD))
    angle = place.astype(F32) * freq
    sin = jnp.sin(angle)
    cos_s[...] = jnp.cos(angle)
    sin_s[...] = jnp.where(element < HEAD // 2, -sin, sin)
    with scope("kw"):
        get_k.wait()
    a, rows = a_s[core], pl.ds(pl.multiple_of(core * OWN, OWN), OWN)
    t = _dot(a, wks[...]).astype(BF)
    for h in range(4):
        stage[h, 0] = turned(t[:, h * HEAD : (h + 1) * HEAD], cos_s[rows, :], sin_s[rows, :])
    get_q(0).start()
    with scope("vw"):
        get_v.wait()
    get_q(1).start()
    t = _dot(a, wqs[2]).astype(BF)
    for h in range(4):
        stage[h, 1] = t[:, h * HEAD : (h + 1) * HEAD]
    get_q(2).start()
    for j in range(3):
        to_mate(j).start()
    kv[core, 4 * line + z] = stage[line]
    along_z(line, start)
    hand(4 * line + z).start()

    with scope("swap"):
        for r in range(OWN // PIECE):
            swap(1 - core, r).wait_recv()
            norm(1 - core, r)

    def q_copy(j):
        return remote(q_stage.at[j], qt.at[line], q_send.at[j], q_recv.at[line], in_plane(mate(j)))

    def project_q(j, _):
        get_q(j).wait()
        q = _dot(a_s[...].reshape(UNIT, D), wqs[lax.rem(j, 3)]).astype(BF)
        for n in range(4):
            q_stage[j, :, n * UNIT : (n + 1) * UNIT] = turned(q[:, n * HEAD : (n + 1) * HEAD], cos_s[...], sin_s[...]).T
        pl.when(j < 3)(lambda: q_copy(j).start())

        @pl.when(j == 0)
        def _():
            get_q(3).start()

        @pl.when(j == 2)
        def _():
            with scope("plane"):
                def take(l, _):
                    @pl.when(l != line)
                    def _():
                        arrived(4 * l + z)
                        along_z(l, start)
                        hand(4 * l + z).start()

                lax.fori_loop(0, 4, take, None)

    with scope("q_proj"):
        lax.fori_loop(0, 4, project_q, None)
    qt[line] = q_stage[3]
    for h in range(4):
        get_o(h).start()

    top_s, mix_s, score_s, most_s, weight_s, keep_s = (top_a, top_b), (mix_a, mix_b), (s_a, s_b), (m_a, m_b), (p_a, p_b), (k_a, k_b)
    for n in range(2):
        top_s[n][...] = jnp.full((4, 1, STRIP), NEG, F32)
        mix_s[n][...] = jnp.zeros((4, HEAD + 8, STRIP), F32)

    def used(l, place):
        return (place != z) & ((l < 3) | (place < z))

    def relayed(l, place):
        return used(l, place) & ~direct(l) & ({0: z == 2, 3: z == 1}.get(place, z < 0))

    def take_relay(l):
        with scope("take_relay"):
            for place in (0, 3):
                @pl.when(relayed(l, place))
                def _():
                    arrived(4 * l + place)
                    relay(l, start)
                    hand(4 * l + place).start()

    def take_z(l):
        with scope("take_z"):
            for place in (0, 3, 1, 2):
                @pl.when(used(l, place) & ~relayed(l, place))
                def _():
                    arrived(4 * l + place)
                    hand(4 * l + place).start()

    def scores(l, g, n, masked):
        t = _dot(kv[:, pl.ds(4 * g, 4), 0].reshape(LINE, HEAD), qt[l, :, n * STRIP : (n + 1) * STRIP])
        if masked:
            at = lax.broadcasted_iota(jnp.int32, (LINE, 1), 0)
            key = lax.div(at, 2 * UNIT) * OWN + lax.div(lax.rem(at, 2 * UNIT), OWN) * UNIT + lax.rem(at, OWN)
            query = z * UNIT + lax.rem(lax.broadcasted_iota(jnp.int32, (1, STRIP), 1), UNIT)
            t = jnp.where(query >= key, t, HIDDEN)
        score_s[n][...] = t
        most_s[n][...] = t.max(axis=0, keepdims=True)

    def weights(l, n):
        old = top_s[n][l]
        top = jnp.maximum(old, most_s[n][...])
        top_s[n][l] = top
        keep_s[n][...] = jnp.exp2((old - top) * E)
        weight_s[n][...] = jnp.exp2((score_s[n][...] - top) * E).astype(BF)

    def values(l, g, n):
        v = jnp.concatenate([vt[g], jnp.ones((8, LINE), BF)], 0)
        mix_s[n][l] = mix_s[n][l] * keep_s[n][...] + _dot(v, weight_s[n][...])

    def attend(l, g, masked):
        with scope("attend_alone"):
            for n in range(2):
                scores(l, g, n, masked)
            for n in range(2):
                weights(l, n)
            for n in range(2):
                values(l, g, n)

    def attend_next(l, g, masked, l0, g0):
        with scope("attend#m=%d" % masked):
            scores(l, g, 0, masked)
            weights(l0, 1)
            values(l0, g0, 0)
            scores(l, g, 1, masked)
            weights(l, 0)
            values(l0, g0, 1)

    def out_copy(l):
        return remote(o_stage.at[l], seen_s.at[line], out_send.at[l], out_recv.at[line], in_plane(l))

    def complete(l):
        with scope("complete"):
            for n in range(2):
                out = (mix_s[n][l, :HEAD, :] * (1 / mix_s[n][l, HEAD : HEAD + 1, :])).astype(BF)
                for m in range(2):
                    h = 2 * n + m
                    o_stage[l, :, h * HEAD : (h + 1) * HEAD] = out[:, m * UNIT : (m + 1) * UNIT].T
            pl.when(l != line)(lambda: out_copy(l).start())

            @pl.when(l == line)
            def _():
                seen_s[line] = o_stage[l]

    def handed(g):
        with scope("hand_wait"):
            for place in range(4):
                @pl.when((g < 3) | (place <= z))
                def _():
                    b = 4 * g + place
                    remote(kv.at[1 - core, b], kv.at[1 - core, b], hand_send.at[b], hand_recv.at[b], partner).wait_recv()
        for i in range(8):
            vt[g, :, i * OWN : (i + 1) * OWN] = kv[i // 4, 4 * g + i % 4, 1].T

    def q_wait(l):
        with scope("q_wait"):
            remote(qt.at[l], qt.at[l], q_send.at[0], q_recv.at[l], partner).wait_recv()

    def other(k):
        return jnp.where(line <= k, k + 1, k)

    across = mate(0)
    early = across > line
    take_z(line)
    handed(line)
    attend(line, line, True)

    @pl.when(early)
    def _():
        q_wait(across)
        attend(across, line, False)

    take_relay(other(0))
    take_relay(other(1))

    @pl.when(line == 0)
    def _():
        complete(line)
        q_wait(mate(1))
        attend(mate(1), line, False)

    weight_s[0][...] = jnp.zeros((LINE, STRIP), BF)
    keep_s[0][...] = jnp.ones((1, STRIP), F32)
    score_s[1][...] = jnp.full((LINE, STRIP), HIDDEN, F32)
    most_s[1][...] = jnp.full((1, STRIP), NEG, F32)

    takes = (0, jnp.where(line == 3, 1, 0), jnp.where(line == 0, 1, 4))
    needs = (0, jnp.where(line == 3, 2, 1), jnp.where(line == 0, 2, 5))

    def row(i, carry):
        j = jnp.where((line == 2) & (i > 0) & (i < 3), 3 - i, i)
        l = mate(j)
        met = (j == 0) & early | (line == 0) & (j == 1)
        pl.when((l != line) & ~met)(lambda: q_wait(l))

        def meet(g, carry):
            s, l0, g0 = carry
            done = (g == line) & ((l == line) | met)

            @pl.when(~done)
            def _():
                pl.when(s == jnp.where(line == 0, 0, 2))(lambda: take_relay(other(2)))
                for k in range(3):
                    pl.when(s == takes[k])(lambda k=k: take_z(other(k)))
                for k in range(3):
                    pl.when(s == needs[k])(lambda k=k: handed(other(k)))
                pl.when(l == g)(lambda: attend_next(l, g, True, l0, g0))
                pl.when(l > g)(lambda: attend_next(l, g, False, l0, g0))
                pl.when((s > 0) & (l0 != l))(lambda: complete(l0))

            return jnp.where(done, s, s + 1), jnp.where(done, l0, l), jnp.where(done, g0, g)

        return lax.fori_loop(0, l + 1, meet, carry)

    _, last, g0 = lax.fori_loop(0, 4, row, (0, line, line))
    with scope("attend_last"):
        weights(last, 1)
        for n in range(2):
            values(last, g0, n)
    complete(last)

    def give(c):
        return remote(part_s.at[c, 1 - core], other_s.at[c], part_send.at[c], part_recv.at[c], partner)

    def product(c, hs):
        at = pl.ds(pl.multiple_of(c * CHUNK, CHUNK), CHUNK)
        seen = jnp.concatenate([seen_s[h] for h in hs], 1)
        return _dot(seen, jnp.concatenate([wos[h, :, at] for h in hs], 0)).reshape(2, OWN, CHUNK)

    def put(c):
        at = pl.ds(pl.multiple_of(c * CHUNK, CHUNK), CHUNK)
        return pltpu.make_async_copy(a_s.at[0, :, at], y_hbm.at[:, at], y_sem.at[c])

    def finish(c):
        give(c).wait_recv()
        at = pl.ds(pl.multiple_of(c * CHUNK, CHUNK), CHUNK)
        a_s[0, :, at] = (xs[core, :, at].astype(F32) + (part_s[c, core] + other_s[c])).astype(BF)
        put(c).start()

    def seen_wait(l):
        with scope("seen_wait"):
            remote(seen_s.at[l], seen_s.at[l], out_send.at[0], out_recv.at[l], partner).wait_recv()

    for h in range(4):
        get_o(h).wait()
    seen_wait(mate(0))

    def project_early(c, _):
        both = [product(2 * c + i, (line, mate(0))) for i in range(2)]
        for i in range(2):
            part_s[2 * c + i] = both[i]

    with scope("o_early"):
        lax.fori_loop(0, 4, project_early, None)
    for r in range(OWN // PIECE):
        swap(core, r).wait_send()
    for j in range(3):
        to_mate(j).wait_send()
        q_copy(j).wait_send()

    def drain(l, _):
        along_z(l, sent)
        relay(l, sent)
        pl.when(l != line)(lambda: out_copy(l).wait_send())
        for place in range(4):
            pl.when((l < 3) | (place <= z))(lambda place=place: hand(4 * l + place).wait_send())

    lax.fori_loop(0, 4, drain, None)

    seen_wait(mate(1))
    seen_wait(mate(2))

    def project_late(c, _):
        both = [part_s[2 * c + i] + product(2 * c + i, (mate(1), mate(2))) for i in range(2)]
        for i in range(2):
            part_s[2 * c + i] = both[i]
        for i in range(2):
            give(2 * c + i).start()

        @pl.when(c > 1)
        def _():
            finish(2 * c - 4)
            finish(2 * c - 3)

    with scope("o_late"):
        lax.fori_loop(0, 4, project_late, None)
    with scope("finish"):
        for c in range(4, 8):
            finish(c)

    def drain_chunk(c, _):
        give(c).wait_send()
        put(c).wait()

    lax.fori_loop(0, 8, drain_chunk, None)


def solution(mesh):
    def step(x, gain, wq, wk, wv, wo):
        hbm = pl.BlockSpec(memory_space=pl.ANY)
        dma = lambda *shape: pltpu.SemaphoreType.DMA(shape)
        return pl.pallas_call(
            kernel,
            out_shape=jax.ShapeDtypeStruct((OWN, D), BF),
            in_specs=[hbm] * 6,
            out_specs=hbm,
            scratch_shapes=[
                pltpu.VMEM((2, OWN, D), BF),
                pltpu.VMEM((D,), BF),
                pltpu.VMEM((2, OWN, D), BF),
                pltpu.VMEM((UNIT, HEAD), F32),
                pltpu.VMEM((UNIT, HEAD), F32),
                pltpu.VMEM((D, 512), BF),
                pltpu.VMEM((3, D, CHUNK), BF),
                pltpu.VMEM((4, CHUNK, D), BF),
                pltpu.VMEM((2, 16, 2, OWN, HEAD), BF),
                pltpu.VMEM((4, 2, OWN, HEAD), BF),
                pltpu.VMEM((4, HEAD, 4 * UNIT), BF),
                pltpu.VMEM((4, HEAD, 4 * UNIT), BF),
                pltpu.VMEM((4, HEAD, LINE), BF),
                *[pltpu.VMEM((4, 1, STRIP), F32)] * 2,
                *[pltpu.VMEM((4, HEAD + 8, STRIP), F32)] * 2,
                *[pltpu.VMEM((LINE, STRIP), F32)] * 2,
                *[pltpu.VMEM((1, STRIP), F32)] * 2,
                *[pltpu.VMEM((LINE, STRIP), BF)] * 2,
                *[pltpu.VMEM((1, STRIP), F32)] * 2,
                pltpu.VMEM((4, UNIT, 4 * HEAD), BF),
                pltpu.VMEM((4, UNIT, 4 * HEAD), BF),
                pltpu.VMEM((8, 2, OWN, CHUNK), F32),
                pltpu.VMEM((8, OWN, CHUNK), F32),
                dma(OWN // PIECE), dma(1), dma(2), dma(4), dma(4), dma(OWN // PIECE), dma(OWN // PIECE),
                dma(3), dma(16), dma(6, 4), dma(4), dma(16), dma(16),
                dma(3), dma(4), dma(4), dma(4), dma(8), dma(8), dma(8),
            ],
            compiler_params=pltpu.CompilerParams(collective_id=0, has_side_effects=True, vmem_limit_bytes=67043328),
        )(x, gain, wq, wk, wv, wo)

    tokens, whole = P(("dp", "sp"), None), P(None, None)
    return jax.shard_map(
        step,
        mesh=mesh,
        in_specs=(tokens, P(None), whole, whole, whole, whole),
        out_specs=tokens,
        check_vma=False,
    )
```

```python
import jax
import jax.numpy as jnp
from jax import lax
from jax.experimental import pallas as pl
from jax.experimental.pallas import tpu as pltpu
from jax.sharding import PartitionSpec as P

scope = jax.named_scope
HEAD = 128
LOG2_THETA = 13.287712379549449
LOG2E = 1.4426950408889634
NEG = -1e30
HIDDEN = -2e30
D = 4096
OWN = 128
PIECE = 32
UNIT = 256
LINE = 4 * UNIT
CHUNK = 512
STRIP = 512
E = HEAD**-0.5 * LOG2E
BF, F32 = jnp.bfloat16, jnp.float32


def _dot(a, b):
    return lax.dot_general(a, b, (((1,), (0,)), ((), ())), preferred_element_type=F32)


def kernel(x_hbm, gain_hbm, wq_hbm, wk_hbm, wv_hbm, wo_hbm, y_hbm,
           xs, gain_s, a_s, cos_s, sin_s, wks, wqs, wos, kv, stage, qt, q_stage, vt, top_a, top_b, mix_a, mix_b, s_a, s_b, m_a, m_b, p_a, p_b, k_a, k_b, seen_s, o_stage, part_s, other_s,
           x_sem, gain_sem, k_sem, wq_sem, wo_sem, swap_send, swap_recv, plane_send, block_recv, z_send, relay_send, hand_send, hand_recv,
           q_send, q_recv, out_send, out_recv, part_send, part_recv, y_sem):
    me = lax.axis_index("sp")
    core, chip = lax.rem(me, 2), lax.div(me, 2)
    z, line = lax.rem(chip, 4), lax.div(chip, 4)
    y, x = lax.rem(line, 2), lax.div(line, 2)
    partner = me + 1 - 2 * core

    def in_plane(l):
        return me + (lax.div(l, 2) - x) * 16 + (lax.rem(l, 2) - y) * 8

    def mate(j):
        dx, dy = 1 - lax.div(j, 2), lax.rem(j + 1, 2)
        return lax.rem(x + dx, 2) * 2 + lax.rem(y + dy, 2)

    def get_x(r):
        at = pl.ds(r * PIECE, PIECE)
        return pltpu.make_async_copy(x_hbm.at[at], xs.at[core, at], x_sem.at[r])

    get_k = pltpu.make_async_copy(wk_hbm, wks, k_sem.at[0])
    get_v = pltpu.make_async_copy(wv_hbm, wqs.at[2], k_sem.at[1])

    def get_q(j):
        at = pl.multiple_of(mate(j) * 1024 + core * 512, CHUNK)
        return pltpu.make_async_copy(wq_hbm.at[:, pl.ds(at, CHUNK)], wqs.at[lax.rem(j, 3)], wq_sem.at[j])

    def get_o(h):
        return pltpu.make_async_copy(wo_hbm.at[pl.ds(pl.multiple_of(h * 1024 + core * 512, CHUNK), CHUNK)], wos.at[h], wo_sem.at[h])

    get_gain = pltpu.make_async_copy(gain_hbm, gain_s, gain_sem.at[0])
    get_x(0).start()
    get_gain.start()
    for r in range(1, OWN // PIECE):
        get_x(r).start()

    kv[:, 12:] = jnp.zeros((2, 4, 2, OWN, HEAD), BF)

    barrier = pltpu.get_barrier_semaphore()

    def greet(device):
        pl.semaphore_signal(barrier, inc=1, device_id={"sp": device}, device_id_type=pl.DeviceIdType.MESH)

    greet(partner)
    for j in range(3):
        greet(in_plane(mate(j)))
    pl.when(z > 0)(lambda: greet(me - 2))
    pl.when(z < 3)(lambda: greet(me + 2))
    greet(jnp.where(z < 2, me + 4, me - 4))
    pl.when(z == 0)(lambda: greet(me + 6))
    pl.when(z == 3)(lambda: greet(me - 6))
    def remote(src, dst, send, recv, device):
        return pltpu.make_async_remote_copy(src_ref=src, dst_ref=dst, send_sem=send, recv_sem=recv, device_id={"sp": device},
                                            device_id_type=pl.DeviceIdType.MESH)

    def swap(which, r):
        at = pl.ds(r * PIECE, PIECE)
        return remote(xs.at[which, at], xs.at[which, at], swap_send.at[r], swap_recv.at[r], partner)

    def norm(which, r):
        at = pl.ds(r * PIECE, PIECE)
        wide = xs[which, at, :].astype(F32)
        scale = lax.rsqrt(jnp.mean(wide * wide, -1, keepdims=True) + 1e-6)
        a_s[which, at, :] = (wide * scale * gain_s[...].astype(F32).reshape(1, D)).astype(BF)

    with scope("x_in"):
        for r in range(OWN // PIECE):
            get_x(r).wait()
            if r == 0:
                get_k.start()
                get_v.start()
                get_gain.wait()
            norm(core, r)
    with scope("barrier"):
        pl.semaphore_wait(barrier, 7)
    for r in range(OWN // PIECE):
        swap(core, r).start()

    def turned(t, cos, sin):
        t = t.astype(F32)
        return (t * cos + pltpu.roll(t, HEAD // 2, 1) * sin).astype(BF)

    def block(b):
        return kv.at[core, b]

    def to_mate(j):
        l = mate(j)
        return remote(stage.at[l], block(4 * line + z), plane_send.at[j], block_recv.at[4 * line + z], in_plane(l))

    def arrived(b):
        remote(block(b), block(b), z_send.at[0, 0], block_recv.at[b], partner).wait_recv()

    STEPS = (3, -3, 2, -2, 1, -1)

    def direct(l):
        return (l == line) | (l == 0)

    def along_z(l, act):
        for i, step in enumerate(STEPS):
            b = 4 * l + z
            copy = remote(block(b), block(b), z_send.at[i, l], block_recv.at[b], me + 2 * step)
            there = z + step
            yes = (there >= 0) & (there < 4)
            if step < 0:
                yes = yes & (l < 3)
            if abs(step) == 3:
                yes = yes & direct(l)
            pl.when(yes)(lambda copy=copy: act(copy))

    def relay(l, act):
        up = remote(block(4 * l), block(4 * l), relay_send.at[l], block_recv.at[4 * l], me + 2)
        down = remote(block(4 * l + 3), block(4 * l + 3), relay_send.at[l], block_recv.at[4 * l + 3], me - 2)
        pl.when((z == 2) & ~direct(l))(lambda: act(up))
        pl.when((z == 1) & (l < 3) & ~direct(l))(lambda: act(down))

    def hand(b):
        return remote(block(b), block(b), hand_send.at[b], hand_recv.at[b], partner)

    start = lambda copy: copy.start()
    sent = lambda copy: copy.wait_send()

    place = chip * UNIT + lax.broadcasted_iota(jnp.int32, (UNIT, HEAD), 0)
    element = lax.broadcasted_iota(jnp.int32, (1, HEAD), 1)
    freq = jnp.exp2(lax.rem(element, HEAD // 2).astype(F32) * (-LOG2_THETA * 2 / HEAD))
    angle = place.astype(F32) * freq
    sin = jnp.sin(angle)
    cos_s[...] = jnp.cos(angle)
    sin_s[...] = jnp.where(element < HEAD // 2, -sin, sin)
    with scope("kw"):
        get_k.wait()
    a, rows = a_s[core], pl.ds(pl.multiple_of(core * OWN, OWN), OWN)
    t = _dot(a, wks[...]).astype(BF)
    for h in range(4):
        stage[h, 0] = turned(t[:, h * HEAD : (h + 1) * HEAD], cos_s[rows, :], sin_s[rows, :])
    get_q(0).start()
    with scope("vw"):
        get_v.wait()
    get_q(1).start()
    t = _dot(a, wqs[2]).astype(BF)
    for h in range(4):
        stage[h, 1] = t[:, h * HEAD : (h + 1) * HEAD]
    get_q(2).start()
    for j in range(3):
        to_mate(j).start()
    kv[core, 4 * line + z] = stage[line]
    along_z(line, start)
    hand(4 * line + z).start()

    with scope("swap"):
        for r in range(OWN // PIECE):
            swap(1 - core, r).wait_recv()
            norm(1 - core, r)

    def q_copy(j):
        return remote(q_stage.at[j], qt.at[line], q_send.at[j], q_recv.at[line], in_plane(mate(j)))

    def take_plane(l):
        arrived(4 * l + z)
        along_z(l, start)
        hand(4 * l + z).start()

    late_y = x == 1

    def project_q(j, _):
        get_q(j).wait()
        q = _dot(a_s[...].reshape(UNIT, D), wqs[lax.rem(j, 3)]).astype(BF)
        for n in range(4):
            q_stage[j, :, n * UNIT : (n + 1) * UNIT] = turned(q[:, n * HEAD : (n + 1) * HEAD], cos_s[...], sin_s[...]).T
        pl.when(j < 3)(lambda: q_copy(j).start())

        @pl.when(j == 0)
        def _():
            get_q(3).start()

        @pl.when(j == 2)
        def _():
            with scope("plane"):
                def take(l, _):
                    pl.when((l != line) & ~(late_y & (l == mate(2))))(lambda: take_plane(l))

                lax.fori_loop(0, 4, take, None)

    with scope("q_proj"):
        lax.fori_loop(0, 4, project_q, None)
    qt[line] = q_stage[3]
    for h in range(4):
        get_o(h).start()

    top_s, mix_s, score_s, most_s, weight_s, keep_s = (top_a, top_b), (mix_a, mix_b), (s_a, s_b), (m_a, m_b), (p_a, p_b), (k_a, k_b)
    for n in range(2):
        top_s[n][...] = jnp.full((4, 1, STRIP), NEG, F32)
        mix_s[n][...] = jnp.zeros((4, HEAD + 8, STRIP), F32)

    def used(l, place):
        return (place != z) & ((l < 3) | (place < z))

    def relayed(l, place):
        return used(l, place) & ~direct(l) & ({0: z == 2, 3: z == 1}.get(place, z < 0))

    def take_relay(l):
        with scope("take_relay"):
            for place in (0, 3):
                @pl.when(relayed(l, place))
                def _():
                    arrived(4 * l + place)
                    relay(l, start)
                    hand(4 * l + place).start()

    def take_z(l):
        with scope("take_z"):
            for place in (0, 3, 1, 2):
                @pl.when(used(l, place) & ~relayed(l, place))
                def _():
                    arrived(4 * l + place)
                    hand(4 * l + place).start()

    def scores(l, g, n, masked):
        t = _dot(kv[:, pl.ds(4 * g, 4), 0].reshape(LINE, HEAD), qt[l, :, n * STRIP : (n + 1) * STRIP])
        if masked:
            at = lax.broadcasted_iota(jnp.int32, (LINE, 1), 0)
            key = lax.div(at, 2 * UNIT) * OWN + lax.div(lax.rem(at, 2 * UNIT), OWN) * UNIT + lax.rem(at, OWN)
            query = z * UNIT + lax.rem(lax.broadcasted_iota(jnp.int32, (1, STRIP), 1), UNIT)
            t = jnp.where(query >= key, t, HIDDEN)
        score_s[n][...] = t
        most_s[n][...] = t.max(axis=0, keepdims=True)

    def weights(l, n):
        old = top_s[n][l]
        top = jnp.maximum(old, most_s[n][...])
        top_s[n][l] = top
        keep_s[n][...] = jnp.exp2((old - top) * E)
        weight_s[n][...] = jnp.exp2((score_s[n][...] - top) * E).astype(BF)

    def values(l, g, n):
        v = jnp.concatenate([vt[g], jnp.ones((8, LINE), BF)], 0)
        mix_s[n][l] = mix_s[n][l] * keep_s[n][...] + _dot(v, weight_s[n][...])

    def attend(l, g, masked):
        with scope("attend_alone"):
            for n in range(2):
                scores(l, g, n, masked)
            for n in range(2):
                weights(l, n)
            for n in range(2):
                values(l, g, n)

    def attend_next(l, g, masked, l0, g0):
        with scope("attend#m=%d" % masked):
            scores(l, g, 0, masked)
            weights(l0, 1)
            values(l0, g0, 0)
            scores(l, g, 1, masked)
            weights(l, 0)
            values(l0, g0, 1)

    def out_copy(l):
        return remote(o_stage.at[l], seen_s.at[line], out_send.at[l], out_recv.at[line], in_plane(l))

    def complete(l):
        with scope("complete"):
            for n in range(2):
                out = (mix_s[n][l, :HEAD, :] * (1 / mix_s[n][l, HEAD : HEAD + 1, :])).astype(BF)
                for m in range(2):
                    h = 2 * n + m
                    o_stage[l, :, h * HEAD : (h + 1) * HEAD] = out[:, m * UNIT : (m + 1) * UNIT].T
            pl.when(l != line)(lambda: out_copy(l).start())

            @pl.when(l == line)
            def _():
                seen_s[line] = o_stage[l]

    def handed(g):
        with scope("hand_wait"):
            for place in range(4):
                @pl.when((g < 3) | (place <= z))
                def _():
                    b = 4 * g + place
                    remote(kv.at[1 - core, b], kv.at[1 - core, b], hand_send.at[b], hand_recv.at[b], partner).wait_recv()
        for i in range(8):
            vt[g, :, i * OWN : (i + 1) * OWN] = kv[i // 4, 4 * g + i % 4, 1].T

    def q_wait(l):
        with scope("q_wait"):
            remote(qt.at[l], qt.at[l], q_send.at[0], q_recv.at[l], partner).wait_recv()

    def other(k):
        return jnp.where(line <= k, k + 1, k)

    across = mate(0)
    early = across > line
    take_z(line)
    handed(line)
    attend(line, line, True)
    with scope("plane_y"):
        pl.when(late_y)(lambda: take_plane(mate(2)))

    @pl.when(early)
    def _():
        q_wait(across)
        attend(across, line, False)

    take_relay(other(0))
    take_relay(other(1))

    @pl.when(line == 0)
    def _():
        complete(line)
        q_wait(mate(1))
        attend(mate(1), line, False)

    weight_s[0][...] = jnp.zeros((LINE, STRIP), BF)
    keep_s[0][...] = jnp.ones((1, STRIP), F32)
    score_s[1][...] = jnp.full((LINE, STRIP), HIDDEN, F32)
    most_s[1][...] = jnp.full((1, STRIP), NEG, F32)

    takes = (0, jnp.where(line == 3, 1, 0), jnp.where(line == 0, 1, 4))
    needs = (0, jnp.where(line == 3, 2, 1), jnp.where(line == 0, 2, 5))

    def row(i, carry):
        j = jnp.where((line == 2) & (i > 0) & (i < 3), 3 - i, i)
        l = mate(j)
        met = (j == 0) & early | (line == 0) & (j == 1)
        pl.when((l != line) & ~met)(lambda: q_wait(l))

        def meet(g, carry):
            s, l0, g0 = carry
            done = (g == line) & ((l == line) | met)

            @pl.when(~done)
            def _():
                pl.when(s == jnp.where(line == 0, 0, 2))(lambda: take_relay(other(2)))
                for k in range(3):
                    pl.when(s == takes[k])(lambda k=k: take_z(other(k)))
                for k in range(3):
                    pl.when(s == needs[k])(lambda k=k: handed(other(k)))
                pl.when(l == g)(lambda: attend_next(l, g, True, l0, g0))
                pl.when(l > g)(lambda: attend_next(l, g, False, l0, g0))
                pl.when((s > 0) & (l0 != l))(lambda: complete(l0))

            return jnp.where(done, s, s + 1), jnp.where(done, l0, l), jnp.where(done, g0, g)

        return lax.fori_loop(0, l + 1, meet, carry)

    _, last, g0 = lax.fori_loop(0, 4, row, (0, line, line))
    with scope("attend_last"):
        weights(last, 1)
        for n in range(2):
            values(last, g0, n)
    complete(last)

    def give(c):
        return remote(part_s.at[c, 1 - core], other_s.at[c], part_send.at[c], part_recv.at[c], partner)

    def product(c, hs):
        at = pl.ds(pl.multiple_of(c * CHUNK, CHUNK), CHUNK)
        seen = jnp.concatenate([seen_s[h] for h in hs], 1)
        return _dot(seen, jnp.concatenate([wos[h, :, at] for h in hs], 0)).reshape(2, OWN, CHUNK)

    def put(c):
        at = pl.ds(pl.multiple_of(c * CHUNK, CHUNK), CHUNK)
        return pltpu.make_async_copy(a_s.at[0, :, at], y_hbm.at[:, at], y_sem.at[c])

    def finish(c):
        give(c).wait_recv()
        at = pl.ds(pl.multiple_of(c * CHUNK, CHUNK), CHUNK)
        a_s[0, :, at] = (xs[core, :, at].astype(F32) + (part_s[c, core] + other_s[c])).astype(BF)
        put(c).start()

    def seen_wait(l):
        with scope("seen_wait"):
            remote(seen_s.at[l], seen_s.at[l], out_send.at[0], out_recv.at[l], partner).wait_recv()

    for h in range(4):
        get_o(h).wait()
    seen_wait(mate(0))

    def project_early(c, _):
        both = [product(2 * c + i, (line, mate(0))) for i in range(2)]
        for i in range(2):
            part_s[2 * c + i] = both[i]

    with scope("o_early"):
        lax.fori_loop(0, 4, project_early, None)
    for r in range(OWN // PIECE):
        swap(core, r).wait_send()
    for j in range(3):
        to_mate(j).wait_send()
        q_copy(j).wait_send()

    def drain(l, _):
        along_z(l, sent)
        relay(l, sent)
        pl.when(l != line)(lambda: out_copy(l).wait_send())
        for place in range(4):
            pl.when((l < 3) | (place <= z))(lambda place=place: hand(4 * l + place).wait_send())

    lax.fori_loop(0, 4, drain, None)

    seen_wait(mate(1))
    seen_wait(mate(2))

    def project_late(c, _):
        both = [part_s[2 * c + i] + product(2 * c + i, (mate(1), mate(2))) for i in range(2)]
        for i in range(2):
            part_s[2 * c + i] = both[i]
        for i in range(2):
            give(2 * c + i).start()

        @pl.when(c > 1)
        def _():
            finish(2 * c - 4)
            finish(2 * c - 3)

    with scope("o_late"):
        lax.fori_loop(0, 4, project_late, None)
    with scope("finish"):
        for c in range(4, 8):
            finish(c)

    def drain_chunk(c, _):
        give(c).wait_send()
        put(c).wait()

    lax.fori_loop(0, 8, drain_chunk, None)


def solution(mesh):
    def step(x, gain, wq, wk, wv, wo):
        hbm = pl.BlockSpec(memory_space=pl.ANY)
        dma = lambda *shape: pltpu.SemaphoreType.DMA(shape)
        return pl.pallas_call(
            kernel,
            out_shape=jax.ShapeDtypeStruct((OWN, D), BF),
            in_specs=[hbm] * 6,
            out_specs=hbm,
            scratch_shapes=[
                pltpu.VMEM((2, OWN, D), BF),
                pltpu.VMEM((D,), BF),
                pltpu.VMEM((2, OWN, D), BF),
                pltpu.VMEM((UNIT, HEAD), F32),
                pltpu.VMEM((UNIT, HEAD), F32),
                pltpu.VMEM((D, 512), BF),
                pltpu.VMEM((3, D, CHUNK), BF),
                pltpu.VMEM((4, CHUNK, D), BF),
                pltpu.VMEM((2, 16, 2, OWN, HEAD), BF),
                pltpu.VMEM((4, 2, OWN, HEAD), BF),
                pltpu.VMEM((4, HEAD, 4 * UNIT), BF),
                pltpu.VMEM((4, HEAD, 4 * UNIT), BF),
                pltpu.VMEM((4, HEAD, LINE), BF),
                *[pltpu.VMEM((4, 1, STRIP), F32)] * 2,
                *[pltpu.VMEM((4, HEAD + 8, STRIP), F32)] * 2,
                *[pltpu.VMEM((LINE, STRIP), F32)] * 2,
                *[pltpu.VMEM((1, STRIP), F32)] * 2,
                *[pltpu.VMEM((LINE, STRIP), BF)] * 2,
                *[pltpu.VMEM((1, STRIP), F32)] * 2,
                pltpu.VMEM((4, UNIT, 4 * HEAD), BF),
                pltpu.VMEM((4, UNIT, 4 * HEAD), BF),
                pltpu.VMEM((8, 2, OWN, CHUNK), F32),
                pltpu.VMEM((8, OWN, CHUNK), F32),
                dma(OWN // PIECE), dma(1), dma(2), dma(4), dma(4), dma(OWN // PIECE), dma(OWN // PIECE),
                dma(3), dma(16), dma(6, 4), dma(4), dma(16), dma(16),
                dma(3), dma(4), dma(4), dma(4), dma(8), dma(8), dma(8),
            ],
            compiler_params=pltpu.CompilerParams(collective_id=0, has_side_effects=True, vmem_limit_bytes=67043328),
        )(x, gain, wq, wk, wv, wo)

    tokens, whole = P(("dp", "sp"), None), P(None, None)
    return jax.shard_map(
        step,
        mesh=mesh,
        in_specs=(tokens, P(None), whole, whole, whole, whole),
        out_specs=tokens,
        check_vma=False,
    )
```

```python
import jax
import jax.numpy as jnp
from jax import lax
from jax.experimental import pallas as pl
from jax.experimental.pallas import tpu as pltpu
from jax.sharding import PartitionSpec as P

scope = jax.named_scope
HEAD = 128
LOG2_THETA = 13.287712379549449
LOG2E = 1.4426950408889634
NEG = -1e30
HIDDEN = -2e30
D = 4096
OWN = 128
PIECE = 32
UNIT = 256
LINE = 4 * UNIT
CHUNK = 512
STRIP = 512
E = HEAD**-0.5 * LOG2E
BF, F32 = jnp.bfloat16, jnp.float32


def _dot(a, b):
    return lax.dot_general(a, b, (((1,), (0,)), ((), ())), preferred_element_type=F32)


def kernel(x_hbm, gain_hbm, wq_hbm, wk_hbm, wv_hbm, wo_hbm, y_hbm,
           xs, gain_s, a_s, cos_s, sin_s, wks, wqs, wos, kv, stage, qt, q_stage, vt, top_a, top_b, mix_a, mix_b, s_a, s_b, m_a, m_b, p_a, p_b, k_a, k_b, seen_s, o_stage, part_s, other_s,
           x_sem, gain_sem, k_sem, wq_sem, wo_sem, swap_send, swap_recv, plane_send, block_recv, z_send, relay_send, hand_send, hand_recv,
           q_send, q_recv, out_send, out_recv, part_send, part_recv, y_sem):
    me = lax.axis_index("sp")
    core, chip = lax.rem(me, 2), lax.div(me, 2)
    z, line = lax.rem(chip, 4), lax.div(chip, 4)
    y, x = lax.rem(line, 2), lax.div(line, 2)
    partner = me + 1 - 2 * core

    def in_plane(l):
        return me + (lax.div(l, 2) - x) * 16 + (lax.rem(l, 2) - y) * 8

    def mate(j):
        dx, dy = 1 - lax.div(j, 2), lax.rem(j + 1, 2)
        return lax.rem(x + dx, 2) * 2 + lax.rem(y + dy, 2)

    def get_x(r):
        at = pl.ds(r * PIECE, PIECE)
        return pltpu.make_async_copy(x_hbm.at[at], xs.at[core, at], x_sem.at[r])

    get_k = pltpu.make_async_copy(wk_hbm, wks, k_sem.at[0])
    get_v = pltpu.make_async_copy(wv_hbm, wqs.at[2], k_sem.at[1])

    def get_q(j):
        at = pl.multiple_of(mate(j) * 1024 + core * 512, CHUNK)
        return pltpu.make_async_copy(wq_hbm.at[:, pl.ds(at, CHUNK)], wqs.at[lax.rem(j, 3)], wq_sem.at[j])

    def get_o(h):
        return pltpu.make_async_copy(wo_hbm.at[pl.ds(pl.multiple_of(h * 1024 + core * 512, CHUNK), CHUNK)], wos.at[h], wo_sem.at[h])

    get_gain = pltpu.make_async_copy(gain_hbm, gain_s, gain_sem.at[0])
    get_x(0).start()
    get_gain.start()
    for r in range(1, OWN // PIECE):
        get_x(r).start()

    kv[:, 12:] = jnp.zeros((2, 4, 2, OWN, HEAD), BF)

    barrier = pltpu.get_barrier_semaphore()

    def greet(device):
        pl.semaphore_signal(barrier, inc=1, device_id={"sp": device}, device_id_type=pl.DeviceIdType.MESH)

    greet(partner)
    for j in range(3):
        greet(in_plane(mate(j)))
    pl.when(z > 0)(lambda: greet(me - 2))
    pl.when(z < 3)(lambda: greet(me + 2))
    greet(jnp.where(z < 2, me + 4, me - 4))
    pl.when(z == 0)(lambda: greet(me + 6))
    pl.when(z == 3)(lambda: greet(me - 6))
    def remote(src, dst, send, recv, device):
        return pltpu.make_async_remote_copy(src_ref=src, dst_ref=dst, send_sem=send, recv_sem=recv, device_id={"sp": device},
                                            device_id_type=pl.DeviceIdType.MESH)

    def swap(which, r):
        at = pl.ds(r * PIECE, PIECE)
        return remote(xs.at[which, at], xs.at[which, at], swap_send.at[r], swap_recv.at[r], partner)

    def norm(which, r):
        at = pl.ds(r * PIECE, PIECE)
        wide = xs[which, at, :].astype(F32)
        scale = lax.rsqrt(jnp.mean(wide * wide, -1, keepdims=True) + 1e-6)
        a_s[which, at, :] = (wide * scale * gain_s[...].astype(F32).reshape(1, D)).astype(BF)

    with scope("x_in"):
        for r in range(OWN // PIECE):
            get_x(r).wait()
            if r == 0:
                get_k.start()
                get_v.start()
                get_gain.wait()
            norm(core, r)
    with scope("barrier"):
        pl.semaphore_wait(barrier, 7)
    for r in range(OWN // PIECE):
        swap(core, r).start()

    def turned(t, cos, sin):
        t = t.astype(F32)
        return (t * cos + pltpu.roll(t, HEAD // 2, 1) * sin).astype(BF)

    def block(b):
        return kv.at[core, b]

    def to_mate(j):
        l = mate(j)
        return remote(stage.at[l], block(4 * line + z), plane_send.at[j], block_recv.at[4 * line + z], in_plane(l))

    def arrived(b):
        remote(block(b), block(b), z_send.at[0, 0], block_recv.at[b], partner).wait_recv()

    STEPS = (3, -3, 2, -2, 1, -1)

    def direct(l):
        return (l == line) | (l == 0)

    def along_z(l, act):
        for i, step in enumerate(STEPS):
            b = 4 * l + z
            copy = remote(block(b), block(b), z_send.at[i, l], block_recv.at[b], me + 2 * step)
            there = z + step
            yes = (there >= 0) & (there < 4)
            if step < 0:
                yes = yes & (l < 3)
            if abs(step) == 3:
                yes = yes & direct(l)
            pl.when(yes)(lambda copy=copy: act(copy))

    def relay(l, act):
        up = remote(block(4 * l), block(4 * l), relay_send.at[l], block_recv.at[4 * l], me + 2)
        down = remote(block(4 * l + 3), block(4 * l + 3), relay_send.at[l], block_recv.at[4 * l + 3], me - 2)
        pl.when((z == 2) & ~direct(l))(lambda: act(up))
        pl.when((z == 1) & (l < 3) & ~direct(l))(lambda: act(down))

    def hand(b):
        return remote(block(b), block(b), hand_send.at[b], hand_recv.at[b], partner)

    start = lambda copy: copy.start()
    sent = lambda copy: copy.wait_send()

    place = chip * UNIT + lax.broadcasted_iota(jnp.int32, (UNIT, HEAD), 0)
    element = lax.broadcasted_iota(jnp.int32, (1, HEAD), 1)
    freq = jnp.exp2(lax.rem(element, HEAD // 2).astype(F32) * (-LOG2_THETA * 2 / HEAD))
    angle = place.astype(F32) * freq
    sin = jnp.sin(angle)
    cos_s[...] = jnp.cos(angle)
    sin_s[...] = jnp.where(element < HEAD // 2, -sin, sin)
    with scope("kw"):
        get_k.wait()
    a, rows = a_s[core], pl.ds(pl.multiple_of(core * OWN, OWN), OWN)
    t = _dot(a, wks[...]).astype(BF)
    for h in range(4):
        stage[h, 0] = turned(t[:, h * HEAD : (h + 1) * HEAD], cos_s[rows, :], sin_s[rows, :])
    get_q(0).start()
    with scope("vw"):
        get_v.wait()
    get_q(1).start()
    t = _dot(a, wqs[2]).astype(BF)
    for h in range(4):
        stage[h, 1] = t[:, h * HEAD : (h + 1) * HEAD]
    get_q(2).start()
    for j in range(3):
        to_mate(j).start()
    kv[core, 4 * line + z] = stage[line]
    along_z(line, start)
    hand(4 * line + z).start()

    with scope("swap"):
        for r in range(OWN // PIECE):
            swap(1 - core, r).wait_recv()
            norm(1 - core, r)

    def q_copy(j):
        return remote(q_stage.at[j], qt.at[line], q_send.at[j], q_recv.at[line], in_plane(mate(j)))

    def take_plane(l):
        arrived(4 * l + z)
        along_z(l, start)
        hand(4 * l + z).start()

    late_y = x == 1

    def project_q(j, _):
        get_q(j).wait()
        q = _dot(a_s[...].reshape(UNIT, D), wqs[lax.rem(j, 3)]).astype(BF)
        for n in range(4):
            q_stage[j, :, n * UNIT : (n + 1) * UNIT] = turned(q[:, n * HEAD : (n + 1) * HEAD], cos_s[...], sin_s[...]).T
        pl.when(j < 3)(lambda: q_copy(j).start())

        @pl.when(j == 0)
        def _():
            get_q(3).start()

        @pl.when(j == 2)
        def _():
            with scope("plane"):
                def take(l, _):
                    pl.when((l != line) & ~(late_y & (l == mate(2))))(lambda: take_plane(l))

                lax.fori_loop(0, 4, take, None)

    with scope("q_proj"):
        lax.fori_loop(0, 4, project_q, None)
    qt[line] = q_stage[3]
    for h in range(4):
        get_o(h).start()

    top_s, mix_s, score_s, most_s, weight_s, keep_s = (top_a, top_b), (mix_a, mix_b), (s_a, s_b), (m_a, m_b), (p_a, p_b), (k_a, k_b)
    for n in range(2):
        top_s[n][...] = jnp.full((4, 1, STRIP), NEG, F32)
        mix_s[n][...] = jnp.zeros((4, HEAD + 8, STRIP), F32)

    def used(l, place):
        return (place != z) & ((l < 3) | (place < z))

    def relayed(l, place):
        return used(l, place) & ~direct(l) & ({0: z == 2, 3: z == 1}.get(place, z < 0))

    def take_relay(l):
        with scope("take_relay"):
            for place in (0, 3):
                @pl.when(relayed(l, place))
                def _():
                    arrived(4 * l + place)
                    relay(l, start)
                    hand(4 * l + place).start()

    def take_z(l):
        with scope("take_z"):
            for place in (0, 3, 1, 2):
                @pl.when(used(l, place) & ~relayed(l, place))
                def _():
                    arrived(4 * l + place)
                    hand(4 * l + place).start()

    def scores(l, g, n, masked):
        t = _dot(kv[:, pl.ds(4 * g, 4), 0].reshape(LINE, HEAD), qt[l, :, n * STRIP : (n + 1) * STRIP])
        if masked:
            at = lax.broadcasted_iota(jnp.int32, (LINE, 1), 0)
            key = lax.div(at, 2 * UNIT) * OWN + lax.div(lax.rem(at, 2 * UNIT), OWN) * UNIT + lax.rem(at, OWN)
            query = z * UNIT + lax.rem(lax.broadcasted_iota(jnp.int32, (1, STRIP), 1), UNIT)
            t = jnp.where(query >= key, t, HIDDEN)
        score_s[n][...] = t
        most_s[n][...] = t.max(axis=0, keepdims=True)

    def weights(l, n):
        old = top_s[n][l]
        top = jnp.maximum(old, most_s[n][...])
        top_s[n][l] = top
        keep_s[n][...] = jnp.exp2((old - top) * E)
        weight_s[n][...] = jnp.exp2((score_s[n][...] - top) * E).astype(BF)

    def values(l, g, n):
        v = jnp.concatenate([vt[g], jnp.ones((8, LINE), BF)], 0)
        mix_s[n][l] = mix_s[n][l] * keep_s[n][...] + _dot(v, weight_s[n][...])

    def attend(l, g, masked):
        with scope("attend_alone"):
            for n in range(2):
                scores(l, g, n, masked)
            for n in range(2):
                weights(l, n)
            for n in range(2):
                values(l, g, n)

    def attend_next(l, g, masked, l0, g0):
        with scope("attend#m=%d" % masked):
            scores(l, g, 0, masked)
            weights(l0, 1)
            values(l0, g0, 0)
            scores(l, g, 1, masked)
            weights(l, 0)
            values(l0, g0, 1)

    def out_copy(l):
        return remote(o_stage.at[l], seen_s.at[line], out_send.at[l], out_recv.at[line], in_plane(l))

    def complete(l):
        with scope("complete"):
            for n in range(2):
                out = (mix_s[n][l, :HEAD, :] * (1 / mix_s[n][l, HEAD : HEAD + 1, :])).astype(BF)
                for m in range(2):
                    h = 2 * n + m
                    o_stage[l, :, h * HEAD : (h + 1) * HEAD] = out[:, m * UNIT : (m + 1) * UNIT].T
            pl.when(l != line)(lambda: out_copy(l).start())

            @pl.when(l == line)
            def _():
                seen_s[line] = o_stage[l]

    def handed(g):
        with scope("hand_wait"):
            for place in range(4):
                @pl.when((g < 3) | (place <= z))
                def _():
                    b = 4 * g + place
                    remote(kv.at[1 - core, b], kv.at[1 - core, b], hand_send.at[b], hand_recv.at[b], partner).wait_recv()
        for i in range(8):
            vt[g, :, i * OWN : (i + 1) * OWN] = kv[i // 4, 4 * g + i % 4, 1].T

    def q_wait(l):
        with scope("q_wait"):
            remote(qt.at[l], qt.at[l], q_send.at[0], q_recv.at[l], partner).wait_recv()

    def other(k):
        return jnp.where(line <= k, k + 1, k)

    across = mate(0)
    early = across > line
    take_z(line)
    handed(line)
    attend(line, line, True)
    with scope("plane_y"):
        pl.when(late_y)(lambda: take_plane(mate(2)))

    @pl.when(early)
    def _():
        q_wait(across)
        attend(across, line, False)

    take_relay(other(0))
    take_relay(other(1))

    @pl.when(line == 0)
    def _():
        complete(line)
        q_wait(mate(1))
        attend(mate(1), line, False)

    weight_s[0][...] = jnp.zeros((LINE, STRIP), BF)
    keep_s[0][...] = jnp.ones((1, STRIP), F32)
    score_s[1][...] = jnp.full((LINE, STRIP), HIDDEN, F32)
    most_s[1][...] = jnp.full((1, STRIP), NEG, F32)

    takes = (0, jnp.where(line == 3, 1, 0), jnp.where(line == 0, 1, 4))
    needs = (0, jnp.where(line == 3, 2, 1), jnp.where(line == 0, 2, 5))

    def row(i, carry):
        j = jnp.where((line == 1) & (i > 0) & (i < 3), 3 - i, i)
        l = mate(j)
        met = (j == 0) & early | (line == 0) & (j == 1)
        pl.when((l != line) & ~met)(lambda: q_wait(l))

        def meet(g, carry):
            s, l0, g0 = carry
            done = (g == line) & ((l == line) | met)

            @pl.when(~done)
            def _():
                pl.when(s == jnp.where(line == 0, 0, 2))(lambda: take_relay(other(2)))
                for k in range(3):
                    pl.when(s == takes[k])(lambda k=k: take_z(other(k)))
                for k in range(3):
                    pl.when(s == needs[k])(lambda k=k: handed(other(k)))
                pl.when(l == g)(lambda: attend_next(l, g, True, l0, g0))
                pl.when(l > g)(lambda: attend_next(l, g, False, l0, g0))
                pl.when((s > 0) & (l0 != l))(lambda: complete(l0))

            return jnp.where(done, s, s + 1), jnp.where(done, l0, l), jnp.where(done, g0, g)

        return lax.fori_loop(0, l + 1, meet, carry)

    _, last, g0 = lax.fori_loop(0, 4, row, (0, line, line))
    with scope("attend_last"):
        weights(last, 1)
        for n in range(2):
            values(last, g0, n)
    complete(last)

    def give(c):
        return remote(part_s.at[c, 1 - core], other_s.at[c], part_send.at[c], part_recv.at[c], partner)

    def product(c, hs):
        at = pl.ds(pl.multiple_of(c * CHUNK, CHUNK), CHUNK)
        seen = jnp.concatenate([seen_s[h] for h in hs], 1)
        return _dot(seen, jnp.concatenate([wos[h, :, at] for h in hs], 0)).reshape(2, OWN, CHUNK)

    def put(c):
        at = pl.ds(pl.multiple_of(c * CHUNK, CHUNK), CHUNK)
        return pltpu.make_async_copy(a_s.at[0, :, at], y_hbm.at[:, at], y_sem.at[c])

    def finish(c):
        give(c).wait_recv()
        at = pl.ds(pl.multiple_of(c * CHUNK, CHUNK), CHUNK)
        a_s[0, :, at] = (xs[core, :, at].astype(F32) + (part_s[c, core] + other_s[c])).astype(BF)
        put(c).start()

    def seen_wait(l):
        with scope("seen_wait"):
            remote(seen_s.at[l], seen_s.at[l], out_send.at[0], out_recv.at[l], partner).wait_recv()

    for h in range(4):
        get_o(h).wait()
    seen_wait(mate(0))

    def project_early(c, _):
        both = [product(2 * c + i, (line, mate(0))) for i in range(2)]
        for i in range(2):
            part_s[2 * c + i] = both[i]

    with scope("o_early"):
        lax.fori_loop(0, 4, project_early, None)
    for r in range(OWN // PIECE):
        swap(core, r).wait_send()
    for j in range(3):
        to_mate(j).wait_send()
        q_copy(j).wait_send()

    def drain(l, _):
        along_z(l, sent)
        relay(l, sent)
        pl.when(l != line)(lambda: out_copy(l).wait_send())
        for place in range(4):
            pl.when((l < 3) | (place <= z))(lambda place=place: hand(4 * l + place).wait_send())

    lax.fori_loop(0, 4, drain, None)

    seen_wait(mate(1))
    seen_wait(mate(2))

    def project_late(c, _):
        both = [part_s[2 * c + i] + product(2 * c + i, (mate(1), mate(2))) for i in range(2)]
        for i in range(2):
            part_s[2 * c + i] = both[i]
        for i in range(2):
            give(2 * c + i).start()

        @pl.when(c > 1)
        def _():
            finish(2 * c - 4)
            finish(2 * c - 3)

    with scope("o_late"):
        lax.fori_loop(0, 4, project_late, None)
    with scope("finish"):
        for c in range(4, 8):
            finish(c)

    def drain_chunk(c, _):
        give(c).wait_send()
        put(c).wait()

    lax.fori_loop(0, 8, drain_chunk, None)


def solution(mesh):
    def step(x, gain, wq, wk, wv, wo):
        hbm = pl.BlockSpec(memory_space=pl.ANY)
        dma = lambda *shape: pltpu.SemaphoreType.DMA(shape)
        return pl.pallas_call(
            kernel,
            out_shape=jax.ShapeDtypeStruct((OWN, D), BF),
            in_specs=[hbm] * 6,
            out_specs=hbm,
            scratch_shapes=[
                pltpu.VMEM((2, OWN, D), BF),
                pltpu.VMEM((D,), BF),
                pltpu.VMEM((2, OWN, D), BF),
                pltpu.VMEM((UNIT, HEAD), F32),
                pltpu.VMEM((UNIT, HEAD), F32),
                pltpu.VMEM((D, 512), BF),
                pltpu.VMEM((3, D, CHUNK), BF),
                pltpu.VMEM((4, CHUNK, D), BF),
                pltpu.VMEM((2, 16, 2, OWN, HEAD), BF),
                pltpu.VMEM((4, 2, OWN, HEAD), BF),
                pltpu.VMEM((4, HEAD, 4 * UNIT), BF),
                pltpu.VMEM((4, HEAD, 4 * UNIT), BF),
                pltpu.VMEM((4, HEAD, LINE), BF),
                *[pltpu.VMEM((4, 1, STRIP), F32)] * 2,
                *[pltpu.VMEM((4, HEAD + 8, STRIP), F32)] * 2,
                *[pltpu.VMEM((LINE, STRIP), F32)] * 2,
                *[pltpu.VMEM((1, STRIP), F32)] * 2,
                *[pltpu.VMEM((LINE, STRIP), BF)] * 2,
                *[pltpu.VMEM((1, STRIP), F32)] * 2,
                pltpu.VMEM((4, UNIT, 4 * HEAD), BF),
                pltpu.VMEM((4, UNIT, 4 * HEAD), BF),
                pltpu.VMEM((8, 2, OWN, CHUNK), F32),
                pltpu.VMEM((8, OWN, CHUNK), F32),
                dma(OWN // PIECE), dma(1), dma(2), dma(4), dma(4), dma(OWN // PIECE), dma(OWN // PIECE),
                dma(3), dma(16), dma(6, 4), dma(4), dma(16), dma(16),
                dma(3), dma(4), dma(4), dma(4), dma(8), dma(8), dma(8),
            ],
            compiler_params=pltpu.CompilerParams(collective_id=0, has_side_effects=True, vmem_limit_bytes=67043328),
        )(x, gain, wq, wk, wv, wo)

    tokens, whole = P(("dp", "sp"), None), P(None, None)
    return jax.shard_map(
        step,
        mesh=mesh,
        in_specs=(tokens, P(None), whole, whole, whole, whole),
        out_specs=tokens,
        check_vma=False,
    )
```

```python
import jax
import jax.numpy as jnp
from jax import lax
from jax.experimental import pallas as pl
from jax.experimental.pallas import tpu as pltpu
from jax.sharding import PartitionSpec as P

scope = jax.named_scope
HEAD = 128
LOG2_THETA = 13.287712379549449
LOG2E = 1.4426950408889634
NEG = -1e30
HIDDEN = -2e30
D = 4096
OWN = 128
PIECE = 32
UNIT = 256
LINE = 4 * UNIT
CHUNK = 512
STRIP = 512
E = HEAD**-0.5 * LOG2E
BF, F32 = jnp.bfloat16, jnp.float32


def _dot(a, b):
    return lax.dot_general(a, b, (((1,), (0,)), ((), ())), preferred_element_type=F32)


def kernel(x_hbm, gain_hbm, wq_hbm, wk_hbm, wv_hbm, wo_hbm, y_hbm,
           xs, gain_s, a_s, cos_s, sin_s, wks, wqs, wos, kv, stage, qt, q_stage, vt, top_a, top_b, mix_a, mix_b, s_a, s_b, m_a, m_b, p_a, p_b, k_a, k_b, seen_s, o_stage, part_s, other_s,
           x_sem, gain_sem, k_sem, wq_sem, wo_sem, swap_send, swap_recv, plane_send, block_recv, z_send, relay_send, hand_send, hand_recv,
           q_send, q_recv, out_send, out_recv, part_send, part_recv, y_sem):
    me = lax.axis_index("sp")
    core, chip = lax.rem(me, 2), lax.div(me, 2)
    z, line = lax.rem(chip, 4), lax.div(chip, 4)
    y, x = lax.rem(line, 2), lax.div(line, 2)
    partner = me + 1 - 2 * core

    def in_plane(l):
        return me + (lax.div(l, 2) - x) * 16 + (lax.rem(l, 2) - y) * 8

    def mate(j):
        dx, dy = 1 - lax.div(j, 2), lax.rem(j + 1, 2)
        return lax.rem(x + dx, 2) * 2 + lax.rem(y + dy, 2)

    def get_x(r):
        at = pl.ds(r * PIECE, PIECE)
        return pltpu.make_async_copy(x_hbm.at[at], xs.at[core, at], x_sem.at[r])

    get_k = pltpu.make_async_copy(wk_hbm, wks, k_sem.at[0])
    get_v = pltpu.make_async_copy(wv_hbm, wqs.at[2], k_sem.at[1])

    def get_q(j):
        at = pl.multiple_of(mate(j) * 1024 + core * 512, CHUNK)
        return pltpu.make_async_copy(wq_hbm.at[:, pl.ds(at, CHUNK)], wqs.at[lax.rem(j, 3)], wq_sem.at[j])

    def get_o(h):
        return pltpu.make_async_copy(wo_hbm.at[pl.ds(pl.multiple_of(h * 1024 + core * 512, CHUNK), CHUNK)], wos.at[h], wo_sem.at[h])

    get_gain = pltpu.make_async_copy(gain_hbm, gain_s, gain_sem.at[0])
    get_x(0).start()
    get_gain.start()
    for r in range(1, OWN // PIECE):
        get_x(r).start()

    kv[:, 12:] = jnp.zeros((2, 4, 2, OWN, HEAD), BF)

    barrier = pltpu.get_barrier_semaphore()

    def greet(device):
        pl.semaphore_signal(barrier, inc=1, device_id={"sp": device}, device_id_type=pl.DeviceIdType.MESH)

    greet(partner)
    for j in range(3):
        greet(in_plane(mate(j)))
    pl.when(z > 0)(lambda: greet(me - 2))
    pl.when(z < 3)(lambda: greet(me + 2))
    greet(jnp.where(z < 2, me + 4, me - 4))
    pl.when(z == 0)(lambda: greet(me + 6))
    pl.when(z == 3)(lambda: greet(me - 6))
    def remote(src, dst, send, recv, device):
        return pltpu.make_async_remote_copy(src_ref=src, dst_ref=dst, send_sem=send, recv_sem=recv, device_id={"sp": device},
                                            device_id_type=pl.DeviceIdType.MESH)

    def swap(which, r):
        at = pl.ds(r * PIECE, PIECE)
        return remote(xs.at[which, at], xs.at[which, at], swap_send.at[r], swap_recv.at[r], partner)

    def norm(which, r):
        at = pl.ds(r * PIECE, PIECE)
        wide = xs[which, at, :].astype(F32)
        scale = lax.rsqrt(jnp.mean(wide * wide, -1, keepdims=True) + 1e-6)
        a_s[which, at, :] = (wide * scale * gain_s[...].astype(F32).reshape(1, D)).astype(BF)

    with scope("x_in"):
        for r in range(OWN // PIECE):
            get_x(r).wait()
            if r == 0:
                get_k.start()
                get_v.start()
                get_gain.wait()
            norm(core, r)
    with scope("barrier"):
        pl.semaphore_wait(barrier, 7)
    for r in range(OWN // PIECE):
        swap(core, r).start()

    def turned(t, cos, sin):
        t = t.astype(F32)
        return (t * cos + pltpu.roll(t, HEAD // 2, 1) * sin).astype(BF)

    def block(b):
        return kv.at[core, b]

    def to_mate(j):
        l = mate(j)
        return remote(stage.at[l], block(4 * line + z), plane_send.at[j], block_recv.at[4 * line + z], in_plane(l))

    def arrived(b):
        remote(block(b), block(b), z_send.at[0, 0], block_recv.at[b], partner).wait_recv()

    STEPS = (3, -3, 2, -2, 1, -1)

    def direct(l):
        return (l == line) | (l == 0)

    def along_z(l, act):
        for i, step in enumerate(STEPS):
            b = 4 * l + z
            copy = remote(block(b), block(b), z_send.at[i, l], block_recv.at[b], me + 2 * step)
            there = z + step
            yes = (there >= 0) & (there < 4)
            if step < 0:
                yes = yes & (l < 3)
            if abs(step) == 3:
                yes = yes & direct(l)
            pl.when(yes)(lambda copy=copy: act(copy))

    def relay(l, act):
        up = remote(block(4 * l), block(4 * l), relay_send.at[l], block_recv.at[4 * l], me + 2)
        down = remote(block(4 * l + 3), block(4 * l + 3), relay_send.at[l], block_recv.at[4 * l + 3], me - 2)
        pl.when((z == 2) & ~direct(l))(lambda: act(up))
        pl.when((z == 1) & (l < 3) & ~direct(l))(lambda: act(down))

    def hand(b):
        return remote(block(b), block(b), hand_send.at[b], hand_recv.at[b], partner)

    start = lambda copy: copy.start()
    sent = lambda copy: copy.wait_send()

    place = chip * UNIT + lax.broadcasted_iota(jnp.int32, (UNIT, HEAD), 0)
    element = lax.broadcasted_iota(jnp.int32, (1, HEAD), 1)
    freq = jnp.exp2(lax.rem(element, HEAD // 2).astype(F32) * (-LOG2_THETA * 2 / HEAD))
    angle = place.astype(F32) * freq
    sin = jnp.sin(angle)
    cos_s[...] = jnp.cos(angle)
    sin_s[...] = jnp.where(element < HEAD // 2, -sin, sin)
    with scope("kw"):
        get_k.wait()
    a, rows = a_s[core], pl.ds(pl.multiple_of(core * OWN, OWN), OWN)
    t = _dot(a, wks[...]).astype(BF)
    for h in range(4):
        stage[h, 0] = turned(t[:, h * HEAD : (h + 1) * HEAD], cos_s[rows, :], sin_s[rows, :])
    get_q(0).start()
    with scope("vw"):
        get_v.wait()
    get_q(1).start()
    t = _dot(a, wqs[2]).astype(BF)
    for h in range(4):
        stage[h, 1] = t[:, h * HEAD : (h + 1) * HEAD]
    get_q(2).start()
    for j in range(3):
        to_mate(j).start()
    kv[core, 4 * line + z] = stage[line]
    along_z(line, start)
    hand(4 * line + z).start()

    with scope("swap"):
        for r in range(OWN // PIECE):
            swap(1 - core, r).wait_recv()
            norm(1 - core, r)

    def q_copy(j):
        return remote(q_stage.at[j], qt.at[line], q_send.at[j], q_recv.at[line], in_plane(mate(j)))

    def take_plane(l):
        arrived(4 * l + z)
        along_z(l, start)
        hand(4 * l + z).start()

    late_y = x == 1

    def project_q(j, _):
        get_q(j).wait()
        q = _dot(a_s[...].reshape(UNIT, D), wqs[lax.rem(j, 3)]).astype(BF)
        for n in range(4):
            q_stage[j, :, n * UNIT : (n + 1) * UNIT] = turned(q[:, n * HEAD : (n + 1) * HEAD], cos_s[...], sin_s[...]).T
        pl.when(j < 3)(lambda: q_copy(j).start())

        @pl.when(j == 0)
        def _():
            get_q(3).start()

        @pl.when(j == 2)
        def _():
            with scope("plane"):
                def take(l, _):
                    pl.when((l != line) & ~(late_y & (l == mate(2))))(lambda: take_plane(l))

                lax.fori_loop(0, 4, take, None)

    with scope("q_proj"):
        lax.fori_loop(0, 4, project_q, None)
    qt[line] = q_stage[3]
    for h in range(4):
        get_o(h).start()

    top_s, mix_s, score_s, most_s, weight_s, keep_s = (top_a, top_b), (mix_a, mix_b), (s_a, s_b), (m_a, m_b), (p_a, p_b), (k_a, k_b)
    for n in range(2):
        top_s[n][...] = jnp.full((4, 1, STRIP), NEG, F32)
        mix_s[n][...] = jnp.zeros((4, HEAD + 8, STRIP), F32)

    def used(l, place):
        return (place != z) & ((l < 3) | (place < z))

    def relayed(l, place):
        return used(l, place) & ~direct(l) & ({0: z == 2, 3: z == 1}.get(place, z < 0))

    def take_relay(l):
        with scope("take_relay"):
            for place in (0, 3):
                @pl.when(relayed(l, place))
                def _():
                    arrived(4 * l + place)
                    relay(l, start)
                    hand(4 * l + place).start()

    def take_z(l):
        with scope("take_z"):
            for place in (0, 3, 1, 2):
                @pl.when(used(l, place) & ~relayed(l, place))
                def _():
                    arrived(4 * l + place)
                    hand(4 * l + place).start()

    def scores(l, g, n, masked):
        t = _dot(kv[:, pl.ds(4 * g, 4), 0].reshape(LINE, HEAD), qt[l, :, n * STRIP : (n + 1) * STRIP])
        if masked:
            at = lax.broadcasted_iota(jnp.int32, (LINE, 1), 0)
            key = lax.div(at, 2 * UNIT) * OWN + lax.div(lax.rem(at, 2 * UNIT), OWN) * UNIT + lax.rem(at, OWN)
            query = z * UNIT + lax.rem(lax.broadcasted_iota(jnp.int32, (1, STRIP), 1), UNIT)
            t = jnp.where(query >= key, t, HIDDEN)
        score_s[n][...] = t
        most_s[n][...] = t.max(axis=0, keepdims=True)

    def weights(l, n):
        old = top_s[n][l]
        top = jnp.maximum(old, most_s[n][...])
        top_s[n][l] = top
        keep_s[n][...] = jnp.exp2((old - top) * E)
        weight_s[n][...] = jnp.exp2((score_s[n][...] - top) * E).astype(BF)

    def values(l, g, n):
        v = jnp.concatenate([vt[g], jnp.ones((8, LINE), BF)], 0)
        mix_s[n][l] = mix_s[n][l] * keep_s[n][...] + _dot(v, weight_s[n][...])

    def attend(l, g, masked):
        with scope("attend_alone"):
            for n in range(2):
                scores(l, g, n, masked)
            for n in range(2):
                weights(l, n)
            for n in range(2):
                values(l, g, n)

    def attend_next(l, g, masked, l0, g0):
        with scope("attend#m=%d" % masked):
            scores(l, g, 0, masked)
            weights(l0, 1)
            values(l0, g0, 0)
            scores(l, g, 1, masked)
            weights(l, 0)
            values(l0, g0, 1)

    def out_copy(l):
        return remote(o_stage.at[l], seen_s.at[line], out_send.at[l], out_recv.at[line], in_plane(l))

    def complete(l):
        with scope("complete"):
            for n in range(2):
                out = (mix_s[n][l, :HEAD, :] * (1 / mix_s[n][l, HEAD : HEAD + 1, :])).astype(BF)
                for m in range(2):
                    h = 2 * n + m
                    o_stage[l, :, h * HEAD : (h + 1) * HEAD] = out[:, m * UNIT : (m + 1) * UNIT].T
            pl.when(l != line)(lambda: out_copy(l).start())

            @pl.when(l == line)
            def _():
                seen_s[line] = o_stage[l]

    def handed(g):
        with scope("hand_wait"):
            for place in range(4):
                @pl.when((g < 3) | (place <= z))
                def _():
                    b = 4 * g + place
                    remote(kv.at[1 - core, b], kv.at[1 - core, b], hand_send.at[b], hand_recv.at[b], partner).wait_recv()
        for i in range(8):
            vt[g, :, i * OWN : (i + 1) * OWN] = kv[i // 4, 4 * g + i % 4, 1].T

    def q_wait(l):
        with scope("q_wait"):
            remote(qt.at[l], qt.at[l], q_send.at[0], q_recv.at[l], partner).wait_recv()

    def other(k):
        return jnp.where(line <= k, k + 1, k)

    across = mate(0)
    early = across > line
    take_z(line)
    handed(line)
    attend(line, line, True)
    with scope("plane_y"):
        pl.when(late_y)(lambda: take_plane(mate(2)))

    @pl.when(early)
    def _():
        q_wait(across)
        attend(across, line, False)

    take_relay(other(0))
    take_relay(other(1))

    @pl.when(line == 0)
    def _():
        complete(line)
        q_wait(mate(1))
        attend(mate(1), line, False)

    weight_s[0][...] = jnp.zeros((LINE, STRIP), BF)
    keep_s[0][...] = jnp.ones((1, STRIP), F32)
    score_s[1][...] = jnp.full((LINE, STRIP), HIDDEN, F32)
    most_s[1][...] = jnp.full((1, STRIP), NEG, F32)

    takes = (0, jnp.where(line == 3, 1, 0), jnp.where(line == 0, 1, 4))
    needs = (0, jnp.where(line == 3, 2, 1), jnp.where(line == 0, 2, 5))

    def row(i, carry):
        j = jnp.where((line == 1) & (i > 0) & (i < 3), 3 - i, i)
        l = mate(j)
        met = (j == 0) & early | (line == 0) & (j == 1)
        pl.when((l != line) & ~met)(lambda: q_wait(l))

        def meet(g, carry):
            s, l0, g0 = carry
            done = (g == line) & ((l == line) | met)

            @pl.when(~done)
            def _():
                pl.when(s == jnp.where(line == 0, 0, 2))(lambda: take_relay(other(2)))
                for k in range(3):
                    pl.when(s == takes[k])(lambda k=k: take_z(other(k)))
                for k in range(3):
                    pl.when(s == needs[k])(lambda k=k: handed(other(k)))
                pl.when(l == g)(lambda: attend_next(l, g, True, l0, g0))
                pl.when(l > g)(lambda: attend_next(l, g, False, l0, g0))
                pl.when((s > 0) & (l0 != l))(lambda: complete(l0))

            return jnp.where(done, s, s + 1), jnp.where(done, l0, l), jnp.where(done, g0, g)

        return lax.fori_loop(0, l + 1, meet, carry)

    _, last, g0 = lax.fori_loop(0, 4, row, (0, line, line))
    with scope("attend_last"):
        weights(last, 1)
        for n in range(2):
            values(last, g0, n)
    complete(last)

    def give(c):
        return remote(part_s.at[c, 1 - core], other_s.at[c], part_send.at[c], part_recv.at[c], partner)

    def product(c, hs):
        at = pl.ds(pl.multiple_of(c * CHUNK, CHUNK), CHUNK)
        seen = jnp.concatenate([seen_s[h] for h in hs], 1)
        return _dot(seen, jnp.concatenate([wos[h, :, at] for h in hs], 0)).reshape(2, OWN, CHUNK)

    def put(c):
        at = pl.ds(pl.multiple_of(c * CHUNK, CHUNK), CHUNK)
        return pltpu.make_async_copy(a_s.at[0, :, at], y_hbm.at[:, at], y_sem.at[c])

    def finish(c):
        give(c).wait_recv()
        at = pl.ds(pl.multiple_of(c * CHUNK, CHUNK), CHUNK)
        a_s[0, :, at] = (xs[core, :, at].astype(F32) + (part_s[c, core] + other_s[c])).astype(BF)
        put(c).start()

    def seen_wait(l):
        with scope("seen_wait"):
            remote(seen_s.at[l], seen_s.at[l], out_send.at[0], out_recv.at[l], partner).wait_recv()

    for h in range(4):
        get_o(h).wait()
    seen_wait(mate(0))

    def project_early(c, _):
        both = [product(2 * c + i, (line, mate(0))) for i in range(2)]
        for i in range(2):
            part_s[2 * c + i] = both[i]

    with scope("o_early"):
        lax.fori_loop(0, 4, project_early, None)
    for r in range(OWN // PIECE):
        swap(core, r).wait_send()
    for j in range(3):
        to_mate(j).wait_send()
        q_copy(j).wait_send()

    def drain(l, _):
        along_z(l, sent)
        relay(l, sent)
        for place in range(4):
            pl.when((l < 3) | (place <= z))(lambda place=place: hand(4 * l + place).wait_send())

    lax.fori_loop(0, 4, drain, None)

    seen_wait(mate(1))
    seen_wait(mate(2))

    def project_late(c, _):
        both = [part_s[2 * c + i] + product(2 * c + i, (mate(1), mate(2))) for i in range(2)]
        for i in range(2):
            part_s[2 * c + i] = both[i]
        for i in range(2):
            give(2 * c + i).start()

        @pl.when(c > 1)
        def _():
            finish(2 * c - 4)
            finish(2 * c - 3)

    with scope("o_late"):
        lax.fori_loop(0, 4, project_late, None)
    with scope("finish"):
        for c in range(4, 8):
            finish(c)

    lax.fori_loop(0, 4, lambda l, _: pl.when(l != line)(lambda: out_copy(l).wait_send()), None)

    def drain_chunk(c, _):
        give(c).wait_send()
        put(c).wait()

    lax.fori_loop(0, 8, drain_chunk, None)


def solution(mesh):
    def step(x, gain, wq, wk, wv, wo):
        hbm = pl.BlockSpec(memory_space=pl.ANY)
        dma = lambda *shape: pltpu.SemaphoreType.DMA(shape)
        return pl.pallas_call(
            kernel,
            out_shape=jax.ShapeDtypeStruct((OWN, D), BF),
            in_specs=[hbm] * 6,
            out_specs=hbm,
            scratch_shapes=[
                pltpu.VMEM((2, OWN, D), BF),
                pltpu.VMEM((D,), BF),
                pltpu.VMEM((2, OWN, D), BF),
                pltpu.VMEM((UNIT, HEAD), F32),
                pltpu.VMEM((UNIT, HEAD), F32),
                pltpu.VMEM((D, 512), BF),
                pltpu.VMEM((3, D, CHUNK), BF),
                pltpu.VMEM((4, CHUNK, D), BF),
                pltpu.VMEM((2, 16, 2, OWN, HEAD), BF),
                pltpu.VMEM((4, 2, OWN, HEAD), BF),
                pltpu.VMEM((4, HEAD, 4 * UNIT), BF),
                pltpu.VMEM((4, HEAD, 4 * UNIT), BF),
                pltpu.VMEM((4, HEAD, LINE), BF),
                *[pltpu.VMEM((4, 1, STRIP), F32)] * 2,
                *[pltpu.VMEM((4, HEAD + 8, STRIP), F32)] * 2,
                *[pltpu.VMEM((LINE, STRIP), F32)] * 2,
                *[pltpu.VMEM((1, STRIP), F32)] * 2,
                *[pltpu.VMEM((LINE, STRIP), BF)] * 2,
                *[pltpu.VMEM((1, STRIP), F32)] * 2,
                pltpu.VMEM((4, UNIT, 4 * HEAD), BF),
                pltpu.VMEM((4, UNIT, 4 * HEAD), BF),
                pltpu.VMEM((8, 2, OWN, CHUNK), F32),
                pltpu.VMEM((8, OWN, CHUNK), F32),
                dma(OWN // PIECE), dma(1), dma(2), dma(4), dma(4), dma(OWN // PIECE), dma(OWN // PIECE),
                dma(3), dma(16), dma(6, 4), dma(4), dma(16), dma(16),
                dma(3), dma(4), dma(4), dma(4), dma(8), dma(8), dma(8),
            ],
            compiler_params=pltpu.CompilerParams(collective_id=0, has_side_effects=True, vmem_limit_bytes=67043328),
        )(x, gain, wq, wk, wv, wo)

    tokens, whole = P(("dp", "sp"), None), P(None, None)
    return jax.shard_map(
        step,
        mesh=mesh,
        in_specs=(tokens, P(None), whole, whole, whole, whole),
        out_specs=tokens,
        check_vma=False,
    )
```
